16 devices in a mesh: dp: 2 (over y, z), tp: 8 (over x, core).
Axes of the slice: x: 4, y: 2, z: 1, core: 2. Of those that a mesh axis runs over, the one named last changes fastest.
The devices are a block of a 4x4x8 slice.
Arguments:
- tokens: int32 [2, 128], P('dp'), parts along dimension 0
- positions: int32 [2, 128], P('dp'), parts along dimension 0
- embedding: bfloat16 [16384, 3072], P('tp')
- gain_attn: float32 [3072], replicated
- gain_mlp: float32 [3072], replicated
- w_query: bfloat16 [3072, 24, 128], P(None, 'tp')
- w_key: bfloat16 [3072, 8, 128], P(None, 'tp')
- w_value: bfloat16 [3072, 8, 128], P(None, 'tp')
- w_out: bfloat16 [24, 128, 3072], P('tp')
- w_gate: bfloat16 [3072, 8192], P(None, 'tp')
- w_up: bfloat16 [3072, 8192], P(None, 'tp')
- w_down: bfloat16 [8192, 3072], P('tp')
- grad_hidden: bfloat16 [2, 128, 3072], P('dp', 'tp'), parts along dimension 0
Outputs:
- output 1: bfloat16 [2, 128, 3072], P('dp', 'tp'), parts along dimension 0
- output 2: float32 [32768, 3072], P(('dp', 'tp')), parts along dimension 0
- output 3: float32 [6144, 24, 128], P('dp', 'tp'), parts along dimension 0
- output 4: float32 [6144, 8, 128], P('dp', 'tp'), parts along dimension 0
- output 5: float32 [6144, 8, 128], P('dp', 'tp'), parts along dimension 0
- output 6: float32 [48, 128, 3072], P(('dp', 'tp')), parts along dimension 0
- output 7: float32 [6144, 8192], P('dp', 'tp'), parts along dimension 0
- output 8: float32 [6144, 8192], P('dp', 'tp'), parts along dimension 0
- output 9: float32 [16384, 3072], P(('dp', 'tp')), parts along dimension 0
- output 10: float32 [6144], P('dp'), parts along dimension 0
- output 11: float32 [6144], P('dp'), parts along dimension 0
There are 2 independent parts. The reference program is written for one: setup_inputs(seed, part) draws one part's arguments, and reference() takes and returns one part's arrays. A program takes and returns all parts, laid end to end along the dimension named above; an argument that names none is the same for every part.
All inputs are finite; a program needn't handle non-finite values.
Results may differ from the reference program's by a relative error of at most 0.02.
Values are sent between devices in bfloat16 or wider.
A program may use at most 768 MiB of HBM per device.

```python
import jax
import jax.numpy as jnp
from jax import lax

BATCH_SIZE = 1
SEQ_LEN = 128
VOCAB_SIZE = 16384
MODEL_DIM = 3072
NUM_HEADS = 24
KV_HEADS = 8
HEAD_DIM = 128
FFN_DIM = 8192
HOT_COUNT = 16
ROPE_THETA = 1000000.0
RMS_EPS = 1e-5


def draw_tokens(rng_key):
    sub_keys = jax.random.split(rng_key, 7)
    tok_shape = (BATCH_SIZE, SEQ_LEN)
    first_draw = jax.random.randint(sub_keys[0], tok_shape, 0, VOCAB_SIZE)
    second_draw = jax.random.randint(sub_keys[1], tok_shape, 0, VOCAB_SIZE)
    base_ids = jnp.minimum(first_draw, second_draw)
    hot_ids = jax.random.randint(sub_keys[2], (HOT_COUNT,), 0, VOCAB_SIZE)
    hot_pick = jax.random.randint(sub_keys[3], tok_shape, 0, HOT_COUNT)
    use_hot = jax.random.randint(sub_keys[4], tok_shape, 0, 4) == 0
    token_ids = jnp.where(use_hot, hot_ids[hot_pick], base_ids)
    top_place = jax.random.randint(sub_keys[5], (), 0, SEQ_LEN // 2)
    low_place = jax.random.randint(sub_keys[6], (), SEQ_LEN // 2, SEQ_LEN)
    token_ids = token_ids.at[0, top_place].set(VOCAB_SIZE - 1)
    token_ids = token_ids.at[0, low_place].set(0)
    return token_ids.astype(jnp.int32)


def draw_positions(rng_key):
    pos_steps = jax.random.randint(rng_key, (BATCH_SIZE, SEQ_LEN), 1, 4)
    return jnp.cumsum(pos_steps, axis=1).astype(jnp.int32)


def scaled_normal(rng_key, dim_shape, factor):
    return (jax.random.normal(rng_key, dim_shape, jnp.float32) * factor).astype(jnp.bfloat16)


def setup_inputs(seed: int = 0, part: int = 0) -> dict:
    shared = jax.random.split(jax.random.key(seed), 10)
    part_keys = jax.random.split(jax.random.fold_in(jax.random.key(seed + 1), part), 3)
    in_scale = MODEL_DIM ** -0.5
    return {
        'tokens': draw_tokens(part_keys[0]),
        'positions': draw_positions(part_keys[1]),
        'embedding': scaled_normal(shared[0], (VOCAB_SIZE, MODEL_DIM), 1.0),
        'gain_attn': 1.0 + 0.25 * jax.random.normal(shared[1], (MODEL_DIM,), jnp.float32),
        'gain_mlp': 1.0 + 0.25 * jax.random.normal(shared[2], (MODEL_DIM,), jnp.float32),
        'w_query': scaled_normal(shared[3], (MODEL_DIM, NUM_HEADS, HEAD_DIM), in_scale),
        'w_key': scaled_normal(shared[4], (MODEL_DIM, KV_HEADS, HEAD_DIM), in_scale),
        'w_value': scaled_normal(shared[5], (MODEL_DIM, KV_HEADS, HEAD_DIM), in_scale),
        'w_out': scaled_normal(shared[6], (NUM_HEADS, HEAD_DIM, MODEL_DIM), (NUM_HEADS * HEAD_DIM) ** -0.5),
        'w_gate': scaled_normal(shared[7], (MODEL_DIM, FFN_DIM), in_scale),
        'w_up': scaled_normal(shared[8], (MODEL_DIM, FFN_DIM), in_scale),
        'w_down': scaled_normal(shared[9], (FFN_DIM, MODEL_DIM), FFN_DIM ** -0.5),
        'grad_hidden': scaled_normal(part_keys[2], (BATCH_SIZE, SEQ_LEN, MODEL_DIM), 1.0),
    }


def rope_tables(positions, head_dim):
    half_dim = head_dim // 2
    inv_freq = ROPE_THETA ** (-jnp.arange(half_dim, dtype=jnp.float32) * (2.0 / head_dim))
    angles = positions.astype(jnp.float32)[:, :, None] * inv_freq
    return jnp.cos(angles)[:, :, None, :], jnp.sin(angles)[:, :, None, :]


def rotate(values, cos_tab, sin_tab):
    half_dim = values.shape[-1] // 2
    first_half = values[..., :half_dim]
    second_half = values[..., half_dim:]
    return jnp.concatenate([first_half * cos_tab - second_half * sin_tab, second_half * cos_tab + first_half * sin_tab], axis=-1)


def rms_norm(hidden, gain_vec):
    hidden_f = hidden.astype(jnp.float32)
    inv_rms = lax.rsqrt(jnp.mean(hidden_f * hidden_f, axis=-1, keepdims=True) + RMS_EPS)
    return (hidden_f * inv_rms * gain_vec).astype(jnp.bfloat16)


def layer(first_x, gain_pair, weight_mats, positions):
    w_query, w_key, w_value, w_out, w_gate, w_up, w_down = weight_mats
    batch_size, seq_len = positions.shape
    num_heads, head_dim = w_query.shape[1], w_query.shape[2]
    kv_heads = w_key.shape[1]
    group_size = num_heads // kv_heads
    cos_tab, sin_tab = rope_tables(positions, head_dim)
    normed1 = rms_norm(first_x, gain_pair[0]).astype(jnp.float32)
    queries = rotate(jnp.einsum('bsd,dhe->bshe', normed1, w_query), cos_tab, sin_tab)
    queries = queries.astype(jnp.bfloat16).astype(jnp.float32).reshape(batch_size, seq_len, kv_heads, group_size, head_dim)
    keys_rot = rotate(jnp.einsum('bsd,dhe->bshe', normed1, w_key), cos_tab, sin_tab).astype(jnp.bfloat16).astype(jnp.float32)
    values = jnp.einsum('bsd,dhe->bshe', normed1, w_value).astype(jnp.bfloat16).astype(jnp.float32)
    causal = jnp.arange(seq_len)[:, None] >= jnp.arange(seq_len)[None, :]
    scores = jnp.einsum('bqkgd,bskd->bkgqs', queries, keys_rot) * head_dim ** -0.5
    probs_f = jax.nn.softmax(jnp.where(causal, scores, -1e30), axis=-1)
    probs_r = probs_f.astype(jnp.bfloat16).astype(jnp.float32)
    attn_heads = jnp.einsum('bkgqs,bskd->bqkgd', probs_r, values).astype(jnp.bfloat16).astype(jnp.float32)
    attn_heads = attn_heads.reshape(batch_size, seq_len, num_heads, head_dim)
    attn_out = jnp.einsum('bshe,hed->bsd', attn_heads, w_out)
    hidden1 = (first_x.astype(jnp.float32) + attn_out).astype(jnp.bfloat16)
    normed2 = rms_norm(hidden1, gain_pair[1]).astype(jnp.float32)
    gate_pre = jnp.einsum('bsd,df->bsf', normed2, w_gate)
    up_pre = jnp.einsum('bsd,df->bsf', normed2, w_up)
    act_r = (jax.nn.silu(gate_pre) * up_pre).astype(jnp.bfloat16).astype(jnp.float32)
    mlp_out = jnp.einsum('bsf,fd->bsd', act_r, w_down)
    return (hidden1.astype(jnp.float32) + mlp_out).astype(jnp.bfloat16)


def reference(tokens, positions, embedding, gain_attn, gain_mlp, w_query, w_key, w_value, w_out, w_gate, w_up, w_down, grad_hidden):
    first_x = jnp.take(embedding, tokens, axis=0)
    weight_mats = tuple(weight.astype(jnp.float32) for weight in (w_query, w_key, w_value, w_out, w_gate, w_up, w_down))
    hidden_out, back_fn = jax.vjp(lambda x_in, gain_pair, mats_in: layer(x_in, gain_pair, mats_in, positions), first_x, (gain_attn, gain_mlp), weight_mats)
    grad_x, grad_gains, grad_mats = back_fn(grad_hidden)
    grad_embedding = jax.ops.segment_sum(grad_x.reshape(-1, MODEL_DIM).astype(jnp.float32), tokens.reshape(-1), num_segments=VOCAB_SIZE)
    return (hidden_out, grad_embedding, grad_mats[0], grad_mats[1], grad_mats[2], grad_mats[3], grad_mats[4], grad_mats[5], grad_mats[6], grad_gains[0], grad_gains[1])
```

```python
import functools

import jax
import jax.numpy as jnp
from jax import lax
from jax.experimental import pallas as pl
from jax.experimental.pallas import tpu as pltpu
from jax.sharding import PartitionSpec as P

ROPE_THETA = 1000000.0
RMS_EPS = 1e-5
BF = jnp.bfloat16
F32 = jnp.float32
VMEM_FULL = 67043328
CHIPS = 4
CORES = 2


def dot(a, b):
    return lax.dot_general(a, b, (((1,), (0,)), ((), ())), preferred_element_type=F32)


def dot_bt(a, b):
    return lax.dot_general(a, b, (((1,), (1,)), ((), ())), preferred_element_type=F32)


def dot_at(a, b):
    return lax.dot_general(a, b, (((0,), (0,)), ((), ())), preferred_element_type=F32)


class Place:
    def __init__(self):
        me = lax.axis_index('tp')
        self.chip, self.core = me // CORES, me % CORES
        self.right_chip = (self.chip + 1) % CHIPS
        self.left_chip = (self.chip + CHIPS - 1) % CHIPS
        self.far_chip = (self.chip + 2) % CHIPS
        self.me = me
        self.other = 1 - self.core
        self.partner = self.chip * CORES + self.other
        self.right = self.right_chip * CORES + self.core
        self.left = self.left_chip * CORES + self.core
        self.far = self.far_chip * CORES + self.core


def remote(src, dst, send, recv, device):
    return pltpu.make_async_remote_copy(src_ref=src, dst_ref=dst, send_sem=send, recv_sem=recv,
                                        device_id={'tp': device}, device_id_type=pl.DeviceIdType.MESH)


def entry_barrier(pos):
    barrier = pltpu.get_barrier_semaphore()
    for device in (pos.left, pos.right, pos.partner):
        pl.semaphore_signal(barrier, inc=1, device_id={'tp': device}, device_id_type=pl.DeviceIdType.MESH)
    pl.semaphore_wait(barrier, 3)


class Gather:
    def __init__(self, pos, buf, send, recv):
        self.pos, self.buf = pos, buf
        half = buf.shape[-1] // 2
        p = pos
        other = p.other - p.core

        def piece(slot, part):
            if part == 2:
                return buf.at[slot]
            return buf.at[slot, :, pl.ds(part * half, half)]

        def copy(index, slot, part, device):
            ref = piece(slot, part)
            return remote(ref, ref, send.at[index], recv.at[index], device)

        plan = {
            0: ((p.me, 0, p.right), (p.left, 0)), 1: ((p.me, 1, p.left), (p.right, 1)),
            2: ((p.me, 2, p.partner), (p.partner, 2)),
            3: ((p.me, 1, p.right), (p.left, 1)), 4: ((p.me, 0, p.left), (p.right, 0)),
            5: ((p.left, 0, p.right), (p.far, 0)), 6: ((p.right, 1, p.left), (p.far, 1)),
            7: ((p.left, 0, p.partner), (p.left + other, 0)), 8: ((p.right, 1, p.partner), (p.right + other, 1)),
            9: ((p.left, 1, p.partner), (p.left + other, 1)), 10: ((p.right, 0, p.partner), (p.right + other, 0)),
            11: ((p.far, 0, p.partner), (p.far + other, 0)), 12: ((p.far, 1, p.partner), (p.far + other, 1)),
        }
        self.out = {i: copy(i, *s) for i, (s, _) in plan.items()}
        self.into = {i: copy(i, slot, part, p.partner) for i, (_, (slot, part)) in plan.items()}

    def start(self):
        for i in (0, 1, 2, 3, 4):
            self.out[i].start()

    def relay(self):
        for i, onward in ((0, (5, 7)), (1, (6, 8)), (3, (9,)), (4, (10,))):
            self.into[i].wait_recv()
            for j in onward:
                self.out[j].start()

    def finish(self):
        for i, j in ((5, 11), (6, 12)):
            self.into[i].wait_recv()
            self.out[j].start()
        for i in (2, 7, 8, 9, 10, 11, 12):
            self.into[i].wait_recv()

    def drain(self):
        for i in range(13):
            self.out[i].wait_send()

    def run(self):
        self.start()
        self.relay()
        self.finish()
        self.drain()


class Scatter:
    def __init__(self, pos, part, from_partner, work, arrive, send, recv):
        p = pos
        self.pos, self.part, self.from_partner, self.work, self.arrive = p, part, from_partner, work, arrive
        self.half = work.shape[-1]
        self.chips = (p.far_chip, p.right_chip, p.left_chip, p.chip)
        self.inner = [remote(part.at[p.other, y], from_partner.at[y], send.at[k], recv.at[k], p.partner)
                      for k, y in enumerate(self.chips)]
        self.outer = [remote(work.at[k], arrive.at[k], send.at[4 + k], recv.at[4 + k], p.right if k % 2 == 0 else p.left)
                      for k in range(6)]

    def pair(self, k, part):
        cols = pl.ds(part * self.half, self.half)
        y = self.chips[k]
        return self.part[self.pos.core, y, :, cols].astype(F32) + self.from_partner[y, :, cols].astype(F32)

    def send_sum(self, k, value):
        self.work[k] = value.astype(BF)
        self.outer[k].start()

    def start(self):
        for copy in self.inner:
            copy.start()

    def relay(self):
        self.inner[0].wait_recv()
        self.send_sum(0, self.pair(0, 0))
        self.send_sum(1, self.pair(0, 1))
        self.inner[1].wait_recv()
        self.send_sum(2, self.pair(1, 1))
        self.inner[2].wait_recv()
        self.send_sum(3, self.pair(2, 0))
        self.outer[0].wait_recv()
        self.send_sum(4, self.pair(1, 0) + self.arrive[0].astype(F32))
        self.outer[1].wait_recv()
        self.send_sum(5, self.pair(2, 1) + self.arrive[1].astype(F32))

    def finish(self):
        self.inner[3].wait_recv()
        for k in (2, 3, 4, 5):
            self.outer[k].wait_recv()
        low = self.pair(3, 0) + self.arrive[3].astype(F32) + self.arrive[4].astype(F32)
        high = self.pair(3, 1) + self.arrive[2].astype(F32) + self.arrive[5].astype(F32)
        return jnp.concatenate([low, high], axis=-1)

    def drain(self):
        for copy in self.inner + self.outer:
            copy.wait_send()

    def run(self):
        self.start()
        self.relay()
        total = self.finish()
        self.drain()
        return total


GATHER_SEMS = [pltpu.SemaphoreType.DMA((13,)), pltpu.SemaphoreType.DMA((13,))]
SCATTER_SEMS = [pltpu.SemaphoreType.DMA((10,)), pltpu.SemaphoreType.DMA((10,))]


def scatter_scratch(rows, dim):
    return [pltpu.VMEM((CHIPS, rows, dim), BF), pltpu.VMEM((6, rows, dim // 2), BF),
            pltpu.VMEM((6, rows, dim // 2), BF)] + SCATTER_SEMS


def put_part(part, value, col):
    rows, width = part.shape[2], value.shape[1]
    for b in range(CHIPS * CORES):
        part[b % CORES, b // CORES, :, pl.ds(col, width)] = value[b * rows:(b + 1) * rows].astype(BF)


def norm_stats(hidden_f):
    inv_rms = lax.rsqrt(jnp.mean(hidden_f * hidden_f, axis=-1, keepdims=True) + RMS_EPS)
    return hidden_f * inv_rms, inv_rms


def norm_bwd(grad_f, normed, inv_rms, gain):
    gain_part = jnp.sum(grad_f * normed, axis=0, keepdims=True)
    scaled = grad_f * gain
    return inv_rms * (scaled - normed * jnp.mean(scaled * normed, axis=-1, keepdims=True)), gain_part


def rope(values, cos2, sin2):
    return values * cos2 + pltpu.roll(values, values.shape[-1] // 2, axis=1) * sin2


def full(buf):
    blocks, rows, dim = buf.shape
    return buf[...].reshape(blocks * rows, dim)


def lookup_kernel(group_ids, pick_ref, emb_hbm, out_ref, groups, sem):
    count = groups.shape[0]

    @pl.loop(0, count)
    def _(i):
        pltpu.make_async_copy(emb_hbm.at[pl.ds(pl.multiple_of(group_ids[i] * 8, 8), 8)], groups.at[i], sem).start()

    pltpu.make_async_copy(groups, groups, sem).wait()
    seq = pick_ref.shape[0]
    col = lax.broadcasted_iota(jnp.int32, (seq, count * 8), 1)
    pick = jnp.where(col == pick_ref[...], 1.0, 0.0).astype(BF)
    dim = groups.shape[2]
    step = 512

    @pl.loop(0, dim // step)
    def _(j):
        cols = pl.ds(pl.multiple_of(j * step, step), step)
        block = groups[:, :, cols].reshape(count * 8, step)
        out_ref[:, cols] = dot(pick, block).astype(BF)


def lookup(tokens, emb):
    rows_local, dim = emb.shape
    seq = tokens.shape[0]
    order = jnp.transpose(tokens.reshape(CHIPS, CORES, -1), (1, 0, 2)).reshape(-1)
    local = order - lax.axis_index('tp') * rows_local
    owned = (local >= 0) & (local < rows_local)
    safe = jnp.clip(local, 0, rows_local - 1)
    pick = jnp.where(owned, jnp.arange(seq, dtype=jnp.int32) * 8 + safe % 8, -1)
    return pl.pallas_call(
        lookup_kernel,
        out_shape=jax.ShapeDtypeStruct((seq, dim), BF),
        grid_spec=pltpu.PrefetchScalarGridSpec(
            num_scalar_prefetch=1, grid=(),
            in_specs=[pl.BlockSpec(memory_space=pltpu.VMEM), pl.BlockSpec(memory_space=pltpu.HBM)],
            out_specs=pl.BlockSpec(memory_space=pltpu.VMEM),
            scratch_shapes=[pltpu.VMEM((seq, 8, dim), BF), pltpu.SemaphoreType.DMA]),
        compiler_params=pltpu.CompilerParams(vmem_limit_bytes=40 << 20),
        name='lookup',
    )((safe // 8).astype(jnp.int32), pick[:, None], emb)


def forward_kernel(emb_part, cos_ref, sin_ref, gain_attn, gain_mlp, grad_own,
                   wq_hbm, wk_hbm, wv_hbm, wo_hbm, wg_hbm, wu_hbm, wd_hbm,
                   x0_out, h1_out, n1_out, n2_out, gh_out, heads_out, q_out, k_out, v_out, probs_out,
                   act_out, dgate_out, dup_out, dn2_part,
                   wqkv, wo, wg, wu, wd, wsem, n1_buf, n2_buf, gh_buf, attn_part, gact,
                   rp1, wk1, ar1, ss1, rs1, rp2, wk2, ar2, ss2, rs2,
                   gs1, gr1, gs2, gr2, gs0, gr0):
    pos = Place()
    num_heads, dim, head_dim = wq_hbm.shape
    seq = n1_out.shape[0]
    ffn = wg.shape[1]
    loads = [pltpu.make_async_copy(wq_hbm.at[h], wqkv.at[:, pl.ds(h * head_dim, head_dim)], wsem.at[h])
             for h in range(num_heads)]
    loads.append(pltpu.make_async_copy(wk_hbm, wqkv.at[:, pl.ds(num_heads * head_dim, head_dim)], wsem.at[3]))
    loads.append(pltpu.make_async_copy(wv_hbm, wqkv.at[:, pl.ds((num_heads + 1) * head_dim, head_dim)], wsem.at[4]))
    for k, (src, dst) in enumerate(((wo_hbm, wo), (wd_hbm, wd), (wg_hbm, wg), (wu_hbm, wu))):
        loads.append(pltpu.make_async_copy(src, dst, wsem.at[5 + k]))
    for load in loads:
        load.start()
    entry_barrier(pos)

    first = Scatter(pos, emb_part, rp1, wk1, ar1, ss1, rs1).run()
    x0 = first
    x0_out[...] = x0.astype(BF)
    normed1, _ = norm_stats(x0)
    n1_buf[pos.me] = (normed1 * gain_attn[...]).astype(BF)
    gather1 = Gather(pos, n1_buf, gs1, gr1)
    gather1.run()

    gh_buf[pos.me] = grad_own[...]
    gather0 = Gather(pos, gh_buf, gs0, gr0)
    gather0.start()

    for load in loads[:5]:
        load.wait()
    n1 = full(n1_buf)
    qkv = dot(n1, wqkv[...])
    n1_out[...] = n1
    gather0.relay()
    cos2, sin2 = cos_ref[...], sin_ref[...]
    kq = num_heads * head_dim
    keys = rope(qkv[:, kq:kq + head_dim], cos2, sin2).astype(BF)
    values = qkv[:, kq + head_dim:].astype(BF)
    k_out[...] = keys
    v_out[...] = values
    row = lax.broadcasted_iota(jnp.int32, (seq, seq), 0)
    colm = lax.broadcasted_iota(jnp.int32, (seq, seq), 1)
    causal = row >= colm
    for h in range(num_heads):
        cols = slice(h * head_dim, (h + 1) * head_dim)
        query = rope(qkv[:, cols], cos2, sin2).astype(BF)
        q_out[:, cols] = query
        scores = jnp.where(causal, dot_bt(query, keys) * (head_dim ** -0.5), -1e30)
        top = jnp.max(scores, axis=-1, keepdims=True)
        expd = jnp.exp(scores - top)
        probs = expd / jnp.sum(expd, axis=-1, keepdims=True)
        probs_out[h] = probs
        heads_out[:, cols] = dot(probs.astype(BF), values).astype(BF)
    loads[5].wait()
    heads = heads_out[...]
    for j in range(dim // 512):
        put_part(attn_part, dot(heads, wo[:, j * 512:(j + 1) * 512]), j * 512)
    scatter2 = Scatter(pos, attn_part, rp2, wk2, ar2, ss2, rs2)
    scatter2.start()
    gather0.finish()
    scatter2.relay()

    loads[6].wait()
    gh = full(gh_buf)
    gh_out[...] = gh

    @pl.loop(0, ffn // 256)
    def _(j):
        rows = pl.ds(pl.multiple_of(j * 256, 256), 256)
        gact[:, rows] = dot_bt(gh_out[...], wd[rows, :]).astype(BF)

    attn_sum = scatter2.finish()
    h1 = (x0 + attn_sum).astype(BF)
    h1_out[...] = h1
    normed2, _ = norm_stats(h1.astype(F32))
    n2_buf[pos.me] = (normed2 * gain_mlp[...]).astype(BF)
    gather2 = Gather(pos, n2_buf, gs2, gr2)
    gather2.start()
    gather2.relay()
    loads[7].wait()
    loads[8].wait()
    gather2.finish()

    n2_out[...] = full(n2_buf)

    @pl.loop(0, ffn // 256)
    def _(j):
        cols = pl.ds(pl.multiple_of(j * 256, 256), 256)
        n2 = n2_out[...]
        gate_pre = dot(n2, wg[:, cols])
        up_pre = dot(n2, wu[:, cols])
        sig = jax.nn.sigmoid(gate_pre)
        gate_act = gate_pre * sig
        act_out[:, cols] = (gate_act * up_pre).astype(BF)
        grad_act = gact[:, cols].astype(F32)
        dup_out[:, cols] = (grad_act * gate_act).astype(BF)
        dgate_out[:, cols] = (grad_act * up_pre * sig * (1.0 + gate_pre * (1.0 - sig))).astype(BF)

    @pl.loop(0, dim // 512)
    def _(j):
        col = pl.multiple_of(j * 512, 512)
        rows = pl.ds(col, 512)
        put_part(dn2_part, dot_bt(dgate_out[...], wg[rows, :]) + dot_bt(dup_out[...], wu[rows, :]), col)

    gather0.drain()
    scatter2.drain()
    gather2.drain()


def forward(emb_part, cos2, sin2, gain_attn, gain_mlp, grad_own, wq, wk, wv, wo, wg, wu, wd):
    num_heads, dim, head_dim = wq.shape
    seq, ffn = cos2.shape[0], wg.shape[1]
    rows = seq // (CHIPS * CORES)
    vmem = pl.BlockSpec(memory_space=pltpu.VMEM)
    hbm = pl.BlockSpec(memory_space=pltpu.HBM)
    width = num_heads * head_dim
    sds = jax.ShapeDtypeStruct
    outs = [sds((rows, dim), BF), sds((rows, dim), BF), sds((seq, dim), BF), sds((seq, dim), BF), sds((seq, dim), BF),
            sds((seq, width), BF), sds((seq, width), BF), sds((seq, head_dim), BF), sds((seq, head_dim), BF),
            sds((num_heads, seq, seq), F32), sds((seq, ffn), BF), sds((seq, ffn), BF), sds((seq, ffn), BF),
            sds((CORES, CHIPS, rows, dim), BF)]
    scratch = [pltpu.VMEM((dim, width + 2 * head_dim), BF), pltpu.VMEM((width, dim), BF), pltpu.VMEM((dim, ffn), BF),
               pltpu.VMEM((dim, ffn), BF), pltpu.VMEM((ffn, dim), BF), pltpu.SemaphoreType.DMA((9,)),
               pltpu.VMEM((CHIPS * CORES, rows, dim), BF), pltpu.VMEM((CHIPS * CORES, rows, dim), BF),
               pltpu.VMEM((CHIPS * CORES, rows, dim), BF), pltpu.VMEM((CORES, CHIPS, rows, dim), BF),
               pltpu.VMEM((seq, ffn), BF)]
    scratch += scatter_scratch(rows, dim) + scatter_scratch(rows, dim) + GATHER_SEMS * 3
    return pl.pallas_call(
        forward_kernel, out_shape=outs, in_specs=[vmem] * 6 + [hbm] * 7, out_specs=[vmem] * len(outs),
        scratch_shapes=scratch,
        compiler_params=pltpu.CompilerParams(collective_id=0, has_side_effects=True, vmem_limit_bytes=56 << 20),
        name='forward',
    )(emb_part, cos2, sin2, gain_attn, gain_mlp, grad_own, wq, wk, wv, wo, wg, wu, wd)


def backward_kernel(dn2_part, act_ref, x0_ref, h1_ref, grad_own, cos_ref, sin_ref, gain_attn, gain_mlp,
                    q_ref, k_ref, v_ref, probs_ref, wq_hbm, wk_hbm, wv_hbm, wo_hbm, wd_hbm,
                    hidden_out, dh1_out, dqkv_out, dx_out, gains_out,
                    wqkv, wo, wd, wsem, dh1_buf, dx_buf, gain_buf, mlp_part, dn1_part,
                    rp6, wk6, ar6, ss6, rs6, rp5, wk5, ar5, ss5, rs5, rp8, wk8, ar8, ss8, rs8,
                    gs7, gr7, gs9, gr9, gsg, grg):
    pos = Place()
    num_heads, dim, head_dim = wq_hbm.shape
    seq, ffn = act_ref.shape
    loads = [pltpu.make_async_copy(wd_hbm, wd, wsem.at[0]), pltpu.make_async_copy(wo_hbm, wo, wsem.at[1])]
    loads += [pltpu.make_async_copy(wq_hbm.at[h], wqkv.at[:, pl.ds(h * head_dim, head_dim)], wsem.at[2 + h])
              for h in range(num_heads)]
    loads.append(pltpu.make_async_copy(wk_hbm, wqkv.at[:, pl.ds(num_heads * head_dim, head_dim)], wsem.at[5]))
    loads.append(pltpu.make_async_copy(wv_hbm, wqkv.at[:, pl.ds((num_heads + 1) * head_dim, head_dim)], wsem.at[6]))
    for load in loads:
        load.start()
    entry_barrier(pos)

    scatter6 = Scatter(pos, dn2_part, rp6, wk6, ar6, ss6, rs6)
    scatter6.start()
    scatter6.relay()
    h1 = h1_ref[...].astype(F32)
    normed2, inv2 = norm_stats(h1)
    grad_n2 = scatter6.finish().astype(BF).astype(F32)
    grad_h1_norm, gain_mlp_part = norm_bwd(grad_n2, normed2, inv2, gain_mlp[...])
    grad_h1 = (grad_own[...].astype(F32) + grad_h1_norm).astype(BF)
    dh1_buf[pos.me] = grad_h1
    gain_buf[pos.me, 1:2, :] = gain_mlp_part
    gather7 = Gather(pos, dh1_buf, gs7, gr7)
    gather7.start()
    gather7.relay()

    loads[0].wait()

    @pl.loop(0, dim // 512)
    def _(j):
        col = pl.multiple_of(j * 512, 512)
        put_part(mlp_part, dot(act_ref[...], wd[:, pl.ds(col, 512)]), col)

    gather7.finish()
    scatter5 = Scatter(pos, mlp_part, rp5, wk5, ar5, ss5, rs5)
    scatter5.start()

    loads[1].wait()
    dh1 = full(dh1_buf)
    dh1_out[...] = dh1
    dheads = dot_bt(dh1, wo[...]).astype(BF)
    scatter5.relay()
    keys, values = k_ref[...], v_ref[...]
    cos2, nsin2 = cos_ref[...], -sin_ref[...]
    dkeys = jnp.zeros((seq, head_dim), F32)
    dvalues = jnp.zeros((seq, head_dim), F32)
    for h in range(num_heads):
        cols = slice(h * head_dim, (h + 1) * head_dim)
        dhead = dheads[:, cols]
        probs = probs_ref[h]
        dprobs = dot_bt(dhead, values).astype(BF).astype(F32)
        dvalues += dot_at(probs.astype(BF), dhead)
        inner = jnp.sum(dprobs * probs, axis=-1, keepdims=True)
        dscores = (probs * (dprobs - inner) * (head_dim ** -0.5)).astype(BF)
        dquery = dot(dscores, keys).astype(BF)
        dkeys += dot_at(dscores, q_ref[:, cols])
        dqkv_out[:, cols] = rope(dquery.astype(F32), cos2, nsin2).astype(BF)
    kq = num_heads * head_dim
    dqkv_out[:, kq:kq + head_dim] = rope(dkeys.astype(BF).astype(F32), cos2, nsin2).astype(BF)
    dqkv_out[:, kq + head_dim:] = dvalues.astype(BF)
    for load in loads[2:]:
        load.wait()

    @pl.loop(0, dim // 512)
    def _(j):
        col = pl.multiple_of(j * 512, 512)
        put_part(dn1_part, dot_bt(dqkv_out[...], wqkv[pl.ds(col, 512), :]), col)

    scatter8 = Scatter(pos, dn1_part, rp8, wk8, ar8, ss8, rs8)
    scatter8.start()
    hidden_out[...] = (h1 + scatter5.finish()).astype(BF)
    scatter8.relay()
    normed1, inv1 = norm_stats(x0_ref[...].astype(F32))
    grad_n1 = scatter8.finish().astype(BF).astype(F32)
    grad_x_norm, gain_attn_part = norm_bwd(grad_n1, normed1, inv1, gain_attn[...])
    dx_buf[pos.me] = (dh1_buf[pos.me].astype(F32) + grad_x_norm).astype(BF)
    gain_buf[pos.me, 0:1, :] = gain_attn_part
    gather9 = Gather(pos, dx_buf, gs9, gr9)
    gatherg = Gather(pos, gain_buf, gsg, grg)
    gather9.start()
    gatherg.start()
    gather9.relay()
    gatherg.relay()
    gather9.finish()
    gatherg.finish()
    dx_out[...] = full(dx_buf)
    total = gain_buf[0]
    for i in range(1, CHIPS * CORES):
        total = total + gain_buf[i]
    gains_out[...] = total
    for op in (scatter6, gather7, scatter5, scatter8, gather9, gatherg):
        op.drain()


def backward(dn2_part, act, x0, h1, grad_own, cos2, sin2, gain_attn, gain_mlp, q, k, v, probs, wq, wk, wv, wo, wd):
    num_heads, dim, head_dim = wq.shape
    seq, ffn = act.shape
    rows = seq // (CHIPS * CORES)
    blocks = CHIPS * CORES
    vmem = pl.BlockSpec(memory_space=pltpu.VMEM)
    hbm = pl.BlockSpec(memory_space=pltpu.HBM)
    width = num_heads * head_dim
    sds = jax.ShapeDtypeStruct
    outs = [sds((rows, dim), BF), sds((seq, dim), BF), sds((seq, width + 2 * head_dim), BF), sds((seq, dim), BF),
            sds((2, dim), F32)]
    scratch = [pltpu.VMEM((dim, width + 2 * head_dim), BF), pltpu.VMEM((width, dim), BF), pltpu.VMEM((ffn, dim), BF),
               pltpu.SemaphoreType.DMA((7,)),
               pltpu.VMEM((blocks, rows, dim), BF), pltpu.VMEM((blocks, rows, dim), BF),
               pltpu.VMEM((blocks, 2, dim), F32), pltpu.VMEM((CORES, CHIPS, rows, dim), BF),
               pltpu.VMEM((CORES, CHIPS, rows, dim), BF)]
    scratch += scatter_scratch(rows, dim) * 3 + GATHER_SEMS * 3
    return pl.pallas_call(
        backward_kernel, out_shape=outs, in_specs=[vmem] * 13 + [hbm] * 5, out_specs=[vmem] * len(outs),
        scratch_shapes=scratch,
        compiler_params=pltpu.CompilerParams(collective_id=1, has_side_effects=True, vmem_limit_bytes=40 << 20),
        name='backward',
    )(dn2_part, act, x0, h1, grad_own, cos2, sin2, gain_attn, gain_mlp, q, k, v, probs, wq, wk, wv, wo, wd)


def mlp_grads_kernel(n2, dgate, dup, act, gh, gw_gate, gw_up, gw_down):
    gw_gate[...] = dot_at(n2[...], dgate[...])
    gw_up[...] = dot_at(n2[...], dup[...])
    gw_down[...] = dot_at(act[...], gh[...])


def mlp_grads(n2, dgate, dup, act, gh):
    seq, dim = n2.shape
    ffn = act.shape[1]
    steps = 8
    sds = jax.ShapeDtypeStruct
    return pl.pallas_call(
        mlp_grads_kernel, grid=(steps,),
        out_shape=[sds((dim, ffn), F32), sds((dim, ffn), F32), sds((ffn, dim), F32)],
        in_specs=[pl.BlockSpec((seq, dim // steps), lambda i: (0, i)), pl.BlockSpec((seq, ffn), lambda i: (0, 0)),
                  pl.BlockSpec((seq, ffn), lambda i: (0, 0)), pl.BlockSpec((seq, ffn // steps), lambda i: (0, i)),
                  pl.BlockSpec((seq, dim), lambda i: (0, 0))],
        out_specs=[pl.BlockSpec((dim // steps, ffn), lambda i: (i, 0)), pl.BlockSpec((dim // steps, ffn), lambda i: (i, 0)),
                   pl.BlockSpec((ffn // steps, dim), lambda i: (i, 0))],
        compiler_params=pltpu.CompilerParams(vmem_limit_bytes=40 << 20),
        name='mlp_grads',
    )(n2, dgate, dup, act, gh)


def rest_grads_kernel(n1, dqkv, heads, dh1, ids, dx, gw_query, gw_key, gw_value, gw_out, g_emb):
    num_heads, _, head_dim = gw_query.shape
    width = num_heads * head_dim
    both = dot_at(n1[...], dqkv[...])
    for h in range(num_heads):
        gw_query[h] = both[:, h * head_dim:(h + 1) * head_dim]
    gw_key[...] = both[:, width:width + head_dim]
    gw_value[...] = both[:, width + head_dim:]
    gw_out[...] = dot_at(heads[...], dh1[...])
    rows, seq = g_emb.shape[0], dx.shape[0]
    row = lax.broadcasted_iota(jnp.int32, (rows, seq), 0) + pl.program_id(0) * rows
    pick = jnp.where(row == ids[...], 1.0, 0.0).astype(BF)
    g_emb[...] = dot(pick, dx[...])


def rest_grads(n1, dqkv, heads, dh1, ids, dx, rows_local, head_dim):
    seq, dim = n1.shape
    width = heads.shape[1]
    num_heads = width // head_dim
    sds = jax.ShapeDtypeStruct
    return pl.pallas_call(
        rest_grads_kernel, grid=(8,),
        out_shape=[sds((num_heads, dim, head_dim), F32), sds((dim, head_dim), F32), sds((dim, head_dim), F32),
                   sds((width, dim), F32), sds((rows_local, dim), F32)],
        in_specs=[pl.BlockSpec((seq, dim // 8), lambda i: (0, i)), pl.BlockSpec((seq, dqkv.shape[1]), lambda i: (0, 0)),
                  pl.BlockSpec((seq, width), lambda i: (0, 0)), pl.BlockSpec((seq, dim // 8), lambda i: (0, i)),
                  pl.BlockSpec((1, seq), lambda i: (0, 0)), pl.BlockSpec((seq, dim), lambda i: (0, 0))],
        out_specs=[pl.BlockSpec((num_heads, dim // 8, head_dim), lambda i: (0, i, 0)),
                   pl.BlockSpec((dim // 8, head_dim), lambda i: (i, 0)), pl.BlockSpec((dim // 8, head_dim), lambda i: (i, 0)),
                   pl.BlockSpec((width, dim // 8), lambda i: (0, i)), pl.BlockSpec((rows_local // 8, dim), lambda i: (i, 0))],
        compiler_params=pltpu.CompilerParams(vmem_limit_bytes=40 << 20),
        name='rest_grads',
    )(n1, dqkv, heads, dh1, ids, dx)


def solution(mesh):
    if mesh.shape['tp'] != CHIPS * CORES:
        raise ValueError('tp size')
    in_specs = (P('dp', None), P('dp', None), P('tp', None), P(None), P(None),
                P(None, 'tp', None), P(None, 'tp', None), P(None, 'tp', None), P('tp', None, None),
                P(None, 'tp'), P(None, 'tp'), P('tp', None), P('dp', 'tp', None))
    out_specs = (P('dp', 'tp', None), P(('dp', 'tp'), None),
                 P('dp', 'tp', None), P('dp', 'tp', None), P('dp', 'tp', None), P(('dp', 'tp'), None, None),
                 P('dp', 'tp'), P('dp', 'tp'), P(('dp', 'tp'), None), P('dp'), P('dp'))

    def device_fn(tokens, positions, emb_shard, gain_attn, gain_mlp, w_query, w_key, w_value, w_out, w_gate, w_up, w_down, grad_hidden):
        rows_local, dim = emb_shard.shape
        seq = tokens.shape[1]
        rows = seq // (CHIPS * CORES)
        num_heads, head_dim = w_query.shape[1], w_query.shape[2]
        half_dim = head_dim // 2
        inv_freq = ROPE_THETA ** (-jnp.arange(half_dim, dtype=F32) * (2.0 / head_dim))
        angles = positions[0].astype(F32)[:, None] * inv_freq
        cos_tab, sin_tab = jnp.cos(angles), jnp.sin(angles)
        cos2 = jnp.concatenate([cos_tab, cos_tab], axis=1)
        sin2 = jnp.concatenate([-sin_tab, sin_tab], axis=1)
        wq = jnp.transpose(w_query, (1, 0, 2))
        wk, wv = w_key.reshape(dim, head_dim), w_value.reshape(dim, head_dim)
        wo = w_out.reshape(num_heads * head_dim, dim)
        ga, gm = gain_attn[None, :], gain_mlp[None, :]
        grad_own = grad_hidden[0]

        emb_part = lookup(tokens[0], emb_shard).reshape(CORES, CHIPS, rows, dim)
        (x0, h1, n1, n2, gh, heads, q, k, v, probs, act, dgate, dup, dn2_part) = forward(
            emb_part, cos2, sin2, ga, gm, grad_own, wq, wk, wv, wo, w_gate, w_up, w_down)
        gw_gate, gw_up, gw_down = mlp_grads(n2, dgate, dup, act, gh)
        hidden, dh1, dqkv, dx, gains = backward(
            dn2_part, act, x0, h1, grad_own, cos2, sin2, ga, gm, q, k, v, probs, wq, wk, wv, wo, w_down)
        local_ids = tokens - lax.axis_index('tp') * rows_local
        gw_query, gw_key, gw_value, gw_out, g_emb = rest_grads(n1, dqkv, heads, dh1, local_ids, dx, rows_local, head_dim)
        return (hidden[None], g_emb, jnp.transpose(gw_query, (1, 0, 2)), gw_key.reshape(dim, 1, head_dim),
                gw_value.reshape(dim, 1, head_dim), gw_out.reshape(num_heads, head_dim, dim),
                gw_gate, gw_up, gw_down, gains[0], gains[1])

    return jax.shard_map(device_fn, mesh=mesh, in_specs=in_specs, out_specs=out_specs, check_vma=False)
```

```python
import jax
import jax.numpy as jnp
import numpy as np
from jax import lax
from jax.experimental import pallas as pl
from jax.experimental.pallas import tpu as pltpu
from jax.sharding import PartitionSpec as P

ROPE_THETA = 1000000.0
RMS_EPS = 1e-5
BF = jnp.bfloat16
F32 = jnp.float32
VMEM_FULL = 67043328
CHIPS = 4
CORES = 2


def dot(a, b):
    return lax.dot_general(a, b, (((1,), (0,)), ((), ())), preferred_element_type=F32)


def dot_bt(a, b):
    return lax.dot_general(a, b, (((1,), (1,)), ((), ())), preferred_element_type=F32)


def dot_at(a, b):
    return lax.dot_general(a, b, (((0,), (0,)), ((), ())), preferred_element_type=F32)


class Place:
    def __init__(self):
        me = lax.axis_index('tp')
        self.chip, self.core = me // CORES, me % CORES
        self.right_chip = (self.chip + 1) % CHIPS
        self.left_chip = (self.chip + CHIPS - 1) % CHIPS
        self.far_chip = (self.chip + 2) % CHIPS
        self.me = me
        self.other = 1 - self.core
        self.partner = self.chip * CORES + self.other
        self.right = self.right_chip * CORES + self.core
        self.left = self.left_chip * CORES + self.core
        self.far = self.far_chip * CORES + self.core


def remote(src, dst, send, recv, device):
    return pltpu.make_async_remote_copy(src_ref=src, dst_ref=dst, send_sem=send, recv_sem=recv,
                                        device_id={'tp': device}, device_id_type=pl.DeviceIdType.MESH)


def entry_barrier(pos):
    barrier = pltpu.get_barrier_semaphore()
    for device in (pos.left, pos.right, pos.partner):
        pl.semaphore_signal(barrier, inc=1, device_id={'tp': device}, device_id_type=pl.DeviceIdType.MESH)
    pl.semaphore_wait(barrier, 3)


class Gather:
    def __init__(self, pos, buf, send, recv):
        self.pos, self.buf = pos, buf
        half = buf.shape[-1] // 2
        p = pos
        other = p.other - p.core

        def piece(slot, part):
            if part == 2:
                return buf.at[slot]
            return buf.at[slot, :, pl.ds(part * half, half)]

        def copy(index, slot, part, device):
            ref = piece(slot, part)
            return remote(ref, ref, send.at[index], recv.at[index], device)

        plan = {
            0: ((p.me, 0, p.right), (p.left, 0)), 1: ((p.me, 1, p.left), (p.right, 1)),
            2: ((p.me, 2, p.partner), (p.partner, 2)),
            3: ((p.me, 1, p.right), (p.left, 1)), 4: ((p.me, 0, p.left), (p.right, 0)),
            5: ((p.left, 0, p.right), (p.far, 0)), 6: ((p.right, 1, p.left), (p.far, 1)),
            7: ((p.left, 0, p.partner), (p.left + other, 0)), 8: ((p.right, 1, p.partner), (p.right + other, 1)),
            9: ((p.left, 1, p.partner), (p.left + other, 1)), 10: ((p.right, 0, p.partner), (p.right + other, 0)),
            11: ((p.far, 0, p.partner), (p.far + other, 0)), 12: ((p.far, 1, p.partner), (p.far + other, 1)),
        }
        self.out = {i: copy(i, *s) for i, (s, _) in plan.items()}
        self.into = {i: copy(i, slot, part, p.partner) for i, (_, (slot, part)) in plan.items()}

    def start(self):
        for i in (0, 1, 2, 3, 4):
            self.out[i].start()

    def relay(self):
        for i, onward in ((0, (5, 7)), (1, (6, 8)), (3, (9,)), (4, (10,))):
            self.into[i].wait_recv()
            for j in onward:
                self.out[j].start()

    def finish(self):
        for i, j in ((5, 11), (6, 12)):
            self.into[i].wait_recv()
            self.out[j].start()
        for i in (2, 7, 8, 9, 10, 11, 12):
            self.into[i].wait_recv()

    def drain(self):
        for i in range(13):
            self.out[i].wait_send()

    def run(self):
        self.start()
        self.relay()
        self.finish()
        self.drain()


class Scatter:
    def __init__(self, pos, part, from_partner, work, arrive, send, recv):
        p = pos
        self.pos, self.part, self.from_partner, self.work, self.arrive = p, part, from_partner, work, arrive
        self.half = work.shape[-1]
        self.chips = (p.far_chip, p.right_chip, p.left_chip, p.chip)
        self.inner = [remote(part.at[p.other, y], from_partner.at[y], send.at[k], recv.at[k], p.partner)
                      for k, y in enumerate(self.chips)]
        self.outer = [remote(work.at[k], arrive.at[k], send.at[4 + k], recv.at[4 + k], p.right if k % 2 == 0 else p.left)
                      for k in range(6)]

    def pair(self, k, part):
        cols = pl.ds(part * self.half, self.half)
        y = self.chips[k]
        return self.part[self.pos.core, y, :, cols].astype(F32) + self.from_partner[y, :, cols].astype(F32)

    def send_sum(self, k, value):
        self.work[k] = value.astype(BF)
        self.outer[k].start()

    def start(self):
        for copy in self.inner:
            copy.start()

    def relay(self):
        self.inner[0].wait_recv()
        self.send_sum(0, self.pair(0, 0))
        self.send_sum(1, self.pair(0, 1))
        self.inner[1].wait_recv()
        self.send_sum(2, self.pair(1, 1))
        self.inner[2].wait_recv()
        self.send_sum(3, self.pair(2, 0))
        self.outer[0].wait_recv()
        self.send_sum(4, self.pair(1, 0) + self.arrive[0].astype(F32))
        self.outer[1].wait_recv()
        self.send_sum(5, self.pair(2, 1) + self.arrive[1].astype(F32))

    def finish(self):
        self.inner[3].wait_recv()
        for k in (2, 3, 4, 5):
            self.outer[k].wait_recv()
        low = self.pair(3, 0) + self.arrive[3].astype(F32) + self.arrive[4].astype(F32)
        high = self.pair(3, 1) + self.arrive[2].astype(F32) + self.arrive[5].astype(F32)
        return jnp.concatenate([low, high], axis=-1)

    def drain(self):
        for copy in self.inner + self.outer:
            copy.wait_send()

    def run(self):
        self.start()
        self.relay()
        total = self.finish()
        self.drain()
        return total


GATHER_SEMS = [pltpu.SemaphoreType.DMA((13,)), pltpu.SemaphoreType.DMA((13,))]
SCATTER_SEMS = [pltpu.SemaphoreType.DMA((10,)), pltpu.SemaphoreType.DMA((10,))]


def scatter_scratch(rows, dim):
    return [pltpu.VMEM((CHIPS, rows, dim), BF), pltpu.VMEM((6, rows, dim // 2), BF),
            pltpu.VMEM((6, rows, dim // 2), BF)] + SCATTER_SEMS


def put_part(part, value, col):
    rows, width = part.shape[2], value.shape[1]
    for b in range(CHIPS * CORES):
        part[b % CORES, b // CORES, :, pl.ds(col, width)] = value[b * rows:(b + 1) * rows].astype(BF)


def norm_stats(hidden_f):
    inv_rms = lax.rsqrt(jnp.mean(hidden_f * hidden_f, axis=-1, keepdims=True) + RMS_EPS)
    return hidden_f * inv_rms, inv_rms


def norm_bwd(grad_f, normed, inv_rms, gain):
    gain_part = jnp.sum(grad_f * normed, axis=0, keepdims=True)
    scaled = grad_f * gain
    return inv_rms * (scaled - normed * jnp.mean(scaled * normed, axis=-1, keepdims=True)), gain_part


def rope(values, cos2, sin2):
    return values * cos2 + pltpu.roll(values, values.shape[-1] // 2, axis=1) * sin2


def full(buf):
    blocks, rows, dim = buf.shape
    return buf[...].reshape(blocks * rows, dim)


def lookup_kernel(ids_smem, ids_ref, pos_ref, freq_ref, emb_hbm, out_ref, cos_ref, sin_ref, groups, sem):
    count, _, dim = groups.shape
    rows_local = emb_hbm.shape[0]
    base = lax.axis_index('tp') * rows_local

    @pl.loop(0, count)
    def _(i):
        local = jnp.clip(ids_smem[0, i] - base, 0, rows_local - 1)
        start = pl.multiple_of((local // 8) * 8, 8)
        pltpu.make_async_copy(emb_hbm.at[pl.ds(start, 8)], groups.at[i], sem).start()

    head_dim = cos_ref.shape[1]
    angles = jnp.transpose(freq_ref[...] * pos_ref[...].astype(F32))
    cos_ref[...] = jnp.cos(angles)
    lane = lax.broadcasted_iota(jnp.int32, angles.shape, 1)
    sin = jnp.sin(angles)
    sin_ref[...] = jnp.where(lane < head_dim // 2, -sin, sin)

    local = ids_ref[...] - base
    owned = (local >= 0) & (local < rows_local)
    place = jnp.where(owned, lax.broadcasted_iota(jnp.int32, local.shape, 1) * 8 + local % 8, -1)
    pick = jnp.where(lax.broadcasted_iota(jnp.int32, (count * 8, count), 0) == place, 1.0, 0.0).astype(BF)
    step = 512
    pltpu.make_async_copy(groups, groups, sem).wait()

    @pl.loop(0, dim // step)
    def _(j):
        col = pl.multiple_of(j * step, step)
        block = groups[:, :, pl.ds(col, step)].reshape(count * 8, step)
        put_part(out_ref, dot_at(pick, block), col)


def lookup(tokens, positions, emb, head_dim):
    dim = emb.shape[1]
    seq = tokens.shape[1]
    half = head_dim // 2
    freq = np.float32(ROPE_THETA) ** (-np.arange(half, dtype=np.float32) * np.float32(2.0 / head_dim))
    freq = jnp.asarray(np.concatenate([freq, freq])[:, None], F32)
    vmem = pl.BlockSpec(memory_space=pltpu.VMEM)
    sds = jax.ShapeDtypeStruct
    return pl.pallas_call(
        lookup_kernel,
        out_shape=[sds((CORES, CHIPS, seq // (CHIPS * CORES), dim), BF), sds((seq, head_dim), F32), sds((seq, head_dim), F32)],
        grid_spec=pltpu.PrefetchScalarGridSpec(
            num_scalar_prefetch=1, grid=(),
            in_specs=[vmem, vmem, vmem, pl.BlockSpec(memory_space=pltpu.HBM)], out_specs=[vmem] * 3,
            scratch_shapes=[pltpu.VMEM((seq, 8, dim), BF), pltpu.SemaphoreType.DMA]),
        compiler_params=pltpu.CompilerParams(vmem_limit_bytes=VMEM_FULL),
        name='lookup',
    )(tokens, tokens, positions, freq, emb)


def layer_kernel(emb_hbm, cos_hbm, sin_hbm, gain_attn, gain_mlp, grad_own, wq_hbm, wk_hbm, wv_hbm, wo_hbm, wg_hbm, wu_hbm, wd_hbm,
                 hidden_out, gains_out, n1_out, n2_out, gh_out, dh1_out, dx_out, heads_out, act_out, dgate_out, dup_out, dqkv_out,
                 emb_part, cos_ref, sin_ref, wqkv, wo, wg, wu, wd, wsem, osem, n1_buf, n2_buf, gh_buf, dh1_buf, dx_buf, gain_buf,
                 attn_part, dn2_part, mlp_part, dn1_part, heads_buf, gact, act_buf, dgate_buf, dup_buf, dqkv_buf, q_buf, probs_buf,
                 *comm):
    pos = Place()
    num_heads, dim, head_dim = wq_hbm.shape
    blocks, rows, _ = n1_buf.shape
    seq, ffn = blocks * rows, wg.shape[1]
    scatters, gathers = comm[:25], comm[25:]
    kq = num_heads * head_dim
    pairs = [(emb_hbm, emb_part), (cos_hbm, cos_ref), (sin_hbm, sin_ref)]
    pairs += [(wq_hbm.at[h], wqkv.at[:, pl.ds(h * head_dim, head_dim)]) for h in range(num_heads)]
    pairs += [(wk_hbm, wqkv.at[:, pl.ds(kq, head_dim)]), (wv_hbm, wqkv.at[:, pl.ds(kq + head_dim, head_dim)])]
    pairs += [(wo_hbm, wo), (wd_hbm, wd), (wg_hbm, wg), (wu_hbm, wu)]
    loads = [pltpu.make_async_copy(src, dst, wsem.at[k]) for k, (src, dst) in enumerate(pairs)]
    for load in loads:
        load.start()
    stores = []

    def store(src, dst):
        stores.append(pltpu.make_async_copy(src, dst, osem.at[len(stores)]))
        stores[-1].start()

    with jax.named_scope('barrier'):
        entry_barrier(pos)
        loads[0].wait()

    with jax.named_scope('rs1'):
        scatter1 = Scatter(pos, emb_part, *scatters[0:5])
        x0 = scatter1.run()
    with jax.named_scope('norm1'):
        normed1, inv1 = norm_stats(x0)
        n1_buf[pos.me] = (normed1 * gain_attn[...]).astype(BF)
    with jax.named_scope('ag1'):
        gather1 = Gather(pos, n1_buf, *gathers[0:2])
        gather1.run()
    store(n1_buf, n1_out)

    gh_buf[pos.me] = grad_own[...]
    gather0 = Gather(pos, gh_buf, *gathers[2:4])
    gather0.start()

    with jax.named_scope('wait_qkv'):
        for load in loads[1:8]:
            load.wait()
    with jax.named_scope('qkv'):
        qkv = dot(full(n1_buf), wqkv[...])
    with jax.named_scope('ag0_relay'):
        gather0.relay()
    with jax.named_scope('attention'):
        cos2, sin2 = cos_ref[...], sin_ref[...]
        keys = rope(qkv[:, kq:kq + head_dim], cos2, sin2).astype(BF)
        values = qkv[:, kq + head_dim:].astype(BF)
        causal = lax.broadcasted_iota(jnp.int32, (seq, seq), 0) >= lax.broadcasted_iota(jnp.int32, (seq, seq), 1)
        for h in range(num_heads):
            cols = slice(h * head_dim, (h + 1) * head_dim)
            query = rope(qkv[:, cols], cos2, sin2).astype(BF)
            q_buf[:, cols] = query
            scores = jnp.where(causal, dot_bt(query, keys) * (head_dim ** -0.5), -1e30)
            expd = jnp.exp(scores - jnp.max(scores, axis=-1, keepdims=True))
            probs = expd / jnp.sum(expd, axis=-1, keepdims=True)
            probs_buf[h] = probs
            heads_buf[:, cols] = dot(probs.astype(BF), values).astype(BF)
    store(heads_buf, heads_out)
    with jax.named_scope('w_out'):
        loads[8].wait()

        @pl.loop(0, dim // 512)
        def _(j):
            cols = pl.ds(pl.multiple_of(j * 512, 512), 512)
            put_part(attn_part, dot(heads_buf[...], wo[:, cols]), cols.start)

    with jax.named_scope('rs3_a'):
        scatter3 = Scatter(pos, attn_part, *scatters[5:10])
        scatter3.start()
        gather0.finish()
        scatter3.relay()
    store(gh_buf, gh_out)

    with jax.named_scope('grad_act'):
        loads[9].wait()

        @pl.loop(0, ffn // 256)
        def _(j):
            cols = pl.ds(pl.multiple_of(j * 256, 256), 256)
            gact[:, cols] = dot_bt(full(gh_buf), wd[cols, :]).astype(BF)

    with jax.named_scope('rs3_b'):
        h1_bf = (x0 + scatter3.finish()).astype(BF)
    with jax.named_scope('norm2'):
        h1 = h1_bf.astype(F32)
        normed2, inv2 = norm_stats(h1)
        n2_buf[pos.me] = (normed2 * gain_mlp[...]).astype(BF)
    with jax.named_scope('ag4'):
        gather4 = Gather(pos, n2_buf, *gathers[4:6])
        gather4.run()
        loads[10].wait()
        loads[11].wait()
    store(n2_buf, n2_out)

    with jax.named_scope('gate_up'):
        @pl.loop(0, ffn // 256)
        def _(j):
            cols = pl.ds(pl.multiple_of(j * 256, 256), 256)
            n2 = full(n2_buf)
            gate_pre = dot(n2, wg[:, cols])
            up_pre = dot(n2, wu[:, cols])
            sig = jax.nn.sigmoid(gate_pre)
            gate_act = gate_pre * sig
            act_buf[:, cols] = (gate_act * up_pre).astype(BF)
            grad_act = gact[:, cols].astype(F32)
            dup_buf[:, cols] = (grad_act * gate_act).astype(BF)
            dgate_buf[:, cols] = (grad_act * up_pre * sig * (1.0 + gate_pre * (1.0 - sig))).astype(BF)

    store(act_buf, act_out)
    store(dgate_buf, dgate_out)
    store(dup_buf, dup_out)
    with jax.named_scope('dn2'):
        @pl.loop(0, dim // 512)
        def _(j):
            col = pl.multiple_of(j * 512, 512)
            put_part(dn2_part, dot_bt(dgate_buf[...], wg[pl.ds(col, 512), :]) + dot_bt(dup_buf[...], wu[pl.ds(col, 512), :]), col)

    with jax.named_scope('rs6_a'):
        scatter6 = Scatter(pos, dn2_part, *scatters[10:15])
        scatter6.start()
        scatter6.relay()
    with jax.named_scope('rs6_b'):
        grad_n2 = scatter6.finish().astype(BF).astype(F32)
    with jax.named_scope('norm2_bwd'):
        grad_h1_norm, gain_mlp_part = norm_bwd(grad_n2, normed2, inv2, gain_mlp[...])
        grad_h1 = (grad_own[...].astype(F32) + grad_h1_norm).astype(BF)
        dh1_buf[pos.me] = grad_h1
        gain_buf[pos.me, 1:2, :] = gain_mlp_part
    with jax.named_scope('ag7_a'):
        gather7 = Gather(pos, dh1_buf, *gathers[6:8])
        gather7.start()
        gather7.relay()

    with jax.named_scope('w_down'):
        @pl.loop(0, dim // 512)
        def _(j):
            col = pl.multiple_of(j * 512, 512)
            put_part(mlp_part, dot(act_buf[...], wd[:, pl.ds(col, 512)]), col)

    with jax.named_scope('ag7_b'):
        gather7.finish()
    store(dh1_buf, dh1_out)
    scatter5 = Scatter(pos, mlp_part, *scatters[15:20])
    scatter5.start()

    with jax.named_scope('dheads'):
        dheads = dot_bt(full(dh1_buf), wo[...]).astype(BF)
    with jax.named_scope('rs5_relay'):
        scatter5.relay()
    with jax.named_scope('attention_bwd'):
        nsin2 = -sin2
        dkeys = jnp.zeros((seq, head_dim), F32)
        dvalues = jnp.zeros((seq, head_dim), F32)
        for h in range(num_heads):
            cols = slice(h * head_dim, (h + 1) * head_dim)
            dhead = dheads[:, cols]
            probs = probs_buf[h]
            dprobs = dot_bt(dhead, values).astype(BF).astype(F32)
            dvalues += dot_at(probs.astype(BF), dhead)
            inner = jnp.sum(dprobs * probs, axis=-1, keepdims=True)
            dscores = (probs * (dprobs - inner) * (head_dim ** -0.5)).astype(BF)
            dquery = dot(dscores, keys).astype(BF)
            dkeys += dot_at(dscores, q_buf[:, cols])
            dqkv_buf[:, cols] = rope(dquery.astype(F32), cos2, nsin2).astype(BF)
        dqkv_buf[:, kq:kq + head_dim] = rope(dkeys.astype(BF).astype(F32), cos2, nsin2).astype(BF)
        dqkv_buf[:, kq + head_dim:] = dvalues.astype(BF)
    store(dqkv_buf, dqkv_out)

    with jax.named_scope('dn1'):
        @pl.loop(0, dim // 512)
        def _(j):
            col = pl.multiple_of(j * 512, 512)
            put_part(dn1_part, dot_bt(dqkv_buf[...], wqkv[pl.ds(col, 512), :]), col)

    with jax.named_scope('rs8'):
        scatter8 = Scatter(pos, dn1_part, *scatters[20:25])
        scatter8.start()
        hidden_out[...] = (h1 + scatter5.finish()).astype(BF)
        scatter8.relay()
        grad_n1 = scatter8.finish().astype(BF).astype(F32)
    with jax.named_scope('norm1_bwd'):
        grad_x_norm, gain_attn_part = norm_bwd(grad_n1, normed1, inv1, gain_attn[...])
        dx_buf[pos.me] = (grad_h1.astype(F32) + grad_x_norm).astype(BF)
        gain_buf[pos.me, 0:1, :] = gain_attn_part
    with jax.named_scope('ag9'):
        gather9 = Gather(pos, dx_buf, *gathers[8:10])
        gatherg = Gather(pos, gain_buf, *gathers[10:12])
        gather9.start()
        gatherg.start()
        gather9.relay()
        gatherg.relay()
        gather9.finish()
        store(dx_buf, dx_out)
        gatherg.finish()
    with jax.named_scope('tail'):
        total = gain_buf[0]
        for i in range(1, blocks):
            total = total + gain_buf[i]
        gains_out[...] = total
        for op in (gather0, scatter3, scatter6, gather7, scatter5, scatter8, gather9, gatherg):
            op.drain()
        for copy in stores:
            copy.wait()


def layer(emb_part, cos2, sin2, gain_attn, gain_mlp, grad_own, wq, wk, wv, wo, wg, wu, wd):
    num_heads, dim, head_dim = wq.shape
    blocks = CHIPS * CORES
    seq, ffn = cos2.shape[0], wg.shape[1]
    rows = seq // blocks
    vmem = pl.BlockSpec(memory_space=pltpu.VMEM)
    hbm = pl.BlockSpec(memory_space=pltpu.HBM)
    width = num_heads * head_dim
    wide = width + 2 * head_dim
    sds = jax.ShapeDtypeStruct
    outs = [sds((rows, dim), BF), sds((2, dim), F32)] + [sds((blocks, rows, dim), BF)] * 5
    outs += [sds((seq, width), BF)] + [sds((seq, ffn), BF)] * 3 + [sds((seq, wide), BF)]
    part = pltpu.VMEM((CORES, CHIPS, rows, dim), BF)
    gathered = pltpu.VMEM((blocks, rows, dim), BF)
    table = pltpu.VMEM((seq, head_dim), F32)
    scratch = [part, table, table, pltpu.VMEM((dim, wide), BF), pltpu.VMEM((width, dim), BF), pltpu.VMEM((dim, ffn), BF),
               pltpu.VMEM((dim, ffn), BF), pltpu.VMEM((ffn, dim), BF), pltpu.SemaphoreType.DMA((12,)), pltpu.SemaphoreType.DMA((10,))]
    scratch += [gathered] * 5 + [pltpu.VMEM((blocks, 2, dim), F32)] + [part] * 4 + [pltpu.VMEM((seq, width), BF)]
    scratch += [pltpu.VMEM((seq, ffn), BF)] * 4 + [pltpu.VMEM((seq, wide), BF), pltpu.VMEM((seq, width), BF),
                                                   pltpu.VMEM((num_heads, seq, seq), F32)]
    scratch += scatter_scratch(rows, dim) * 5 + GATHER_SEMS * 6
    return pl.pallas_call(
        layer_kernel, out_shape=outs, in_specs=[hbm] * 3 + [vmem] * 3 + [hbm] * 7, out_specs=[vmem] * 2 + [hbm] * 10,
        scratch_shapes=scratch,
        compiler_params=pltpu.CompilerParams(collective_id=0, has_side_effects=True, vmem_limit_bytes=VMEM_FULL),
        name='layer',
    )(emb_part, cos2, sin2, gain_attn, gain_mlp, grad_own, wq, wk, wv, wo, wg, wu, wd)


def mlp_grads_kernel(n2, dgate, dup, act, gh, gw_gate, gw_up, gw_down):
    gw_gate[...] = dot_at(n2[...], dgate[...])
    gw_up[...] = dot_at(n2[...], dup[...])
    gw_down[...] = dot_at(act[...], gh[...])


def mlp_grads(n2, dgate, dup, act, gh):
    seq, dim = n2.shape
    ffn = act.shape[1]
    steps = 8
    sds = jax.ShapeDtypeStruct
    return pl.pallas_call(
        mlp_grads_kernel, grid=(steps,),
        out_shape=[sds((dim, ffn), F32), sds((dim, ffn), F32), sds((ffn, dim), F32)],
        in_specs=[pl.BlockSpec((seq, dim // steps), lambda i: (0, i)), pl.BlockSpec((seq, ffn), lambda i: (0, 0)),
                  pl.BlockSpec((seq, ffn), lambda i: (0, 0)), pl.BlockSpec((seq, ffn // steps), lambda i: (0, i)),
                  pl.BlockSpec((seq, dim), lambda i: (0, 0))],
        out_specs=[pl.BlockSpec((dim // steps, ffn), lambda i: (i, 0)), pl.BlockSpec((dim // steps, ffn), lambda i: (i, 0)),
                   pl.BlockSpec((ffn // steps, dim), lambda i: (i, 0))],
        compiler_params=pltpu.CompilerParams(vmem_limit_bytes=VMEM_FULL),
        name='mlp_grads',
    )(n2, dgate, dup, act, gh)


def rest_grads_kernel(n1, dqkv, heads, dh1, tokens, dx, hidden_in, gains_in,
                      gw_query, gw_key, gw_value, gw_out, g_emb, hidden, g_attn, g_mlp):
    num_heads, _, head_dim = gw_query.shape
    width = num_heads * head_dim
    both = dot_at(n1[...], dqkv[...])
    for h in range(num_heads):
        gw_query[h] = both[:, h * head_dim:(h + 1) * head_dim]
    gw_key[...] = both[:, width:width + head_dim]
    gw_value[...] = both[:, width + head_dim:]
    gw_out[...] = dot_at(heads[...], dh1[...])
    rows, seq = g_emb.shape[0], dx.shape[0]
    steps = pl.num_programs(0)
    first = lax.axis_index('tp') * (rows * steps) + pl.program_id(0) * rows
    row = lax.broadcasted_iota(jnp.int32, (rows, seq), 0) + first
    pick = jnp.where(row == tokens[...], 1.0, 0.0).astype(BF)
    g_emb[...] = dot(pick, dx[...])

    @pl.when(pl.program_id(0) == 0)
    def _():
        hidden[...] = hidden_in[...]
        g_attn[...] = gains_in[0:1, :]
        g_mlp[...] = gains_in[1:2, :]


def rest_grads(n1, dqkv, heads, dh1, tokens, dx, hidden, gains, rows_local, head_dim):
    seq, dim = n1.shape
    width = heads.shape[1]
    num_heads = width // head_dim
    steps = 8
    sds = jax.ShapeDtypeStruct

    def whole(shape):
        return pl.BlockSpec(shape, lambda i: (0,) * len(shape))

    return pl.pallas_call(
        rest_grads_kernel, grid=(steps,),
        out_shape=[sds((num_heads, dim, head_dim), F32), sds((dim, head_dim), F32), sds((dim, head_dim), F32),
                   sds((width, dim), F32), sds((rows_local, dim), F32), sds(hidden.shape, BF), sds((1, dim), F32), sds((1, dim), F32)],
        in_specs=[pl.BlockSpec((seq, dim // steps), lambda i: (0, i)), whole(dqkv.shape), whole(heads.shape),
                  pl.BlockSpec((seq, dim // steps), lambda i: (0, i)), whole(tokens.shape), whole(dx.shape),
                  whole(hidden.shape), whole(gains.shape)],
        out_specs=[pl.BlockSpec((num_heads, dim // steps, head_dim), lambda i: (0, i, 0)),
                   pl.BlockSpec((dim // steps, head_dim), lambda i: (i, 0)), pl.BlockSpec((dim // steps, head_dim), lambda i: (i, 0)),
                   pl.BlockSpec((width, dim // steps), lambda i: (0, i)), pl.BlockSpec((rows_local // steps, dim), lambda i: (i, 0)),
                   whole(hidden.shape), whole((1, dim)), whole((1, dim))],
        compiler_params=pltpu.CompilerParams(vmem_limit_bytes=VMEM_FULL),
        name='rest_grads',
    )(n1, dqkv, heads, dh1, tokens, dx, hidden, gains)


def solution(mesh):
    if mesh.shape['tp'] != CHIPS * CORES:
        raise ValueError('tp size')
    in_specs = (P('dp', None), P('dp', None), P('tp', None), P(None), P(None),
                P(None, 'tp', None), P(None, 'tp', None), P(None, 'tp', None), P('tp', None, None),
                P(None, 'tp'), P(None, 'tp'), P('tp', None), P('dp', 'tp', None))
    out_specs = (P('dp', 'tp', None), P(('dp', 'tp'), None),
                 P('dp', 'tp', None), P('dp', 'tp', None), P('dp', 'tp', None), P(('dp', 'tp'), None, None),
                 P('dp', 'tp'), P('dp', 'tp'), P(('dp', 'tp'), None), P('dp'), P('dp'))

    def device_fn(tokens, positions, emb_shard, gain_attn, gain_mlp, w_query, w_key, w_value, w_out, w_gate, w_up, w_down, grad_hidden):
        rows_local, dim = emb_shard.shape
        seq = tokens.shape[1]
        num_heads, head_dim = w_query.shape[1], w_query.shape[2]
        wq = jnp.transpose(w_query, (1, 0, 2))
        wk, wv = w_key.reshape(dim, head_dim), w_value.reshape(dim, head_dim)
        wo = w_out.reshape(num_heads * head_dim, dim)

        emb_part, cos2, sin2 = lookup(tokens, positions, emb_shard, head_dim)
        hidden, gains, n1, n2, gh, dh1, dx, heads, act, dgate, dup, dqkv = layer(
            emb_part, cos2, sin2, gain_attn[None, :], gain_mlp[None, :], grad_hidden[0], wq, wk, wv, wo, w_gate, w_up, w_down)
        n1, n2, gh, dh1, dx = (x.reshape(seq, dim) for x in (n1, n2, gh, dh1, dx))
        gw_gate, gw_up, gw_down = mlp_grads(n2, dgate, dup, act, gh)
        gw_query, gw_key, gw_value, gw_out, g_emb, hidden, g_attn, g_mlp = rest_grads(
            n1, dqkv, heads, dh1, tokens, dx, hidden, gains, rows_local, head_dim)
        return (hidden[None], g_emb, jnp.transpose(gw_query, (1, 0, 2)), gw_key.reshape(dim, 1, head_dim),
                gw_value.reshape(dim, 1, head_dim), gw_out.reshape(num_heads, head_dim, dim),
                gw_gate, gw_up, gw_down, g_attn[0], g_mlp[0])

    return jax.shard_map(device_fn, mesh=mesh, in_specs=in_specs, out_specs=out_specs, check_vma=False)
```

```python
import jax
import jax.numpy as jnp
import numpy as np
from jax import lax
from jax.experimental import pallas as pl
from jax.experimental.pallas import tpu as pltpu
from jax.sharding import PartitionSpec as P

ROPE_THETA = 1000000.0
RMS_EPS = 1e-5
BF = jnp.bfloat16
F32 = jnp.float32
VMEM_FULL = 67043328
CHIPS = 4
CORES = 2


def dot(a, b):
    return lax.dot_general(a, b, (((1,), (0,)), ((), ())), preferred_element_type=F32)


def dot_bt(a, b):
    return lax.dot_general(a, b, (((1,), (1,)), ((), ())), preferred_element_type=F32)


def dot_at(a, b):
    return lax.dot_general(a, b, (((0,), (0,)), ((), ())), preferred_element_type=F32)


class Place:
    def __init__(self):
        me = lax.axis_index('tp')
        self.chip, self.core = me // CORES, me % CORES
        self.right_chip = (self.chip + 1) % CHIPS
        self.left_chip = (self.chip + CHIPS - 1) % CHIPS
        self.far_chip = (self.chip + 2) % CHIPS
        self.me = me
        self.other = 1 - self.core
        self.partner = self.chip * CORES + self.other
        self.right = self.right_chip * CORES + self.core
        self.left = self.left_chip * CORES + self.core
        self.far = self.far_chip * CORES + self.core


def remote(src, dst, send, recv, device):
    return pltpu.make_async_remote_copy(src_ref=src, dst_ref=dst, send_sem=send, recv_sem=recv,
                                        device_id={'tp': device}, device_id_type=pl.DeviceIdType.MESH)


def entry_barrier(pos):
    barrier = pltpu.get_barrier_semaphore()
    for device in (pos.left, pos.right, pos.partner):
        pl.semaphore_signal(barrier, inc=1, device_id={'tp': device}, device_id_type=pl.DeviceIdType.MESH)
    pl.semaphore_wait(barrier, 3)


class Gather:
    def __init__(self, pos, buf, send, recv):
        self.pos, self.buf = pos, buf
        half = buf.shape[-1] // 2
        p = pos
        other = p.other - p.core

        def piece(slot, part):
            if part == 2:
                return buf.at[slot]
            return buf.at[slot, :, pl.ds(part * half, half)]

        def copy(index, slot, part, device):
            ref = piece(slot, part)
            return remote(ref, ref, send.at[index], recv.at[index], device)

        plan = {
            0: ((p.me, 0, p.right), (p.left, 0)), 1: ((p.me, 1, p.left), (p.right, 1)),
            2: ((p.me, 2, p.partner), (p.partner, 2)),
            3: ((p.me, 1, p.right), (p.left, 1)), 4: ((p.me, 0, p.left), (p.right, 0)),
            5: ((p.left, 0, p.right), (p.far, 0)), 6: ((p.right, 1, p.left), (p.far, 1)),
            7: ((p.left, 0, p.partner), (p.left + other, 0)), 8: ((p.right, 1, p.partner), (p.right + other, 1)),
            9: ((p.left, 1, p.partner), (p.left + other, 1)), 10: ((p.right, 0, p.partner), (p.right + other, 0)),
            11: ((p.far, 0, p.partner), (p.far + other, 0)), 12: ((p.far, 1, p.partner), (p.far + other, 1)),
        }
        self.out = {i: copy(i, *s) for i, (s, _) in plan.items()}
        self.into = {i: copy(i, slot, part, p.partner) for i, (_, (slot, part)) in plan.items()}

    def start(self):
        for i in (0, 1, 2, 3, 4):
            self.out[i].start()

    def relay(self):
        for i, onward in ((0, (5, 7)), (1, (6, 8)), (3, (9,)), (4, (10,))):
            self.into[i].wait_recv()
            for j in onward:
                self.out[j].start()

    def finish(self):
        for i, j in ((5, 11), (6, 12)):
            self.into[i].wait_recv()
            self.out[j].start()
        for i in (2, 7, 8, 9, 10, 11, 12):
            self.into[i].wait_recv()

    def drain(self):
        for i in range(13):
            self.out[i].wait_send()


class Scatter:
    def __init__(self, pos, part, from_partner, work, arrive, send, recv):
        p = pos
        self.pos, self.part, self.from_partner, self.work, self.arrive = p, part, from_partner, work, arrive
        self.half = work.shape[-1]
        self.chips = (p.far_chip, p.right_chip, p.left_chip, p.chip)
        self.inner = [[remote(part.at[p.other, y, :, self.cols(h)], from_partner.at[y, :, self.cols(h)],
                              send.at[4 * h + k], recv.at[4 * h + k], p.partner) for k, y in enumerate(self.chips)]
                      for h in range(2)]
        self.outer = [remote(work.at[k], arrive.at[k], send.at[8 + k], recv.at[8 + k], p.right if k % 2 == 0 else p.left)
                      for k in range(6)]

    def cols(self, h):
        return pl.ds(h * self.half, self.half)

    def pair(self, k, h):
        y = self.chips[k]
        return self.part[self.pos.core, y, :, self.cols(h)].astype(F32) + self.from_partner[y, :, self.cols(h)].astype(F32)

    def send_sum(self, k, value):
        self.work[k] = value.astype(BF)
        self.outer[k].start()

    def start(self, h):
        for copy in self.inner[h]:
            copy.start()

    def relay_low(self):
        self.inner[0][0].wait_recv()
        self.send_sum(0, self.pair(0, 0))
        self.inner[0][2].wait_recv()
        self.send_sum(3, self.pair(2, 0))

    def relay_high(self):
        self.inner[1][0].wait_recv()
        self.send_sum(1, self.pair(0, 1))
        self.inner[1][1].wait_recv()
        self.send_sum(2, self.pair(1, 1))

    def relay_far(self):
        self.inner[0][1].wait_recv()
        self.outer[0].wait_recv()
        self.send_sum(4, self.pair(1, 0) + self.arrive[0].astype(F32))
        self.inner[1][2].wait_recv()
        self.outer[1].wait_recv()
        self.send_sum(5, self.pair(2, 1) + self.arrive[1].astype(F32))

    def finish(self):
        self.inner[0][3].wait_recv()
        self.inner[1][3].wait_recv()
        for k in (2, 3, 4, 5):
            self.outer[k].wait_recv()
        low = self.pair(3, 0) + self.arrive[3].astype(F32) + self.arrive[4].astype(F32)
        high = self.pair(3, 1) + self.arrive[2].astype(F32) + self.arrive[5].astype(F32)
        return jnp.concatenate([low, high], axis=-1)

    def drain(self):
        for copy in self.inner[0] + self.inner[1] + self.outer:
            copy.wait_send()


GATHER_SEMS = [pltpu.SemaphoreType.DMA((13,)), pltpu.SemaphoreType.DMA((13,))]
SCATTER_SEMS = [pltpu.SemaphoreType.DMA((14,)), pltpu.SemaphoreType.DMA((14,))]


def scatter_scratch(rows, dim):
    return [pltpu.VMEM((CHIPS, rows, dim), BF), pltpu.VMEM((6, rows, dim // 2), BF),
            pltpu.VMEM((6, rows, dim // 2), BF)] + SCATTER_SEMS


def put_part(part, value, col):
    rows, width = part.shape[2], value.shape[1]
    for b in range(CHIPS * CORES):
        part[b % CORES, b // CORES, :, pl.ds(col, width)] = value[b * rows:(b + 1) * rows].astype(BF)


def norm_stats(hidden_f):
    inv_rms = lax.rsqrt(jnp.mean(hidden_f * hidden_f, axis=-1, keepdims=True) + RMS_EPS)
    return hidden_f * inv_rms, inv_rms


def norm_bwd(grad_f, normed, inv_rms, gain):
    gain_part = jnp.sum(grad_f * normed, axis=0, keepdims=True)
    scaled = grad_f * gain
    return inv_rms * (scaled - normed * jnp.mean(scaled * normed, axis=-1, keepdims=True)), gain_part


def rope(values, cos2, sin2):
    return values * cos2 + pltpu.roll(values, values.shape[-1] // 2, axis=1) * sin2


def full(buf):
    blocks, rows, dim = buf.shape
    return buf[...].reshape(blocks * rows, dim)


def rope_tables(pos_row, freq_col):
    angles = jnp.transpose(freq_col * pos_row.astype(F32))
    lane = lax.broadcasted_iota(jnp.int32, angles.shape, 1)
    sin = jnp.sin(angles)
    return jnp.cos(angles), jnp.where(lane < angles.shape[1] // 2, -sin, sin)


def layer_kernel(tokens, positions, freq, gain_attn, gain_mlp, grad_own, emb_hbm, wq_hbm, wk_hbm, wv_hbm, wo_hbm, wg_hbm, wu_hbm, wd_hbm,
                 hidden_out, gains_out, n1_out, n2_out, gh_out, dh1_out, dx_out, heads_out, act_out, dgate_out, dup_out, dqkv_out,
                 emb, pick_buf, wqkv, wo, wg, wu, wd, wsem, osem, n1_buf, n2_buf, gh_buf, dh1_buf, dx_buf, gain_buf,
                 emb_part, attn_part, dn2_part, mlp_part, dn1_part, heads_buf, gact, act_buf, dgate_buf, dup_buf, dqkv_buf,
                 q_buf, probs_buf, cos_ref, sin_ref, *comm):
    pos = Place()
    num_heads, dim, head_dim = wq_hbm.shape
    rows_local = emb_hbm.shape[0]
    blocks, rows, _ = n1_buf.shape
    seq, ffn = blocks * rows, wg.shape[1]
    scatters, gathers = comm[:25], comm[25:]
    kq = num_heads * head_dim
    step = 512
    chunks = dim // step

    def emb_load(j):
        cols = pl.ds(pl.multiple_of(j * step, step), step)
        return pltpu.make_async_copy(emb_hbm.at[:, cols], emb.at[:, cols], wsem.at[j])

    for j in range(chunks):
        emb_load(j).start()
    pairs = [(wq_hbm.at[h], wqkv.at[:, pl.ds(h * head_dim, head_dim)]) for h in range(num_heads)]
    pairs += [(wk_hbm, wqkv.at[:, pl.ds(kq, head_dim)]), (wv_hbm, wqkv.at[:, pl.ds(kq + head_dim, head_dim)])]
    pairs += [(wo_hbm, wo), (wd_hbm, wd), (wg_hbm, wg), (wu_hbm, wu)]
    loads = [pltpu.make_async_copy(src, dst, wsem.at[chunks + k]) for k, (src, dst) in enumerate(pairs)]
    for load in loads:
        load.start()
    stores = []

    def store(src, dst):
        stores.append(pltpu.make_async_copy(src, dst, osem.at[len(stores)]))
        stores[-1].start()

    def halves(scatter, product):
        for h in range(2):
            @pl.loop(h * chunks // 2, (h + 1) * chunks // 2)
            def _(j):
                col = pl.multiple_of(j * step, step)
                put_part(scatter.part, product(j, col), col)

            scatter.start(h)

    gh_buf[pos.me] = grad_own[...]
    with jax.named_scope('barrier'):
        entry_barrier(pos)
    gather0 = Gather(pos, gh_buf, *gathers[2:4])
    gather0.start()

    with jax.named_scope('lookup'):
        local = jnp.transpose(jnp.broadcast_to(tokens[...] - pos.me * rows_local, (seq, seq)))
        lane = lax.broadcasted_iota(jnp.int32, (seq, seq), 1)
        for j in range(rows_local // seq):
            pick_buf[:, j * seq:(j + 1) * seq] = jnp.where(local == lane + j * seq, 1.0, 0.0).astype(BF)
        cos_ref[...], sin_ref[...] = rope_tables(positions[...], freq[...])

        def looked_up(j, col):
            emb_load(j).wait()
            return dot(pick_buf[...], emb[:, pl.ds(col, step)])

        scatter1 = Scatter(pos, emb_part, *scatters[0:5])
        halves(scatter1, looked_up)
    with jax.named_scope('rs1'):
        scatter1.relay_low()
        scatter1.relay_high()
        gather0.relay()
        scatter1.relay_far()
        gather0.finish()
        x0 = scatter1.finish()
    with jax.named_scope('norm1'):
        normed1, inv1 = norm_stats(x0)
        n1_buf[pos.me] = (normed1 * gain_attn[...]).astype(BF)
    with jax.named_scope('ag1'):
        gather1 = Gather(pos, n1_buf, *gathers[0:2])
        gather1.start()
        store(gh_buf, gh_out)
        gather1.relay()
        gather1.finish()
    store(n1_buf, n1_out)

    with jax.named_scope('qkv'):
        for load in loads[:5]:
            load.wait()
        qkv = dot(full(n1_buf), wqkv[...])
    with jax.named_scope('attention'):
        cos2, sin2 = cos_ref[...], sin_ref[...]
        keys = rope(qkv[:, kq:kq + head_dim], cos2, sin2).astype(BF)
        values = qkv[:, kq + head_dim:].astype(BF)
        causal = lax.broadcasted_iota(jnp.int32, (seq, seq), 0) >= lax.broadcasted_iota(jnp.int32, (seq, seq), 1)
        for h in range(num_heads):
            cols = slice(h * head_dim, (h + 1) * head_dim)
            query = rope(qkv[:, cols], cos2, sin2).astype(BF)
            q_buf[:, cols] = query
            scores = jnp.where(causal, dot_bt(query, keys) * (head_dim ** -0.5), -1e30)
            expd = jnp.exp(scores - jnp.max(scores, axis=-1, keepdims=True))
            probs = expd / jnp.sum(expd, axis=-1, keepdims=True)
            probs_buf[h] = probs
            heads_buf[:, cols] = dot(probs.astype(BF), values).astype(BF)
    store(heads_buf, heads_out)
    with jax.named_scope('w_out'):
        loads[5].wait()
        scatter3 = Scatter(pos, attn_part, *scatters[5:10])
        halves(scatter3, lambda j, col: dot(heads_buf[...], wo[:, pl.ds(col, step)]))

    with jax.named_scope('rs3_a'):
        scatter3.relay_low()
        scatter3.relay_high()

    with jax.named_scope('grad_act'):
        loads[6].wait()

        @pl.loop(0, ffn // 256)
        def _(j):
            cols = pl.ds(pl.multiple_of(j * 256, 256), 256)
            gact[:, cols] = dot_bt(full(gh_buf), wd[cols, :]).astype(BF)

    with jax.named_scope('rs3_b'):
        scatter3.relay_far()
        h1_bf = (x0 + scatter3.finish()).astype(BF)
    with jax.named_scope('norm2'):
        h1 = h1_bf.astype(F32)
        normed2, inv2 = norm_stats(h1)
        n2_buf[pos.me] = (normed2 * gain_mlp[...]).astype(BF)
    with jax.named_scope('ag4'):
        gather4 = Gather(pos, n2_buf, *gathers[4:6])
        gather4.start()
        gather4.relay()
        loads[7].wait()
        loads[8].wait()
        gather4.finish()
    store(n2_buf, n2_out)

    with jax.named_scope('gate_up'):
        @pl.loop(0, ffn // 256)
        def _(j):
            cols = pl.ds(pl.multiple_of(j * 256, 256), 256)
            n2 = full(n2_buf)
            gate_pre = dot(n2, wg[:, cols])
            up_pre = dot(n2, wu[:, cols])
            sig = jax.nn.sigmoid(gate_pre)
            gate_act = gate_pre * sig
            act_buf[:, cols] = (gate_act * up_pre).astype(BF)
            grad_act = gact[:, cols].astype(F32)
            dup_buf[:, cols] = (grad_act * gate_act).astype(BF)
            dgate_buf[:, cols] = (grad_act * up_pre * sig * (1.0 + gate_pre * (1.0 - sig))).astype(BF)

    store(act_buf, act_out)
    store(dgate_buf, dgate_out)
    store(dup_buf, dup_out)
    with jax.named_scope('dn2'):
        scatter6 = Scatter(pos, dn2_part, *scatters[10:15])
        halves(scatter6, lambda j, col: dot_bt(dgate_buf[...], wg[pl.ds(col, step), :]) + dot_bt(dup_buf[...], wu[pl.ds(col, step), :]))

    with jax.named_scope('rs6'):
        scatter6.relay_low()
        scatter6.relay_high()
        scatter6.relay_far()
        grad_n2 = scatter6.finish().astype(BF).astype(F32)
    with jax.named_scope('norm2_bwd'):
        grad_h1_norm, gain_mlp_part = norm_bwd(grad_n2, normed2, inv2, gain_mlp[...])
        grad_h1 = (grad_own[...].astype(F32) + grad_h1_norm).astype(BF)
        dh1_buf[pos.me] = grad_h1
        gain_buf[pos.me, 1:2, :] = gain_mlp_part
    gather7 = Gather(pos, dh1_buf, *gathers[6:8])
    gather7.start()
    with jax.named_scope('w_down'):
        @pl.loop(0, chunks)
        def _(j):
            col = pl.multiple_of(j * step, step)
            put_part(mlp_part, dot(act_buf[...], wd[:, pl.ds(col, step)]), col)

    with jax.named_scope('ag7'):
        gather7.relay()
        gather7.finish()
    scatter5 = Scatter(pos, mlp_part, *scatters[15:20])
    scatter5.start(0)
    scatter5.start(1)
    store(dh1_buf, dh1_out)

    with jax.named_scope('dheads'):
        dheads = dot_bt(full(dh1_buf), wo[...]).astype(BF)
    with jax.named_scope('rs5_relay'):
        scatter5.relay_low()
        scatter5.relay_high()
    with jax.named_scope('attention_bwd'):
        nsin2 = -sin2
        dkeys = jnp.zeros((seq, head_dim), F32)
        dvalues = jnp.zeros((seq, head_dim), F32)
        for h in range(num_heads):
            cols = slice(h * head_dim, (h + 1) * head_dim)
            dhead = dheads[:, cols]
            probs = probs_buf[h]
            dprobs = dot_bt(dhead, values).astype(BF).astype(F32)
            dvalues += dot_at(probs.astype(BF), dhead)
            inner = jnp.sum(dprobs * probs, axis=-1, keepdims=True)
            dscores = (probs * (dprobs - inner) * (head_dim ** -0.5)).astype(BF)
            dquery = dot(dscores, keys).astype(BF)
            dkeys += dot_at(dscores, q_buf[:, cols])
            dqkv_buf[:, cols] = rope(dquery.astype(F32), cos2, nsin2).astype(BF)
        dqkv_buf[:, kq:kq + head_dim] = rope(dkeys.astype(BF).astype(F32), cos2, nsin2).astype(BF)
        dqkv_buf[:, kq + head_dim:] = dvalues.astype(BF)
    store(dqkv_buf, dqkv_out)

    with jax.named_scope('dn1'):
        scatter8 = Scatter(pos, dn1_part, *scatters[20:25])
        halves(scatter8, lambda j, col: dot_bt(dqkv_buf[...], wqkv[pl.ds(col, step), :]))

    with jax.named_scope('rs8'):
        scatter5.relay_far()
        scatter8.relay_low()
        scatter8.relay_high()
        scatter8.relay_far()
        hidden_out[...] = (h1 + scatter5.finish()).astype(BF)
        grad_n1 = scatter8.finish().astype(BF).astype(F32)
    with jax.named_scope('norm1_bwd'):
        grad_x_norm, gain_attn_part = norm_bwd(grad_n1, normed1, inv1, gain_attn[...])
        dx_buf[pos.me] = (grad_h1.astype(F32) + grad_x_norm).astype(BF)
        gain_buf[pos.me, 0:1, :] = gain_attn_part
    with jax.named_scope('ag9'):
        gather9 = Gather(pos, dx_buf, *gathers[8:10])
        gatherg = Gather(pos, gain_buf, *gathers[10:12])
        gather9.start()
        gatherg.start()
        gather9.relay()
        gatherg.relay()
        gather9.finish()
        store(dx_buf, dx_out)
        gatherg.finish()
    with jax.named_scope('tail'):
        total = gain_buf[0]
        for i in range(1, blocks):
            total = total + gain_buf[i]
        gains_out[...] = total
        for op in (gather0, scatter1, gather1, scatter3, gather4, scatter6, gather7, scatter5, scatter8, gather9, gatherg):
            op.drain()
        for copy in stores:
            copy.wait()


def layer(tokens, positions, gain_attn, gain_mlp, grad_own, emb, wq, wk, wv, wo, wg, wu, wd):
    num_heads, dim, head_dim = wq.shape
    blocks = CHIPS * CORES
    seq, ffn, rows_local = tokens.shape[1], wg.shape[1], emb.shape[0]
    rows = seq // blocks
    half = head_dim // 2
    freq = np.float32(ROPE_THETA) ** (-np.arange(half, dtype=np.float32) * np.float32(2.0 / head_dim))
    freq = jnp.asarray(np.concatenate([freq, freq])[:, None], F32)
    vmem = pl.BlockSpec(memory_space=pltpu.VMEM)
    hbm = pl.BlockSpec(memory_space=pltpu.HBM)
    width = num_heads * head_dim
    wide = width + 2 * head_dim
    sds = jax.ShapeDtypeStruct
    outs = [sds((rows, dim), BF), sds((2, dim), F32)] + [sds((blocks, rows, dim), BF)] * 5
    outs += [sds((seq, width), BF)] + [sds((seq, ffn), BF)] * 3 + [sds((seq, wide), BF)]
    part = pltpu.VMEM((CORES, CHIPS, rows, dim), BF)
    gathered = pltpu.VMEM((blocks, rows, dim), BF)
    table = pltpu.VMEM((seq, head_dim), F32)
    scratch = [pltpu.VMEM((rows_local, dim), BF), pltpu.VMEM((seq, rows_local), BF), pltpu.VMEM((dim, wide), BF),
               pltpu.VMEM((width, dim), BF), pltpu.VMEM((dim, ffn), BF),
               pltpu.VMEM((dim, ffn), BF), pltpu.VMEM((ffn, dim), BF), pltpu.SemaphoreType.DMA((16,)), pltpu.SemaphoreType.DMA((10,))]
    scratch += [gathered] * 5 + [pltpu.VMEM((blocks, 2, dim), F32)] + [part] * 5 + [pltpu.VMEM((seq, width), BF)]
    scratch += [pltpu.VMEM((seq, ffn), BF)] * 4 + [pltpu.VMEM((seq, wide), BF), pltpu.VMEM((seq, width), BF),
                                                   pltpu.VMEM((num_heads, seq, seq), F32), table, table]
    scratch += scatter_scratch(rows, dim) * 5 + GATHER_SEMS * 6
    return pl.pallas_call(
        layer_kernel, out_shape=outs, in_specs=[vmem] * 6 + [hbm] * 8, out_specs=[vmem] * 2 + [hbm] * 10,
        scratch_shapes=scratch,
        compiler_params=pltpu.CompilerParams(collective_id=0, has_side_effects=True, vmem_limit_bytes=VMEM_FULL),
        name='layer',
    )(tokens, positions, freq, gain_attn, gain_mlp, grad_own, emb, wq, wk, wv, wo, wg, wu, wd)


def grads_kernel(n1, n2, dqkv, dgate, dup, heads, act, dh1, gh, tokens, dx, hidden_in, gains_in,
                 gw_query, gw_key, gw_value, gw_out, gw_gate, gw_up, gw_down, g_emb, hidden, g_attn, g_mlp, pick):
    num_heads, _, head_dim = gw_query.shape
    width = num_heads * head_dim
    rows_local, seq = pick.shape

    @pl.when(pl.program_id(0) == 0)
    def _():
        hidden[...] = hidden_in[...]
        g_attn[...] = gains_in[0:1, :]
        g_mlp[...] = gains_in[1:2, :]
        local = tokens[...] - lax.axis_index('tp') * rows_local
        pick[...] = jnp.where(lax.broadcasted_iota(jnp.int32, (rows_local, seq), 0) == local, 1.0, 0.0).astype(BF)

    gw_gate[...] = dot_at(n2[...], dgate[...])
    gw_up[...] = dot_at(n2[...], dup[...])
    gw_down[...] = dot_at(act[...], gh[...])
    both = dot_at(n1[...], dqkv[...])
    for h in range(num_heads):
        gw_query[h] = both[:, h * head_dim:(h + 1) * head_dim]
    gw_key[...] = both[:, width:width + head_dim]
    gw_value[...] = both[:, width + head_dim:]
    gw_out[...] = dot_at(heads[...], dh1[...])
    g_emb[...] = dot(pick[...], dx[...])


def grads(n1, n2, dqkv, dgate, dup, heads, act, dh1, gh, tokens, dx, hidden, gains, rows_local, head_dim):
    seq, dim = n1.shape
    width, ffn = heads.shape[1], act.shape[1]
    num_heads = width // head_dim
    tile = 256
    sds = jax.ShapeDtypeStruct

    def whole(x):
        return pl.BlockSpec(x.shape, lambda i: (0,) * len(x.shape))

    def by_col(n):
        return pl.BlockSpec((n, tile), lambda i: (0, i))

    def by_row(n):
        return pl.BlockSpec((tile, n), lambda i: (i, 0))

    gain = sds((1, dim), F32)
    return pl.pallas_call(
        grads_kernel, grid=(dim // tile,),
        out_shape=[sds((num_heads, dim, head_dim), F32), sds((dim, head_dim), F32), sds((dim, head_dim), F32), sds((width, dim), F32),
                   sds((dim, ffn), F32), sds((dim, ffn), F32), sds((ffn, dim), F32), sds((rows_local, dim), F32),
                   sds(hidden.shape, BF), gain, gain],
        in_specs=[by_col(seq), by_col(seq), whole(dqkv), whole(dgate), whole(dup), whole(heads), whole(act), by_col(seq), by_col(seq),
                  whole(tokens), by_col(seq), whole(hidden), whole(gains)],
        out_specs=[pl.BlockSpec((num_heads, tile, head_dim), lambda i: (0, i, 0)), by_row(head_dim), by_row(head_dim), by_col(width),
                   by_row(ffn), by_row(ffn), by_col(ffn), by_col(rows_local), whole(hidden), whole(gain), whole(gain)],
        scratch_shapes=[pltpu.VMEM((rows_local, seq), BF)],
        compiler_params=pltpu.CompilerParams(vmem_limit_bytes=VMEM_FULL),
        name='grads',
    )(n1, n2, dqkv, dgate, dup, heads, act, dh1, gh, tokens, dx, hidden, gains)


def solution(mesh):
    if mesh.shape['tp'] != CHIPS * CORES:
        raise ValueError('tp size')
    in_specs = (P('dp', None), P('dp', None), P('tp', None), P(None), P(None),
                P(None, 'tp', None), P(None, 'tp', None), P(None, 'tp', None), P('tp', None, None),
                P(None, 'tp'), P(None, 'tp'), P('tp', None), P('dp', 'tp', None))
    out_specs = (P('dp', 'tp', None), P(('dp', 'tp'), None),
                 P('dp', 'tp', None), P('dp', 'tp', None), P('dp', 'tp', None), P(('dp', 'tp'), None, None),
                 P('dp', 'tp'), P('dp', 'tp'), P(('dp', 'tp'), None), P('dp'), P('dp'))

    def device_fn(tokens, positions, emb_shard, gain_attn, gain_mlp, w_query, w_key, w_value, w_out, w_gate, w_up, w_down, grad_hidden):
        rows_local, dim = emb_shard.shape
        seq = tokens.shape[1]
        num_heads, head_dim = w_query.shape[1], w_query.shape[2]
        wq = jnp.transpose(w_query, (1, 0, 2))
        wk, wv = w_key.reshape(dim, head_dim), w_value.reshape(dim, head_dim)
        wo = w_out.reshape(num_heads * head_dim, dim)

        hidden, gains, n1, n2, gh, dh1, dx, heads, act, dgate, dup, dqkv = layer(
            tokens, positions, gain_attn[None, :], gain_mlp[None, :], grad_hidden[0], emb_shard, wq, wk, wv, wo, w_gate, w_up, w_down)
        n1, n2, gh, dh1, dx = (x.reshape(seq, dim) for x in (n1, n2, gh, dh1, dx))
        gw_query, gw_key, gw_value, gw_out, gw_gate, gw_up, gw_down, g_emb, hidden, g_attn, g_mlp = grads(
            n1, n2, dqkv, dgate, dup, heads, act, dh1, gh, tokens, dx, hidden, gains, rows_local, head_dim)
        return (hidden[None], g_emb, jnp.transpose(gw_query, (1, 0, 2)), gw_key.reshape(dim, 1, head_dim),
                gw_value.reshape(dim, 1, head_dim), gw_out.reshape(num_heads, head_dim, dim),
                gw_gate, gw_up, gw_down, g_attn[0], g_mlp[0])

    return jax.shard_map(device_fn, mesh=mesh, in_specs=in_specs, out_specs=out_specs, check_vma=False)
```

```python
import jax
import jax.numpy as jnp
import numpy as np
from jax import lax
from jax.experimental import pallas as pl
from jax.experimental.pallas import tpu as pltpu
from jax.sharding import PartitionSpec as P

ROPE_THETA = 1000000.0
RMS_EPS = 1e-5
BF = jnp.bfloat16
F32 = jnp.float32
VMEM_FULL = 67043328
CHIPS = 4
CORES = 2


def dot(a, b):
    return lax.dot_general(a, b, (((1,), (0,)), ((), ())), preferred_element_type=F32)


def dot_bt(a, b):
    return lax.dot_general(a, b, (((1,), (1,)), ((), ())), preferred_element_type=F32)


def dot_at(a, b):
    return lax.dot_general(a, b, (((0,), (0,)), ((), ())), preferred_element_type=F32)


class Place:
    def __init__(self):
        me = lax.axis_index('tp')
        self.chip, self.core = me // CORES, me % CORES
        self.right_chip = (self.chip + 1) % CHIPS
        self.left_chip = (self.chip + CHIPS - 1) % CHIPS
        self.far_chip = (self.chip + 2) % CHIPS
        self.me = me
        self.other = 1 - self.core
        self.partner = self.chip * CORES + self.other
        self.right = self.right_chip * CORES + self.core
        self.left = self.left_chip * CORES + self.core
        self.far = self.far_chip * CORES + self.core


def remote(src, dst, send, recv, device):
    return pltpu.make_async_remote_copy(src_ref=src, dst_ref=dst, send_sem=send, recv_sem=recv,
                                        device_id={'tp': device}, device_id_type=pl.DeviceIdType.MESH)


def entry_barrier(pos):
    barrier = pltpu.get_barrier_semaphore()
    for device in (pos.left, pos.right, pos.partner):
        pl.semaphore_signal(barrier, inc=1, device_id={'tp': device}, device_id_type=pl.DeviceIdType.MESH)
    pl.semaphore_wait(barrier, 3)


class Gather:
    def __init__(self, pos, buf, send, recv):
        self.pos, self.buf = pos, buf
        half = buf.shape[-1] // 2
        p = pos
        other = p.other - p.core

        def piece(slot, part):
            if part == 2:
                return buf.at[slot]
            return buf.at[slot, :, pl.ds(part * half, half)]

        def copy(index, slot, part, device):
            ref = piece(slot, part)
            return remote(ref, ref, send.at[index], recv.at[index], device)

        plan = {
            0: ((p.me, 0, p.right), (p.left, 0)), 1: ((p.me, 1, p.left), (p.right, 1)),
            2: ((p.me, 2, p.partner), (p.partner, 2)),
            3: ((p.me, 1, p.right), (p.left, 1)), 4: ((p.me, 0, p.left), (p.right, 0)),
            5: ((p.left, 0, p.right), (p.far, 0)), 6: ((p.right, 1, p.left), (p.far, 1)),
            7: ((p.left, 0, p.partner), (p.left + other, 0)), 8: ((p.right, 1, p.partner), (p.right + other, 1)),
            9: ((p.left, 1, p.partner), (p.left + other, 1)), 10: ((p.right, 0, p.partner), (p.right + other, 0)),
            11: ((p.far, 0, p.partner), (p.far + other, 0)), 12: ((p.far, 1, p.partner), (p.far + other, 1)),
        }
        self.out = {i: copy(i, *s) for i, (s, _) in plan.items()}
        self.into = {i: copy(i, slot, part, p.partner) for i, (_, (slot, part)) in plan.items()}

    def start(self):
        for i in (0, 1, 2, 3, 4):
            self.out[i].start()

    def relay(self):
        for i, onward in ((0, (5, 7)), (1, (6, 8)), (3, (9,)), (4, (10,))):
            self.into[i].wait_recv()
            for j in onward:
                self.out[j].start()

    def finish(self):
        for i, j in ((5, 11), (6, 12)):
            self.into[i].wait_recv()
            self.out[j].start()
        for i in (2, 7, 8, 9, 10, 11, 12):
            self.into[i].wait_recv()

    def drain(self):
        for i in range(13):
            self.out[i].wait_send()


class Spread:
    def __init__(self, pos, buf, send, recv):
        p = pos
        other = p.other - p.core

        def copy(index, slot, device):
            return remote(buf.at[slot], buf.at[slot], send.at[index], recv.at[index], device)

        sent = ((p.me, p.right), (p.me, p.left), (p.me, p.partner), (p.left, p.right),
                (p.left, p.partner), (p.right, p.partner), (p.far, p.partner))
        got = (p.left, p.right, p.partner, p.far, p.left + other, p.right + other, p.far + other)
        self.out = [copy(i, slot, device) for i, (slot, device) in enumerate(sent)]
        self.into = [copy(i, slot, p.partner) for i, slot in enumerate(got)]

    def start(self):
        for i in (0, 1, 2):
            self.out[i].start()

    def relay(self):
        self.into[0].wait_recv()
        self.out[3].start()
        self.out[4].start()
        self.into[1].wait_recv()
        self.out[5].start()

    def relay_far(self):
        self.into[3].wait_recv()
        self.out[6].start()

    def finish(self):
        for i in (2, 4, 5, 6):
            self.into[i].wait_recv()

    def drain(self):
        for copy in self.out:
            copy.wait_send()


class Scatter:
    def __init__(self, pos, part, from_partner, work, arrive, send, recv):
        p = pos
        self.pos, self.part, self.from_partner, self.work, self.arrive = p, part, from_partner, work, arrive
        self.half = work.shape[-1]
        self.chips = (p.far_chip, p.right_chip, p.left_chip, p.chip)
        self.inner = [[remote(part.at[p.other, y, :, self.cols(h)], from_partner.at[y, :, self.cols(h)],
                              send.at[4 * h + k], recv.at[4 * h + k], p.partner) for k, y in enumerate(self.chips)]
                      for h in range(2)]
        self.outer = [remote(work.at[k], arrive.at[k], send.at[8 + k], recv.at[8 + k], p.right if k % 2 == 0 else p.left)
                      for k in range(6)]

    def cols(self, h):
        return pl.ds(h * self.half, self.half)

    def pair(self, k, h):
        y = self.chips[k]
        return self.part[self.pos.core, y, :, self.cols(h)].astype(F32) + self.from_partner[y, :, self.cols(h)].astype(F32)

    def send_sum(self, k, value):
        self.work[k] = value.astype(BF)
        self.outer[k].start()

    def start(self, h):
        for copy in self.inner[h]:
            copy.start()

    def relay_low(self):
        self.inner[0][0].wait_recv()
        self.send_sum(0, self.pair(0, 0))
        self.inner[0][2].wait_recv()
        self.send_sum(3, self.pair(2, 0))

    def relay_high(self):
        self.inner[1][0].wait_recv()
        self.send_sum(1, self.pair(0, 1))
        self.inner[1][1].wait_recv()
        self.send_sum(2, self.pair(1, 1))

    def relay_far(self):
        self.inner[0][1].wait_recv()
        self.outer[0].wait_recv()
        self.send_sum(4, self.pair(1, 0) + self.arrive[0].astype(F32))
        self.inner[1][2].wait_recv()
        self.outer[1].wait_recv()
        self.send_sum(5, self.pair(2, 1) + self.arrive[1].astype(F32))

    def finish(self):
        self.inner[0][3].wait_recv()
        self.inner[1][3].wait_recv()
        for k in (2, 3, 4, 5):
            self.outer[k].wait_recv()
        low = self.pair(3, 0) + self.arrive[3].astype(F32) + self.arrive[4].astype(F32)
        high = self.pair(3, 1) + self.arrive[2].astype(F32) + self.arrive[5].astype(F32)
        return jnp.concatenate([low, high], axis=-1)

    def drain(self):
        for copy in self.inner[0] + self.inner[1] + self.outer:
            copy.wait_send()


GATHER_SEMS = [pltpu.SemaphoreType.DMA((13,)), pltpu.SemaphoreType.DMA((13,))]
SCATTER_SEMS = [pltpu.SemaphoreType.DMA((14,)), pltpu.SemaphoreType.DMA((14,))]


def scatter_scratch(rows, dim):
    return [pltpu.VMEM((CHIPS, rows, dim), BF), pltpu.VMEM((6, rows, dim // 2), BF),
            pltpu.VMEM((6, rows, dim // 2), BF)]


def put_part(part, value, col):
    rows, width = part.shape[2], value.shape[1]
    for b in range(CHIPS * CORES):
        part[b % CORES, b // CORES, :, pl.ds(col, width)] = value[b * rows:(b + 1) * rows].astype(BF)


def norm_stats(hidden_f):
    inv_rms = lax.rsqrt(jnp.mean(hidden_f * hidden_f, axis=-1, keepdims=True) + RMS_EPS)
    return hidden_f * inv_rms, inv_rms


def norm_bwd(grad_f, normed, inv_rms, gain):
    gain_part = jnp.sum(grad_f * normed, axis=0, keepdims=True)
    scaled = grad_f * gain
    return inv_rms * (scaled - normed * jnp.mean(scaled * normed, axis=-1, keepdims=True)), gain_part


def rope(values, cos2, sin2):
    return values * cos2 + pltpu.roll(values, values.shape[-1] // 2, axis=1) * sin2


def full(buf):
    blocks, rows, dim = buf.shape
    return buf[...].reshape(blocks * rows, dim)


def rope_tables(pos_row, freq_col):
    angles = jnp.transpose(freq_col * pos_row.astype(F32))
    lane = lax.broadcasted_iota(jnp.int32, angles.shape, 1)
    sin = jnp.sin(angles)
    return jnp.cos(angles), jnp.where(lane < angles.shape[1] // 2, -sin, sin)


def layer_kernel(tokens, positions, freq, gain_attn, gain_mlp, grad_own, emb_hbm, wq_hbm, wk_hbm, wv_hbm, wo_hbm, wg_hbm, wu_hbm, wd_hbm,
                 hidden_out, gains_out, n1_out, n2_out, gh_out, dh1_out, dx_out, heads_out, act_out, dgu_out, dqkv_out,
                 emb, pick_buf, wqkv, wqkv_t, wo, wg, wu, wd, wsem, osem, n1_buf, n2_buf, gh_buf, dh1_buf, dx_buf, gain_buf,
                 emb_part, attn_part, dn2_part, mlp_part, dn1_part, heads_buf, gact, act_buf, dgu_buf, dqkv_buf,
                 q_buf, probs_buf, cos_ref, sin_ref, hidden_buf, gain_sum, *comm):
    pos = Place()
    num_heads, dim, head_dim = wq_hbm.shape
    rows_local = emb_hbm.shape[0]
    blocks, rows, _ = n1_buf.shape
    seq, ffn = blocks * rows, wg.shape[1]
    scatters = [comm[3 * i:3 * i + 3] for i in range(5)]
    main_s, side_s, main_g, side_g, gain_s = (comm[15 + 2 * i:17 + 2 * i] for i in range(5))
    kq = num_heads * head_dim
    step = 512
    chunks = dim // step

    def emb_load(j):
        cols = pl.ds(pl.multiple_of(j * step, step), step)
        return pltpu.make_async_copy(emb_hbm.at[:, cols], emb.at[:, cols], wsem.at[j])

    for j in range(chunks):
        emb_load(j).start()
    pairs = [(wq_hbm.at[h], wqkv.at[:, pl.ds(h * head_dim, head_dim)]) for h in range(num_heads)]
    pairs += [(wk_hbm, wqkv.at[:, pl.ds(kq, head_dim)]), (wv_hbm, wqkv.at[:, pl.ds(kq + head_dim, head_dim)])]
    pairs += [(wo_hbm, wo), (wd_hbm, wd), (wg_hbm, wg), (wu_hbm, wu)]
    loads = [pltpu.make_async_copy(src, dst, wsem.at[chunks + k]) for k, (src, dst) in enumerate(pairs)]
    for load in loads:
        load.start()
    stores = []

    def store(src, dst):
        stores.append(pltpu.make_async_copy(src, dst, osem.at[len(stores)]))
        stores[-1].start()

    def halves(scatter, product):
        for h in range(2):
            @pl.loop(h * chunks // 2, (h + 1) * chunks // 2)
            def _(j):
                col = pl.multiple_of(j * step, step)
                put_part(scatter.part, product(j, col), col)

            scatter.start(h)

    def turn(src, dst, first):
        @pl.loop(0, src.shape[0] // 128)
        def _(j):
            at = pl.multiple_of(j * 128, 128)
            dst[first:first + src.shape[1], pl.ds(at, 128)] = jnp.transpose(src[pl.ds(at, 128), :])

    gh_buf[pos.me] = grad_own[...]
    with jax.named_scope('barrier'):
        entry_barrier(pos)
    gather0 = Gather(pos, gh_buf, *side_g)
    gather0.start()

    with jax.named_scope('lookup'):
        local = jnp.transpose(jnp.broadcast_to(tokens[...] - pos.me * rows_local, (seq, seq)))
        lane = lax.broadcasted_iota(jnp.int32, (seq, seq), 1)
        for j in range(rows_local // seq):
            pick_buf[:, j * seq:(j + 1) * seq] = jnp.where(local == lane + j * seq, 1.0, 0.0).astype(BF)
        cos_ref[...], sin_ref[...] = rope_tables(positions[...], freq[...])

        def looked_up(j, col):
            emb_load(j).wait()
            return dot(pick_buf[...], emb[:, pl.ds(col, step)])

        scatter1 = Scatter(pos, emb_part, *scatters[0], *main_s)
        halves(scatter1, looked_up)
    with jax.named_scope('rs1'):
        scatter1.relay_low()
        scatter1.relay_high()
        gather0.relay()
        scatter1.relay_far()
        gather0.finish()
        x0 = scatter1.finish()
    with jax.named_scope('norm1'):
        normed1, inv1 = norm_stats(x0)
        n1_buf[pos.me] = (normed1 * gain_attn[...]).astype(BF)
    with jax.named_scope('ag1'):
        gather1 = Gather(pos, n1_buf, *main_g)
        gather1.start()
        store(gh_buf, gh_out)
    with jax.named_scope('turn_gate'):
        loads[7].wait()
        turn(wg, emb, 0)
    with jax.named_scope('ag1_relay'):
        gather1.relay()
    with jax.named_scope('turn_up'):
        loads[8].wait()
        turn(wu, emb, ffn)
    with jax.named_scope('ag1_finish'):
        gather1.finish()
    store(n1_buf, n1_out)

    with jax.named_scope('qkv'):
        for load in loads[:5]:
            load.wait()
        qkv = dot(full(n1_buf), wqkv[...])
    with jax.named_scope('attention'):
        cos2, sin2 = cos_ref[...], sin_ref[...]
        keys = rope(qkv[:, kq:kq + head_dim], cos2, sin2).astype(BF)
        values = qkv[:, kq + head_dim:].astype(BF)
        causal = lax.broadcasted_iota(jnp.int32, (seq, seq), 0) >= lax.broadcasted_iota(jnp.int32, (seq, seq), 1)
        for h in range(num_heads):
            cols = slice(h * head_dim, (h + 1) * head_dim)
            query = rope(qkv[:, cols], cos2, sin2).astype(BF)
            q_buf[:, cols] = query
            scores = jnp.where(causal, dot_bt(query, keys) * (head_dim ** -0.5), -1e30)
            expd = jnp.exp(scores - jnp.max(scores, axis=-1, keepdims=True))
            probs = expd / jnp.sum(expd, axis=-1, keepdims=True)
            probs_buf[h] = probs
            heads_buf[:, cols] = dot(probs.astype(BF), values).astype(BF)
    store(heads_buf, heads_out)
    with jax.named_scope('w_out'):
        loads[5].wait()
        scatter3 = Scatter(pos, attn_part, *scatters[1], *main_s)
        scatter1.drain()
        halves(scatter3, lambda j, col: dot(heads_buf[...], wo[:, pl.ds(col, step)]))

    with jax.named_scope('rs3_a'):
        scatter3.relay_low()
        scatter3.relay_high()

    with jax.named_scope('grad_act'):
        loads[6].wait()

        @pl.loop(0, ffn // 256)
        def _(j):
            cols = pl.ds(pl.multiple_of(j * 256, 256), 256)
            gact[:, cols] = dot_bt(full(gh_buf), wd[cols, :]).astype(BF)

    with jax.named_scope('rs3_b'):
        scatter3.relay_far()
        h1_bf = (x0 + scatter3.finish()).astype(BF)
    with jax.named_scope('norm2'):
        h1 = h1_bf.astype(F32)
        normed2, inv2 = norm_stats(h1)
        n2_buf[pos.me] = (normed2 * gain_mlp[...]).astype(BF)
    with jax.named_scope('ag4'):
        gather4 = Gather(pos, n2_buf, *main_g)
        gather1.drain()
        gather4.start()
        turn(wqkv, wqkv_t, 0)
        gather4.relay()
        gather4.finish()
    store(n2_buf, n2_out)

    with jax.named_scope('gate_up'):
        @pl.loop(0, ffn // 256)
        def _(j):
            cols = pl.ds(pl.multiple_of(j * 256, 256), 256)
            n2 = full(n2_buf)
            gate_pre = dot(n2, wg[:, cols])
            up_pre = dot(n2, wu[:, cols])
            sig = jax.nn.sigmoid(gate_pre)
            gate_act = gate_pre * sig
            act_buf[:, cols] = (gate_act * up_pre).astype(BF)
            grad_act = gact[:, cols].astype(F32)
            dgu_buf[:, pl.ds(pl.multiple_of(ffn + j * 256, 256), 256)] = (grad_act * gate_act).astype(BF)
            dgu_buf[:, cols] = (grad_act * up_pre * sig * (1.0 + gate_pre * (1.0 - sig))).astype(BF)

    store(act_buf, act_out)
    store(dgu_buf, dgu_out)
    with jax.named_scope('dn2'):
        scatter6 = Scatter(pos, dn2_part, *scatters[2], *main_s)
        scatter3.drain()
        halves(scatter6, lambda j, col: dot(dgu_buf[...], emb[:, pl.ds(col, step)]))

    with jax.named_scope('rs6'):
        scatter6.relay_low()
        scatter6.relay_high()
        scatter6.relay_far()
        grad_n2 = scatter6.finish().astype(BF).astype(F32)
    with jax.named_scope('norm2_bwd'):
        grad_h1_norm, gain_mlp_part = norm_bwd(grad_n2, normed2, inv2, gain_mlp[...])
        grad_h1 = (grad_own[...].astype(F32) + grad_h1_norm).astype(BF)
        dh1_buf[pos.me] = grad_h1
        gain_buf[pos.me, 1:2, :] = gain_mlp_part
    gather7 = Gather(pos, dh1_buf, *main_g)
    gather4.drain()
    gather7.start()
    with jax.named_scope('w_down'):
        @pl.loop(0, chunks)
        def _(j):
            col = pl.multiple_of(j * step, step)
            put_part(mlp_part, dot(act_buf[...], wd[:, pl.ds(col, step)]), col)

    scatter5 = Scatter(pos, mlp_part, *scatters[3], *side_s)
    with jax.named_scope('ag7'):
        gather7.relay()
        scatter5.start(0)
        scatter5.start(1)
        gather7.finish()
    with jax.named_scope('rs5_relay'):
        scatter5.relay_low()
        scatter5.relay_high()
    store(dh1_buf, dh1_out)

    with jax.named_scope('dheads'):
        dheads = dot_bt(full(dh1_buf), wo[...]).astype(BF)
    with jax.named_scope('attention_bwd'):
        nsin2 = -sin2
        dkeys = jnp.zeros((seq, head_dim), F32)
        dvalues = jnp.zeros((seq, head_dim), F32)
        for h in range(num_heads):
            cols = slice(h * head_dim, (h + 1) * head_dim)
            dhead = dheads[:, cols]
            probs = probs_buf[h]
            dprobs = dot_bt(dhead, values).astype(BF).astype(F32)
            dvalues += dot_at(probs.astype(BF), dhead)
            inner = jnp.sum(dprobs * probs, axis=-1, keepdims=True)
            dscores = (probs * (dprobs - inner) * (head_dim ** -0.5)).astype(BF)
            dquery = dot(dscores, keys).astype(BF)
            dkeys += dot_at(dscores, q_buf[:, cols])
            dqkv_buf[:, cols] = rope(dquery.astype(F32), cos2, nsin2).astype(BF)
        dqkv_buf[:, kq:kq + head_dim] = rope(dkeys.astype(BF).astype(F32), cos2, nsin2).astype(BF)
        dqkv_buf[:, kq + head_dim:] = dvalues.astype(BF)
    store(dqkv_buf, dqkv_out)

    with jax.named_scope('dn1'):
        scatter8 = Scatter(pos, dn1_part, *scatters[4], *main_s)
        scatter6.drain()
        halves(scatter8, lambda j, col: dot(dqkv_buf[...], wqkv_t[:, pl.ds(col, step)]))

    with jax.named_scope('rs8'):
        scatter8.relay_low()
        scatter8.relay_high()
        scatter5.relay_far()
        scatter8.relay_far()
        hidden_buf[...] = (h1 + scatter5.finish()).astype(BF)
        store(hidden_buf, hidden_out)
        grad_n1 = scatter8.finish().astype(BF).astype(F32)
    with jax.named_scope('norm1_bwd'):
        grad_x_norm, gain_attn_part = norm_bwd(grad_n1, normed1, inv1, gain_attn[...])
        dx_buf[pos.me] = (grad_h1.astype(F32) + grad_x_norm).astype(BF)
        gain_buf[pos.me, 0:1, :] = gain_attn_part
    with jax.named_scope('ag9'):
        gather7.drain()
        spread = Spread(pos, gain_buf, *gain_s)
        gather9 = Gather(pos, dx_buf, *main_g)
        spread.start()
        gather9.start()
        spread.relay()
        gather9.relay()
        spread.relay_far()
        gather9.finish()
        store(dx_buf, dx_out)
        spread.finish()
    with jax.named_scope('tail'):
        total = gain_buf[0]
        for i in range(1, blocks):
            total = total + gain_buf[i]
        gain_sum[...] = total
        store(gain_sum, gains_out)
        for op in (gather0, scatter5, scatter8, gather9, spread):
            op.drain()
        for copy in stores:
            copy.wait()


def layer(tokens, positions, gain_attn, gain_mlp, grad_own, emb, wq, wk, wv, wo, wg, wu, wd):
    num_heads, dim, head_dim = wq.shape
    blocks = CHIPS * CORES
    seq, ffn, rows_local = tokens.shape[1], wg.shape[1], emb.shape[0]
    rows = seq // blocks
    if rows_local != 2 * ffn:
        raise ValueError('shard rows')
    half = head_dim // 2
    freq = np.float32(ROPE_THETA) ** (-np.arange(half, dtype=np.float32) * np.float32(2.0 / head_dim))
    freq = jnp.asarray(np.concatenate([freq, freq])[:, None], F32)
    vmem = pl.BlockSpec(memory_space=pltpu.VMEM)
    hbm = pl.BlockSpec(memory_space=pltpu.HBM)
    width = num_heads * head_dim
    wide = width + 2 * head_dim
    sds = jax.ShapeDtypeStruct
    outs = [sds((rows, dim), BF), sds((2, dim), F32)] + [sds((blocks, rows, dim), BF)] * 5
    outs += [sds((seq, width), BF), sds((seq, ffn), BF), sds((seq, 2 * ffn), BF), sds((seq, wide), BF)]
    part = pltpu.VMEM((CORES, CHIPS, rows, dim), BF)
    gathered = pltpu.VMEM((blocks, rows, dim), BF)
    table = pltpu.VMEM((seq, head_dim), F32)
    scratch = [pltpu.VMEM((rows_local, dim), BF), pltpu.VMEM((seq, rows_local), BF), pltpu.VMEM((dim, wide), BF), pltpu.VMEM((wide, dim), BF),
               pltpu.VMEM((width, dim), BF), pltpu.VMEM((dim, ffn), BF),
               pltpu.VMEM((dim, ffn), BF), pltpu.VMEM((ffn, dim), BF), pltpu.SemaphoreType.DMA((15,)), pltpu.SemaphoreType.DMA((11,))]
    scratch += [gathered] * 5 + [pltpu.VMEM((blocks, 2, dim), F32)] + [part] * 5 + [pltpu.VMEM((seq, width), BF)]
    scratch += [pltpu.VMEM((seq, ffn), BF)] * 2 + [pltpu.VMEM((seq, 2 * ffn), BF), pltpu.VMEM((seq, wide), BF), pltpu.VMEM((seq, width), BF),
                                                   pltpu.VMEM((num_heads, seq, seq), F32), table, table,
                                                   pltpu.VMEM((rows, dim), BF), pltpu.VMEM((2, dim), F32)]
    scratch += scatter_scratch(rows, dim) * 5 + SCATTER_SEMS * 2 + GATHER_SEMS * 2 + [pltpu.SemaphoreType.DMA((7,))] * 2
    return pl.pallas_call(
        layer_kernel, out_shape=outs, in_specs=[vmem] * 6 + [hbm] * 8, out_specs=[hbm] * 11,
        scratch_shapes=scratch,
        compiler_params=pltpu.CompilerParams(collective_id=0, has_side_effects=True, vmem_limit_bytes=VMEM_FULL),
        name='layer',
    )(tokens, positions, freq, gain_attn, gain_mlp, grad_own, emb, wq, wk, wv, wo, wg, wu, wd)


def grads_kernel(n1, n2, dqkv, dgate, dup, heads, act, dh1, gh, tokens, dx, hidden_in, gains_in,
                 gw_query, gw_key, gw_value, gw_out, gw_gate, gw_up, gw_down, g_emb, hidden, g_attn, g_mlp, pick):
    num_heads, _, head_dim = gw_query.shape
    width = num_heads * head_dim
    rows_local, seq = pick.shape

    @pl.when(pl.program_id(0) == 0)
    def _():
        hidden[...] = hidden_in[...]
        g_attn[...] = gains_in[0:1, :]
        g_mlp[...] = gains_in[1:2, :]
        local = tokens[...] - lax.axis_index('tp') * rows_local
        pick[...] = jnp.where(lax.broadcasted_iota(jnp.int32, (rows_local, seq), 0) == local, 1.0, 0.0).astype(BF)

    gw_gate[...] = dot_at(n2[...], dgate[...])
    gw_up[...] = dot_at(n2[...], dup[...])
    gw_down[...] = dot_at(act[...], gh[...])
    both = dot_at(n1[...], dqkv[...])
    for h in range(num_heads):
        gw_query[h] = both[:, h * head_dim:(h + 1) * head_dim]
    gw_key[...] = both[:, width:width + head_dim]
    gw_value[...] = both[:, width + head_dim:]
    gw_out[...] = dot_at(heads[...], dh1[...])
    g_emb[...] = dot(pick[...], dx[...])


def grads(n1, n2, dqkv, dgu, heads, act, dh1, gh, tokens, dx, hidden, gains, rows_local, head_dim):
    seq, dim = n1.shape
    width, ffn = heads.shape[1], act.shape[1]
    num_heads = width // head_dim
    tile = 128
    sds = jax.ShapeDtypeStruct

    def whole(x):
        return pl.BlockSpec(x.shape, lambda i: (0,) * len(x.shape))

    def by_col(n):
        return pl.BlockSpec((n, tile), lambda i: (0, i))

    def by_row(n):
        return pl.BlockSpec((tile, n), lambda i: (i, 0))

    gain = sds((1, dim), F32)
    return pl.pallas_call(
        grads_kernel, grid=(dim // tile,),
        out_shape=[sds((num_heads, dim, head_dim), F32), sds((dim, head_dim), F32), sds((dim, head_dim), F32), sds((width, dim), F32),
                   sds((dim, ffn), F32), sds((dim, ffn), F32), sds((ffn, dim), F32), sds((rows_local, dim), F32),
                   sds(hidden.shape, BF), gain, gain],
        in_specs=[by_col(seq), by_col(seq), whole(dqkv), pl.BlockSpec((seq, ffn), lambda i: (0, 0)),
                  pl.BlockSpec((seq, ffn), lambda i: (0, 1)), whole(heads), whole(act), by_col(seq), by_col(seq),
                  whole(tokens), by_col(seq), whole(hidden), whole(gains)],
        out_specs=[pl.BlockSpec((num_heads, tile, head_dim), lambda i: (0, i, 0)), by_row(head_dim), by_row(head_dim), by_col(width),
                   by_row(ffn), by_row(ffn), by_col(ffn), by_col(rows_local), whole(hidden), whole(gain), whole(gain)],
        scratch_shapes=[pltpu.VMEM((rows_local, seq), BF)],
        compiler_params=pltpu.CompilerParams(vmem_limit_bytes=VMEM_FULL),
        name='grads',
    )(n1, n2, dqkv, dgu, dgu, heads, act, dh1, gh, tokens, dx, hidden, gains)


def solution(mesh):
    if mesh.shape['tp'] != CHIPS * CORES:
        raise ValueError('tp size')
    in_specs = (P('dp', None), P('dp', None), P('tp', None), P(None), P(None),
                P(None, 'tp', None), P(None, 'tp', None), P(None, 'tp', None), P('tp', None, None),
                P(None, 'tp'), P(None, 'tp'), P('tp', None), P('dp', 'tp', None))
    out_specs = (P('dp', 'tp', None), P(('dp', 'tp'), None),
                 P('dp', 'tp', None), P('dp', 'tp', None), P('dp', 'tp', None), P(('dp', 'tp'), None, None),
                 P('dp', 'tp'), P('dp', 'tp'), P(('dp', 'tp'), None), P('dp'), P('dp'))

    def device_fn(tokens, positions, emb_shard, gain_attn, gain_mlp, w_query, w_key, w_value, w_out, w_gate, w_up, w_down, grad_hidden):
        rows_local, dim = emb_shard.shape
        seq = tokens.shape[1]
        num_heads, head_dim = w_query.shape[1], w_query.shape[2]
        wq = jnp.transpose(w_query, (1, 0, 2))
        wk, wv = w_key.reshape(dim, head_dim), w_value.reshape(dim, head_dim)
        wo = w_out.reshape(num_heads * head_dim, dim)

        hidden, gains, n1, n2, gh, dh1, dx, heads, act, dgu, dqkv = layer(
            tokens, positions, gain_attn[None, :], gain_mlp[None, :], grad_hidden[0], emb_shard, wq, wk, wv, wo, w_gate, w_up, w_down)
        n1, n2, gh, dh1, dx = (x.reshape(seq, dim) for x in (n1, n2, gh, dh1, dx))
        gw_query, gw_key, gw_value, gw_out, gw_gate, gw_up, gw_down, g_emb, hidden, g_attn, g_mlp = grads(
            n1, n2, dqkv, dgu, heads, act, dh1, gh, tokens, dx, hidden, gains, rows_local, head_dim)
        return (hidden[None], g_emb, jnp.transpose(gw_query, (1, 0, 2)), gw_key.reshape(dim, 1, head_dim),
                gw_value.reshape(dim, 1, head_dim), gw_out.reshape(num_heads, head_dim, dim),
                gw_gate, gw_up, gw_down, g_attn[0], g_mlp[0])

    return jax.shard_map(device_fn, mesh=mesh, in_specs=in_specs, out_specs=out_specs, check_vma=False)
```

```python
import jax
import jax.numpy as jnp
import numpy as np
from jax import lax
from jax.experimental import pallas as pl
from jax.experimental.pallas import tpu as pltpu
from jax.sharding import PartitionSpec as P

ROPE_THETA = 1000000.0
RMS_EPS = 1e-5
BF = jnp.bfloat16
F32 = jnp.float32
VMEM_FULL = 67043328
CHIPS = 4
CORES = 2


def dot(a, b):
    return lax.dot_general(a, b, (((1,), (0,)), ((), ())), preferred_element_type=F32)


def dot_bt(a, b):
    return lax.dot_general(a, b, (((1,), (1,)), ((), ())), preferred_element_type=F32)


def dot_at(a, b):
    return lax.dot_general(a, b, (((0,), (0,)), ((), ())), preferred_element_type=F32)


class Place:
    def __init__(self):
        me = lax.axis_index('tp')
        self.chip, self.core = me // CORES, me % CORES
        self.right_chip = (self.chip + 1) % CHIPS
        self.left_chip = (self.chip + CHIPS - 1) % CHIPS
        self.far_chip = (self.chip + 2) % CHIPS
        self.me = me
        self.other = 1 - self.core
        self.partner = self.chip * CORES + self.other
        self.right = self.right_chip * CORES + self.core
        self.left = self.left_chip * CORES + self.core
        self.far = self.far_chip * CORES + self.core


def remote(src, dst, send, recv, device):
    return pltpu.make_async_remote_copy(src_ref=src, dst_ref=dst, send_sem=send, recv_sem=recv,
                                        device_id={'tp': device}, device_id_type=pl.DeviceIdType.MESH)


def entry_barrier(pos):
    barrier = pltpu.get_barrier_semaphore()
    for device in (pos.left, pos.right, pos.partner):
        pl.semaphore_signal(barrier, inc=1, device_id={'tp': device}, device_id_type=pl.DeviceIdType.MESH)
    pl.semaphore_wait(barrier, 3)


class Gather:
    def __init__(self, pos, buf, send, recv):
        self.pos, self.buf = pos, buf
        half = buf.shape[-1] // 2
        p = pos
        other = p.other - p.core

        def piece(slot, part):
            if part == 2:
                return buf.at[slot]
            return buf.at[slot, :, pl.ds(part * half, half)]

        def copy(index, slot, part, device):
            ref = piece(slot, part)
            return remote(ref, ref, send.at[index], recv.at[index], device)

        plan = {
            0: ((p.me, 0, p.right), (p.left, 0)), 1: ((p.me, 1, p.left), (p.right, 1)),
            2: ((p.me, 2, p.partner), (p.partner, 2)),
            3: ((p.me, 1, p.right), (p.left, 1)), 4: ((p.me, 0, p.left), (p.right, 0)),
            5: ((p.left, 0, p.right), (p.far, 0)), 6: ((p.right, 1, p.left), (p.far, 1)),
            7: ((p.left, 0, p.partner), (p.left + other, 0)), 8: ((p.right, 1, p.partner), (p.right + other, 1)),
            9: ((p.left, 1, p.partner), (p.left + other, 1)), 10: ((p.right, 0, p.partner), (p.right + other, 0)),
            11: ((p.far, 0, p.partner), (p.far + other, 0)), 12: ((p.far, 1, p.partner), (p.far + other, 1)),
        }
        self.out = {i: copy(i, *s) for i, (s, _) in plan.items()}
        self.into = {i: copy(i, slot, part, p.partner) for i, (_, (slot, part)) in plan.items()}

    def start(self):
        for i in (0, 1, 2, 3, 4):
            self.out[i].start()

    def relay(self):
        for i, onward in ((0, (5, 7)), (1, (6, 8)), (3, (9,)), (4, (10,))):
            self.into[i].wait_recv()
            for j in onward:
                self.out[j].start()

    def finish(self):
        for i, j in ((5, 11), (6, 12)):
            self.into[i].wait_recv()
            self.out[j].start()
        for i in (2, 7, 8, 9, 10, 11, 12):
            self.into[i].wait_recv()

    def drain(self):
        for i in range(13):
            self.out[i].wait_send()


class Scatter:
    def __init__(self, pos, part, from_partner, work, arrive, send, recv):
        p = pos
        self.pos, self.part, self.from_partner, self.work, self.arrive = p, part, from_partner, work, arrive
        self.half = work.shape[-1]
        self.chips = (p.far_chip, p.right_chip, p.left_chip, p.chip)
        self.inner = [[remote(part.at[p.other, y, :, self.cols(h)], from_partner.at[y, :, self.cols(h)],
                              send.at[4 * h + k], recv.at[4 * h + k], p.partner) for k, y in enumerate(self.chips)]
                      for h in range(2)]
        self.outer = [remote(work.at[k], arrive.at[k], send.at[8 + k], recv.at[8 + k], p.right if k % 2 == 0 else p.left)
                      for k in range(6)]

    def cols(self, h):
        return pl.ds(h * self.half, self.half)

    def pair(self, k, h):
        y = self.chips[k]
        return self.part[self.pos.core, y, :, self.cols(h)].astype(F32) + self.from_partner[y, :, self.cols(h)].astype(F32)

    def send_sum(self, k, value):
        self.work[k] = value.astype(BF)
        self.outer[k].start()

    def start(self, h):
        for copy in self.inner[h]:
            copy.start()

    def relay_low(self):
        self.inner[0][0].wait_recv()
        self.send_sum(0, self.pair(0, 0))
        self.inner[0][2].wait_recv()
        self.send_sum(3, self.pair(2, 0))

    def relay_high(self):
        self.inner[1][0].wait_recv()
        self.send_sum(1, self.pair(0, 1))
        self.inner[1][1].wait_recv()
        self.send_sum(2, self.pair(1, 1))

    def relay_far(self):
        self.inner[0][1].wait_recv()
        self.outer[0].wait_recv()
        self.send_sum(4, self.pair(1, 0) + self.arrive[0].astype(F32))
        self.inner[1][2].wait_recv()
        self.outer[1].wait_recv()
        self.send_sum(5, self.pair(2, 1) + self.arrive[1].astype(F32))

    def finish(self):
        self.inner[0][3].wait_recv()
        self.inner[1][3].wait_recv()
        for k in (2, 3, 4, 5):
            self.outer[k].wait_recv()
        low = self.pair(3, 0) + self.arrive[3].astype(F32) + self.arrive[4].astype(F32)
        high = self.pair(3, 1) + self.arrive[2].astype(F32) + self.arrive[5].astype(F32)
        return jnp.concatenate([low, high], axis=-1)

    def drain(self):
        for copy in self.inner[0] + self.inner[1] + self.outer:
            copy.wait_send()


GATHER_SEMS = [pltpu.SemaphoreType.DMA((13,)), pltpu.SemaphoreType.DMA((13,))]
SCATTER_SEMS = [pltpu.SemaphoreType.DMA((14,)), pltpu.SemaphoreType.DMA((14,))]


def scatter_scratch(rows, dim):
    return [pltpu.VMEM((CHIPS, rows, dim), BF), pltpu.VMEM((6, rows, dim // 2), BF),
            pltpu.VMEM((6, rows, dim // 2), BF)]


def put_part(part, value, col):
    rows, width = part.shape[2], value.shape[1]
    for b in range(CHIPS * CORES):
        part[b % CORES, b // CORES, :, pl.ds(col, width)] = value[b * rows:(b + 1) * rows].astype(BF)


def norm_stats(hidden_f):
    inv_rms = lax.rsqrt(jnp.mean(hidden_f * hidden_f, axis=-1, keepdims=True) + RMS_EPS)
    return hidden_f * inv_rms, inv_rms


def norm_bwd(grad_f, normed, inv_rms, gain):
    gain_part = jnp.sum(grad_f * normed, axis=0, keepdims=True)
    scaled = grad_f * gain
    return inv_rms * (scaled - normed * jnp.mean(scaled * normed, axis=-1, keepdims=True)), gain_part


def rope(values, cos2, sin2):
    return values * cos2 + pltpu.roll(values, values.shape[-1] // 2, axis=1) * sin2


def full(buf):
    blocks, rows, dim = buf.shape
    return buf[...].reshape(blocks * rows, dim)


def rope_tables(pos_row, freq_col):
    angles = jnp.transpose(freq_col * pos_row.astype(F32))
    lane = lax.broadcasted_iota(jnp.int32, angles.shape, 1)
    sin = jnp.sin(angles)
    return jnp.cos(angles), jnp.where(lane < angles.shape[1] // 2, -sin, sin)


def layer_kernel(tokens, positions, freq, gain_attn, gain_mlp, grad_own, emb_hbm, wq_hbm, wk_hbm, wv_hbm, wo_hbm, wg_hbm, wu_hbm, wd_hbm,
                 dx_own, hidden_out, n1_out, n2_out, gh_out, dh1_out, heads_out, act_out, dgu_out, dqkv_out,
                 emb, pick_buf, wqkv, wqkv_t, wo, wg, wu, wd, wsem, osem, n1_buf, n2_buf, gh_buf, dh1_buf,
                 emb_part, attn_part, dn2_part, mlp_part, dn1_part, heads_buf, gact, act_buf, dgu_buf, dqkv_buf,
                 q_buf, probs_buf, cos_ref, sin_ref, hidden_buf, *comm):
    pos = Place()
    num_heads, dim, head_dim = wq_hbm.shape
    rows_local = emb_hbm.shape[0]
    blocks, rows, _ = n1_buf.shape
    seq, ffn = blocks * rows, wg.shape[1]
    scatters = [comm[3 * i:3 * i + 3] for i in range(5)]
    main_s, side_s, main_g, side_g = (comm[15 + 2 * i:17 + 2 * i] for i in range(4))
    kq = num_heads * head_dim
    step = 512
    chunks = dim // step
    wide = dim // 2

    def emb_load(j):
        cols = pl.ds(pl.multiple_of(j * step, step), step)
        return pltpu.make_async_copy(emb_hbm.at[:, cols], emb.at[:, cols], wsem.at[j])

    for j in range(chunks):
        emb_load(j).start()
    pairs = [(wq_hbm.at[h], wqkv.at[:, pl.ds(h * head_dim, head_dim)]) for h in range(num_heads)]
    pairs += [(wk_hbm, wqkv.at[:, pl.ds(kq, head_dim)]), (wv_hbm, wqkv.at[:, pl.ds(kq + head_dim, head_dim)])]
    pairs += [(wo_hbm, wo), (wd_hbm, wd), (wg_hbm, wg), (wu_hbm, wu)]
    loads = [pltpu.make_async_copy(src, dst, wsem.at[chunks + k]) for k, (src, dst) in enumerate(pairs)]
    for load in loads:
        load.start()
    stores = []

    def store(src, dst):
        stores.append(pltpu.make_async_copy(src, dst, osem.at[len(stores)]))
        stores[-1].start()

    def halves(scatter, product):
        for h in range(2):
            put_part(scatter.part, product(h * wide), h * wide)
            scatter.start(h)

    def turn(src, dst, first):
        @pl.loop(0, src.shape[0] // 128)
        def _(j):
            at = pl.multiple_of(j * 128, 128)
            dst[first:first + src.shape[1], pl.ds(at, 128)] = jnp.transpose(src[pl.ds(at, 128), :])

    gh_buf[pos.me] = grad_own[...]
    with jax.named_scope('barrier'):
        entry_barrier(pos)
    gather0 = Gather(pos, gh_buf, *side_g)
    gather0.start()

    with jax.named_scope('lookup'):
        local = jnp.transpose(jnp.broadcast_to(tokens[...] - pos.me * rows_local, (seq, seq)))
        lane = lax.broadcasted_iota(jnp.int32, (seq, seq), 1)
        for j in range(rows_local // seq):
            pick_buf[:, j * seq:(j + 1) * seq] = jnp.where(local == lane + j * seq, 1.0, 0.0).astype(BF)
        cos_ref[...], sin_ref[...] = rope_tables(positions[...], freq[...])

        scatter1 = Scatter(pos, emb_part, *scatters[0], *main_s)
        for h in range(2):
            @pl.loop(h * chunks // 2, (h + 1) * chunks // 2)
            def _(j):
                col = pl.multiple_of(j * step, step)
                emb_load(j).wait()
                put_part(scatter1.part, dot(pick_buf[...], emb[:, pl.ds(col, step)]), col)

            scatter1.start(h)
    with jax.named_scope('rs1'):
        scatter1.relay_low()
        scatter1.relay_high()
        gather0.relay()
        scatter1.relay_far()
        gather0.finish()
        x0 = scatter1.finish()
    with jax.named_scope('norm1'):
        normed1, inv1 = norm_stats(x0)
        n1_buf[pos.me] = (normed1 * gain_attn[...]).astype(BF)
    with jax.named_scope('ag1'):
        gather1 = Gather(pos, n1_buf, *main_g)
        gather1.start()
        store(gh_buf, gh_out)
    with jax.named_scope('turn_gate'):
        loads[7].wait()
        turn(wg, emb, 0)
    with jax.named_scope('ag1_relay'):
        gather1.relay()
    with jax.named_scope('turn_up'):
        loads[8].wait()
        turn(wu, emb, ffn)
    with jax.named_scope('ag1_finish'):
        gather1.finish()
    store(n1_buf, n1_out)

    with jax.named_scope('qkv'):
        for load in loads[:5]:
            load.wait()
        qkv = dot(full(n1_buf), wqkv[...])
    with jax.named_scope('attention'):
        cos2, sin2 = cos_ref[...], sin_ref[...]
        keys = rope(qkv[:, kq:kq + head_dim], cos2, sin2).astype(BF)
        values = qkv[:, kq + head_dim:].astype(BF)
        causal = lax.broadcasted_iota(jnp.int32, (seq, seq), 0) >= lax.broadcasted_iota(jnp.int32, (seq, seq), 1)
        for h in range(num_heads):
            cols = slice(h * head_dim, (h + 1) * head_dim)
            query = rope(qkv[:, cols], cos2, sin2).astype(BF)
            q_buf[:, cols] = query
            scores = jnp.where(causal, dot_bt(query, keys) * (head_dim ** -0.5), -1e30)
            expd = jnp.exp(scores - jnp.max(scores, axis=-1, keepdims=True))
            probs = expd / jnp.sum(expd, axis=-1, keepdims=True)
            probs_buf[h] = probs
            heads_buf[:, cols] = dot(probs.astype(BF), values).astype(BF)
    store(heads_buf, heads_out)
    with jax.named_scope('w_out'):
        loads[5].wait()
        scatter3 = Scatter(pos, attn_part, *scatters[1], *main_s)
        scatter1.drain()
        halves(scatter3, lambda col: dot(heads_buf[...], wo[:, pl.ds(col, wide)]))

    with jax.named_scope('rs3_a'):
        scatter3.relay_low()
        scatter3.relay_high()

    with jax.named_scope('grad_act'):
        loads[6].wait()

        @pl.loop(0, ffn // 256)
        def _(j):
            cols = pl.ds(pl.multiple_of(j * 256, 256), 256)
            gact[:, cols] = dot_bt(full(gh_buf), wd[cols, :]).astype(BF)

    with jax.named_scope('rs3_b'):
        scatter3.relay_far()
        h1_bf = (x0 + scatter3.finish()).astype(BF)
    with jax.named_scope('norm2'):
        h1 = h1_bf.astype(F32)
        normed2, inv2 = norm_stats(h1)
        n2_buf[pos.me] = (normed2 * gain_mlp[...]).astype(BF)
    with jax.named_scope('ag4'):
        gather4 = Gather(pos, n2_buf, *main_g)
        gather1.drain()
        gather4.start()
        turn(wqkv, wqkv_t, 0)
        gather4.relay()
        gather4.finish()
    store(n2_buf, n2_out)

    with jax.named_scope('gate_up'):
        @pl.loop(0, ffn // 512)
        def _(j):
            cols = pl.ds(pl.multiple_of(j * 512, 512), 512)
            n2 = full(n2_buf)
            gate_pre = dot(n2, wg[:, cols])
            up_pre = dot(n2, wu[:, cols])
            sig = jax.nn.sigmoid(gate_pre)
            gate_act = gate_pre * sig
            act_buf[:, cols] = (gate_act * up_pre).astype(BF)
            grad_act = gact[:, cols].astype(F32)
            dgu_buf[:, pl.ds(pl.multiple_of(ffn + j * 512, 512), 512)] = (grad_act * gate_act).astype(BF)
            dgu_buf[:, cols] = (grad_act * up_pre * sig * (1.0 + gate_pre * (1.0 - sig))).astype(BF)

    store(act_buf, act_out)
    store(dgu_buf, dgu_out)
    with jax.named_scope('dn2'):
        scatter6 = Scatter(pos, dn2_part, *scatters[2], *main_s)
        scatter3.drain()
        halves(scatter6, lambda col: dot(dgu_buf[...], emb[:, pl.ds(col, wide)]))

    with jax.named_scope('rs6'):
        scatter6.relay_low()
        scatter6.relay_high()
        scatter6.relay_far()
        grad_n2 = scatter6.finish().astype(BF).astype(F32)
    with jax.named_scope('norm2_bwd'):
        grad_h1_norm, gain_mlp_part = norm_bwd(grad_n2, normed2, inv2, gain_mlp[...])
        grad_h1 = (grad_own[...].astype(F32) + grad_h1_norm).astype(BF)
        dh1_buf[pos.me] = grad_h1
    gather7 = Gather(pos, dh1_buf, *main_g)
    gather4.drain()
    gather7.start()
    with jax.named_scope('w_down'):
        @pl.loop(0, chunks)
        def _(j):
            col = pl.multiple_of(j * step, step)
            put_part(mlp_part, dot(act_buf[...], wd[:, pl.ds(col, step)]), col)

    scatter5 = Scatter(pos, mlp_part, *scatters[3], *side_s)
    with jax.named_scope('ag7'):
        gather7.relay()
        scatter5.start(0)
        scatter5.start(1)
        gather7.finish()
    with jax.named_scope('rs5_relay'):
        scatter5.relay_low()
        scatter5.relay_high()
    store(dh1_buf, dh1_out)

    with jax.named_scope('dheads'):
        dheads = dot_bt(full(dh1_buf), wo[...]).astype(BF)
    with jax.named_scope('attention_bwd'):
        nsin2 = -sin2
        dkeys = jnp.zeros((seq, head_dim), F32)
        dvalues = jnp.zeros((seq, head_dim), F32)
        for h in range(num_heads):
            cols = slice(h * head_dim, (h + 1) * head_dim)
            dhead = dheads[:, cols]
            probs = probs_buf[h]
            dprobs = dot_bt(dhead, values).astype(BF).astype(F32)
            dvalues += dot_at(probs.astype(BF), dhead)
            inner = jnp.sum(dprobs * probs, axis=-1, keepdims=True)
            dscores = (probs * (dprobs - inner) * (head_dim ** -0.5)).astype(BF)
            dquery = dot(dscores, keys).astype(BF)
            dkeys += dot_at(dscores, q_buf[:, cols])
            dqkv_buf[:, cols] = rope(dquery.astype(F32), cos2, nsin2).astype(BF)
        dqkv_buf[:, kq:kq + head_dim] = rope(dkeys.astype(BF).astype(F32), cos2, nsin2).astype(BF)
        dqkv_buf[:, kq + head_dim:] = dvalues.astype(BF)
    store(dqkv_buf, dqkv_out)

    with jax.named_scope('dn1'):
        scatter8 = Scatter(pos, dn1_part, *scatters[4], *main_s)
        scatter6.drain()
        halves(scatter8, lambda col: dot(dqkv_buf[...], wqkv_t[:, pl.ds(col, wide)]))

    with jax.named_scope('rs8'):
        scatter8.relay_low()
        scatter8.relay_high()
        scatter5.relay_far()
        scatter8.relay_far()
        hidden_buf[...] = (h1 + scatter5.finish()).astype(BF)
        store(hidden_buf, hidden_out)
        grad_n1 = scatter8.finish().astype(BF).astype(F32)
    with jax.named_scope('norm1_bwd'):
        grad_x_norm, gain_attn_part = norm_bwd(grad_n1, normed1, inv1, gain_attn[...])
        dx_own[0:rows, :] = (grad_h1.astype(F32) + grad_x_norm).astype(BF)
        gain_parts = jnp.concatenate([gain_attn_part, gain_mlp_part], axis=0)
        high = gain_parts.astype(BF)
        dx_own[rows:rows + 2, :] = high
        dx_own[rows + 2:rows + 4, :] = (gain_parts - high.astype(F32)).astype(BF)
    with jax.named_scope('tail'):
        for op in (gather0, scatter5, scatter8, gather7):
            op.drain()
        for copy in stores:
            copy.wait()


def layer(tokens, positions, gain_attn, gain_mlp, grad_own, emb, wq, wk, wv, wo, wg, wu, wd):
    num_heads, dim, head_dim = wq.shape
    blocks = CHIPS * CORES
    seq, ffn, rows_local = tokens.shape[1], wg.shape[1], emb.shape[0]
    rows = seq // blocks
    if rows_local != 2 * ffn:
        raise ValueError('shard rows')
    half = head_dim // 2
    freq = np.float32(ROPE_THETA) ** (-np.arange(half, dtype=np.float32) * np.float32(2.0 / head_dim))
    freq = jnp.asarray(np.concatenate([freq, freq])[:, None], F32)
    vmem = pl.BlockSpec(memory_space=pltpu.VMEM)
    hbm = pl.BlockSpec(memory_space=pltpu.HBM)
    width = num_heads * head_dim
    wide = width + 2 * head_dim
    sds = jax.ShapeDtypeStruct
    outs = [sds((rows + 4, dim), BF), sds((rows, dim), BF)] + [sds((blocks, rows, dim), BF)] * 4
    outs += [sds((seq, width), BF), sds((seq, ffn), BF), sds((seq, 2 * ffn), BF), sds((seq, wide), BF)]
    part = pltpu.VMEM((CORES, CHIPS, rows, dim), BF)
    gathered = pltpu.VMEM((blocks, rows, dim), BF)
    table = pltpu.VMEM((seq, head_dim), F32)
    scratch = [pltpu.VMEM((rows_local, dim), BF), pltpu.VMEM((seq, rows_local), BF), pltpu.VMEM((dim, wide), BF), pltpu.VMEM((wide, dim), BF),
               pltpu.VMEM((width, dim), BF), pltpu.VMEM((dim, ffn), BF),
               pltpu.VMEM((dim, ffn), BF), pltpu.VMEM((ffn, dim), BF), pltpu.SemaphoreType.DMA((15,)), pltpu.SemaphoreType.DMA((9,))]
    scratch += [gathered] * 4 + [part] * 5 + [pltpu.VMEM((seq, width), BF)]
    scratch += [pltpu.VMEM((seq, ffn), BF)] * 2 + [pltpu.VMEM((seq, 2 * ffn), BF), pltpu.VMEM((seq, wide), BF), pltpu.VMEM((seq, width), BF),
                                                   pltpu.VMEM((num_heads, seq, seq), F32), table, table,
                                                   pltpu.VMEM((rows, dim), BF)]
    scratch += scatter_scratch(rows, dim) * 5 + SCATTER_SEMS * 2 + GATHER_SEMS * 2
    return pl.pallas_call(
        layer_kernel, out_shape=outs, in_specs=[vmem] * 6 + [hbm] * 8, out_specs=[vmem] + [hbm] * 9,
        scratch_shapes=scratch,
        compiler_params=pltpu.CompilerParams(collective_id=0, has_side_effects=True, vmem_limit_bytes=VMEM_FULL),
        name='layer',
    )(tokens, positions, freq, gain_attn, gain_mlp, grad_own, emb, wq, wk, wv, wo, wg, wu, wd)


def grads_kernel(n1, n2, dqkv, dgate, dup, heads, act, dh1, gh, hidden_in,
                 gw_query, gw_key, gw_value, gw_out, gw_gate, gw_up, gw_down, hidden):
    num_heads, _, head_dim = gw_query.shape
    width = num_heads * head_dim

    @pl.when(pl.program_id(0) == 0)
    def _():
        hidden[...] = hidden_in[...]

    gw_gate[...] = dot_at(n2[...], dgate[...])
    gw_up[...] = dot_at(n2[...], dup[...])
    gw_down[...] = dot_at(act[...], gh[...])
    both = dot_at(n1[...], dqkv[...])
    for h in range(num_heads):
        gw_query[h] = both[:, h * head_dim:(h + 1) * head_dim]
    gw_key[...] = both[:, width:width + head_dim]
    gw_value[...] = both[:, width + head_dim:]
    gw_out[...] = dot_at(heads[...], dh1[...])


def grads(n1, n2, dqkv, dgu, heads, act, dh1, gh, hidden, head_dim):
    seq, dim = n1.shape
    width, ffn = heads.shape[1], act.shape[1]
    num_heads = width // head_dim
    tile = 256
    sds = jax.ShapeDtypeStruct

    def whole(x):
        return pl.BlockSpec(x.shape, lambda i: (0,) * len(x.shape))

    def by_col(n):
        return pl.BlockSpec((n, tile), lambda i: (0, i))

    def by_row(n):
        return pl.BlockSpec((tile, n), lambda i: (i, 0))

    return pl.pallas_call(
        grads_kernel, grid=(dim // tile,),
        out_shape=[sds((num_heads, dim, head_dim), F32), sds((dim, head_dim), F32), sds((dim, head_dim), F32), sds((width, dim), F32),
                   sds((dim, ffn), F32), sds((dim, ffn), F32), sds((ffn, dim), F32), sds(hidden.shape, BF)],
        in_specs=[by_col(seq), by_col(seq), whole(dqkv), pl.BlockSpec((seq, ffn), lambda i: (0, 0)),
                  pl.BlockSpec((seq, ffn), lambda i: (0, 1)), whole(heads), whole(act), by_col(seq), by_col(seq), whole(hidden)],
        out_specs=[pl.BlockSpec((num_heads, tile, head_dim), lambda i: (0, i, 0)), by_row(head_dim), by_row(head_dim), by_col(width),
                   by_row(ffn), by_row(ffn), by_col(ffn), whole(hidden)],
        compiler_params=pltpu.CompilerParams(vmem_limit_bytes=VMEM_FULL),
        cost_estimate=pl.CostEstimate(flops=20_000_000_000, bytes_accessed=50_000_000, transcendentals=0),
        name='grads',
    )(n1, n2, dqkv, dgu, dgu, heads, act, dh1, gh, hidden)


def emb_grad_kernel(tokens, *refs):
    blocks = refs[:CHIPS * CORES]
    g_emb, g_attn, g_mlp, dx, gains = refs[CHIPS * CORES:]
    rows = dx.shape[0] // len(blocks)
    me = lax.axis_index('tp')

    @pl.when(pl.program_id(0) == 0)
    def _():
        for k, block in enumerate(blocks):
            source = (me + len(blocks) - k) % len(blocks)
            dx[pl.ds(pl.multiple_of(source * rows, rows), rows), :] = block[0:rows, :]
            gains[source] = block[rows:rows + 2, :].astype(F32) + block[rows + 2:rows + 4, :].astype(F32)
        total = gains[0]
        for i in range(1, len(blocks)):
            total = total + gains[i]
        g_attn[...] = total[0:1, :]
        g_mlp[...] = total[1:2, :]

    height, seq = g_emb.shape[0], dx.shape[0]
    first = me * (height * pl.num_programs(0)) + pl.program_id(0) * height
    row = lax.broadcasted_iota(jnp.int32, (height, seq), 0) + first
    g_emb[...] = dot(jnp.where(row == tokens[...], 1.0, 0.0).astype(BF), dx[...])


def emb_grad(tokens, blocks, rows_local):
    seq, dim = tokens.shape[1], blocks[0].shape[1]
    steps = 8
    sds = jax.ShapeDtypeStruct

    def whole(x):
        return pl.BlockSpec(x.shape, lambda i: (0,) * len(x.shape))

    gain = sds((1, dim), F32)
    return pl.pallas_call(
        emb_grad_kernel, grid=(steps,),
        out_shape=[sds((rows_local, dim), F32), gain, gain],
        in_specs=[whole(tokens)] + [whole(x) for x in blocks],
        out_specs=[pl.BlockSpec((rows_local // steps, dim), lambda i: (i, 0)), whole(gain), whole(gain)],
        scratch_shapes=[pltpu.VMEM((seq, dim), BF), pltpu.VMEM((len(blocks), 2, dim), F32)],
        compiler_params=pltpu.CompilerParams(vmem_limit_bytes=VMEM_FULL),
        name='emb_grad',
    )(tokens, *blocks)


def solution(mesh):
    if mesh.shape['tp'] != CHIPS * CORES:
        raise ValueError('tp size')
    in_specs = (P('dp', None), P('dp', None), P('tp', None), P(None), P(None),
                P(None, 'tp', None), P(None, 'tp', None), P(None, 'tp', None), P('tp', None, None),
                P(None, 'tp'), P(None, 'tp'), P('tp', None), P('dp', 'tp', None))
    out_specs = (P('dp', 'tp', None), P(('dp', 'tp'), None),
                 P('dp', 'tp', None), P('dp', 'tp', None), P('dp', 'tp', None), P(('dp', 'tp'), None, None),
                 P('dp', 'tp'), P('dp', 'tp'), P(('dp', 'tp'), None), P('dp'), P('dp'))

    def device_fn(tokens, positions, emb_shard, gain_attn, gain_mlp, w_query, w_key, w_value, w_out, w_gate, w_up, w_down, grad_hidden):
        rows_local, dim = emb_shard.shape
        seq = tokens.shape[1]
        num_heads, head_dim = w_query.shape[1], w_query.shape[2]
        wq = jnp.transpose(w_query, (1, 0, 2))
        wk, wv = w_key.reshape(dim, head_dim), w_value.reshape(dim, head_dim)
        wo = w_out.reshape(num_heads * head_dim, dim)

        dx_own, hidden, n1, n2, gh, dh1, heads, act, dgu, dqkv = layer(
            tokens, positions, gain_attn[None, :], gain_mlp[None, :], grad_hidden[0], emb_shard, wq, wk, wv, wo, w_gate, w_up, w_down)
        n = CHIPS * CORES
        arrived = [dx_own] + [lax.ppermute(dx_own, 'tp', [(i, (i + k) % n) for i in range(n)]) for k in range(1, n)]
        n1, n2, gh, dh1 = (x.reshape(seq, dim) for x in (n1, n2, gh, dh1))
        gw_query, gw_key, gw_value, gw_out, gw_gate, gw_up, gw_down, hidden = grads(
            n1, n2, dqkv, dgu, heads, act, dh1, gh, hidden, head_dim)
        g_emb, g_attn, g_mlp = emb_grad(tokens, arrived, rows_local)
        return (hidden[None], g_emb, jnp.transpose(gw_query, (1, 0, 2)), gw_key.reshape(dim, 1, head_dim),
                gw_value.reshape(dim, 1, head_dim), gw_out.reshape(num_heads, head_dim, dim),
                gw_gate, gw_up, gw_down, g_attn[0], g_mlp[0])

    return jax.shard_map(device_fn, mesh=mesh, in_specs=in_specs, out_specs=out_specs, check_vma=False)
```

```python
import jax
import jax.numpy as jnp
import numpy as np
from jax import lax
from jax.experimental import pallas as pl
from jax.experimental.pallas import tpu as pltpu
from jax.sharding import PartitionSpec as P

ROPE_THETA = 1000000.0
RMS_EPS = 1e-5
BF = jnp.bfloat16
F32 = jnp.float32
VMEM_FULL = 67043328
CHIPS = 4
CORES = 2


def dot(a, b):
    return lax.dot_general(a, b, (((1,), (0,)), ((), ())), preferred_element_type=F32)


def dot_bt(a, b):
    return lax.dot_general(a, b, (((1,), (1,)), ((), ())), preferred_element_type=F32)


def dot_at(a, b):
    return lax.dot_general(a, b, (((0,), (0,)), ((), ())), preferred_element_type=F32)


class Place:
    def __init__(self):
        me = lax.axis_index('tp')
        self.chip, self.core = me // CORES, me % CORES
        self.right_chip = (self.chip + 1) % CHIPS
        self.left_chip = (self.chip + CHIPS - 1) % CHIPS
        self.far_chip = (self.chip + 2) % CHIPS
        self.me = me
        self.other = 1 - self.core
        self.partner = self.chip * CORES + self.other
        self.right = self.right_chip * CORES + self.core
        self.left = self.left_chip * CORES + self.core
        self.far = self.far_chip * CORES + self.core


def remote(src, dst, send, recv, device):
    return pltpu.make_async_remote_copy(src_ref=src, dst_ref=dst, send_sem=send, recv_sem=recv,
                                        device_id={'tp': device}, device_id_type=pl.DeviceIdType.MESH)


def announce(pos):
    barrier = pltpu.get_barrier_semaphore()
    for device in (pos.left, pos.right, pos.partner):
        pl.semaphore_signal(barrier, inc=1, device_id={'tp': device}, device_id_type=pl.DeviceIdType.MESH)
    return barrier


class Gather:
    COPIES = 19

    def __init__(self, pos, buf, send, recv):
        p = pos
        quarter = buf.shape[-1] // 4
        other = p.other - p.core
        low, high, whole = (0, 2), (2, 4), (0, 4)
        pieces = ((0, 1), (1, 2), (2, 3), (3, 4))

        def copy(index, slot, part, device):
            ref = buf.at[slot, :, pl.ds(part[0] * quarter, (part[1] - part[0]) * quarter)]
            return remote(ref, ref, send.at[index], recv.at[index], device)

        plan = [((p.me, pieces[0], p.right), (p.left, pieces[0])), ((p.me, pieces[2], p.left), (p.right, pieces[2])),
                ((p.me, pieces[1], p.right), (p.left, pieces[1])), ((p.me, pieces[3], p.left), (p.right, pieces[3])),
                ((p.me, whole, p.partner), (p.partner, whole)),
                ((p.me, high, p.right), (p.left, high)), ((p.me, low, p.left), (p.right, low)),
                ((p.left, pieces[0], p.right), (p.far, pieces[0])), ((p.right, pieces[2], p.left), (p.far, pieces[2])),
                ((p.left, pieces[1], p.right), (p.far, pieces[1])), ((p.right, pieces[3], p.left), (p.far, pieces[3])),
                ((p.left, low, p.partner), (p.left + other, low)), ((p.right, high, p.partner), (p.right + other, high)),
                ((p.left, high, p.partner), (p.left + other, high)), ((p.right, low, p.partner), (p.right + other, low))]
        plan += [((p.far, pieces[i], p.partner), (p.far + other, pieces[i])) for i in (0, 2, 1, 3)]
        self.out = [copy(i, *sent) for i, (sent, _) in enumerate(plan)]
        self.into = [copy(i, slot, part, p.partner) for i, (_, (slot, part)) in enumerate(plan)]

    def start(self):
        for i in range(7):
            self.out[i].start()

    def pass_on(self, steps):
        for i, onward in steps:
            self.into[i].wait_recv()
            for j in onward:
                self.out[j].start()

    def relay(self):
        self.pass_on(((0, (7,)), (1, (8,)), (2, (9, 11)), (3, (10, 12)), (5, (13,)), (6, (14,))))

    def finish(self):
        self.pass_on(((7, (15,)), (8, (16,)), (9, (17,)), (10, (18,))))
        for i in (4, 11, 12, 13, 14, 15, 16, 17, 18):
            self.into[i].wait_recv()

    def drain(self):
        for copy in self.out:
            copy.wait_send()


class Scatter:
    COPIES = 18

    def __init__(self, pos, part, from_partner, work, arrive, work_half, arrive_half, send, recv):
        p = pos
        self.pos, self.part, self.from_partner = p, part, from_partner
        self.work, self.arrive, self.work_half, self.arrive_half = work, arrive, work_half, arrive_half
        self.quarter = work.shape[-1]
        self.chips = (p.far_chip, p.right_chip, p.left_chip, p.chip)
        self.inner = [[remote(part.at[p.other, y, :, self.cols(2 * h, 2)], from_partner.at[y, :, self.cols(2 * h, 2)],
                              send.at[4 * h + k], recv.at[4 * h + k], p.partner) for k, y in enumerate(self.chips)]
                      for h in range(2)]
        self.outer = [remote(work.at[k], arrive.at[k], send.at[8 + k], recv.at[8 + k], p.right if k % 4 < 2 else p.left)
                      for k in range(8)]
        self.straight = [remote(work_half.at[k], arrive_half.at[k], send.at[16 + k], recv.at[16 + k], device)
                         for k, device in enumerate((p.right, p.left))]

    def cols(self, q, n=1):
        return pl.ds(q * self.quarter, n * self.quarter)

    def pair(self, k, q, n=1):
        y = self.chips[k]
        return self.part[self.pos.core, y, :, self.cols(q, n)].astype(F32) + self.from_partner[y, :, self.cols(q, n)].astype(F32)

    def send_sum(self, k, value):
        self.work[k] = value.astype(BF)
        self.outer[k].start()

    def send_straight(self, k, value):
        self.work_half[k] = value.astype(BF)
        self.straight[k].start()

    def start(self, h):
        for copy in self.inner[h]:
            copy.start()

    def relay_low(self):
        self.inner[0][0].wait_recv()
        self.send_sum(0, self.pair(0, 0))
        self.send_sum(1, self.pair(0, 1))
        self.inner[0][2].wait_recv()
        self.send_straight(1, self.pair(2, 0, 2))

    def relay_high(self):
        self.inner[1][0].wait_recv()
        self.send_sum(2, self.pair(0, 2))
        self.send_sum(3, self.pair(0, 3))
        self.inner[1][1].wait_recv()
        self.send_straight(0, self.pair(1, 2, 2))

    def relay_far(self):
        self.inner[0][1].wait_recv()
        self.inner[1][2].wait_recv()
        for q, k in ((0, 1), (2, 2), (1, 1), (3, 2)):
            self.outer[q].wait_recv()
            self.send_sum(4 + q, self.pair(k, q) + self.arrive[q].astype(F32))

    def finish(self):
        self.inner[0][3].wait_recv()
        self.inner[1][3].wait_recv()
        self.straight[0].wait_recv()
        self.straight[1].wait_recv()
        low = self.pair(3, 0, 2) + self.arrive_half[1].astype(F32)
        high = self.pair(3, 2, 2) + self.arrive_half[0].astype(F32)
        for k in (4, 6, 5, 7):
            self.outer[k].wait_recv()
        far = [self.arrive[4 + q].astype(F32) for q in range(4)]
        return jnp.concatenate([low, high], axis=-1) + jnp.concatenate(far, axis=-1)

    def drain(self):
        for copy in self.inner[0] + self.inner[1] + self.outer + self.straight:
            copy.wait_send()


GATHER_SEMS = [pltpu.SemaphoreType.DMA((Gather.COPIES,))] * 2
SCATTER_SEMS = [pltpu.SemaphoreType.DMA((Scatter.COPIES,))] * 2


def scatter_scratch(rows, dim):
    return [pltpu.VMEM((CHIPS, rows, dim), BF)] + [pltpu.VMEM((8, rows, dim // 4), BF)] * 2 + [pltpu.VMEM((2, rows, dim // 2), BF)] * 2


def put_part(part, value, col):
    rows, width = part.shape[2], value.shape[1]
    for b in range(CHIPS * CORES):
        part[b % CORES, b // CORES, :, pl.ds(col, width)] = value[b * rows:(b + 1) * rows].astype(BF)


def norm_stats(hidden_f):
    inv_rms = lax.rsqrt(jnp.mean(hidden_f * hidden_f, axis=-1, keepdims=True) + RMS_EPS)
    return hidden_f * inv_rms, inv_rms


def norm_bwd(grad_f, normed, inv_rms, gain):
    gain_part = jnp.sum(grad_f * normed, axis=0, keepdims=True)
    scaled = grad_f * gain
    return inv_rms * (scaled - normed * jnp.mean(scaled * normed, axis=-1, keepdims=True)), gain_part


def rope(values, cos2, sin2):
    return values * cos2 + pltpu.roll(values, values.shape[-1] // 2, axis=1) * sin2


def full(buf):
    blocks, rows, dim = buf.shape
    return buf[...].reshape(blocks * rows, dim)


def rope_tables(pos_row, freq_col):
    angles = jnp.transpose(freq_col * pos_row.astype(F32))
    lane = lax.broadcasted_iota(jnp.int32, angles.shape, 1)
    sin = jnp.sin(angles)
    return jnp.cos(angles), jnp.where(lane < angles.shape[1] // 2, -sin, sin)


def layer_kernel(tokens, positions, freq, gain_attn, gain_mlp, grad_own, emb_hbm, wq_hbm, wk_hbm, wv_hbm, wo_hbm, wg_hbm, wu_hbm, wd_hbm,
                 dx_out, hidden_out, n1_out, n2_out, gh_out, dh1_out, heads_out, act_out, dgu_out, dqkv_out,
                 emb, pick_buf, wqkv, wqkv_t, wo, wg, wu, wd, wsem, osem, n1_buf, n2_buf, gh_buf, dh1_buf,
                 emb_part, attn_part, dn2_part, mlp_part, dn1_part, heads_buf, gact, act_buf, dgu_buf, dqkv_buf,
                 q_buf, probs_buf, cos_ref, sin_ref, hidden_buf, dx_pair, *comm):
    pos = Place()
    num_heads, dim, head_dim = wq_hbm.shape
    rows_local = emb_hbm.shape[0]
    blocks, rows, _ = n1_buf.shape
    seq, ffn = blocks * rows, wg.shape[1]
    scatters = [comm[5 * i:5 * i + 5] for i in range(5)]
    main_s, side_s, main_g, side_g, pair_s = (comm[25 + 2 * i:27 + 2 * i] for i in range(5))
    kq = num_heads * head_dim
    step = 512
    chunks = dim // step
    wide = dim // 2

    def emb_load(j):
        cols = pl.ds(pl.multiple_of(j * step, step), step)
        return pltpu.make_async_copy(emb_hbm.at[:, cols], emb.at[:, cols], wsem.at[j])

    for j in range(chunks):
        emb_load(j).start()
    pairs = [(wq_hbm.at[h], wqkv.at[:, pl.ds(h * head_dim, head_dim)]) for h in range(num_heads)]
    pairs += [(wk_hbm, wqkv.at[:, pl.ds(kq, head_dim)]), (wv_hbm, wqkv.at[:, pl.ds(kq + head_dim, head_dim)])]
    pairs += [(wo_hbm, wo), (wd_hbm, wd), (wg_hbm, wg), (wu_hbm, wu)]
    loads = [pltpu.make_async_copy(src, dst, wsem.at[chunks + k]) for k, (src, dst) in enumerate(pairs)]
    for load in loads:
        load.start()
    stores = []

    def store(src, dst):
        stores.append(pltpu.make_async_copy(src, dst, osem.at[len(stores)]))
        stores[-1].start()

    def halves(scatter, product):
        for h in range(2):
            put_part(scatter.part, product(h * wide), h * wide)
            scatter.start(h)

    def turn(src, dst, first):
        @pl.loop(0, src.shape[0] // 128)
        def _(j):
            at = pl.multiple_of(j * 128, 128)
            dst[first:first + src.shape[1], pl.ds(at, 128)] = jnp.transpose(src[pl.ds(at, 128), :])

    barrier = announce(pos)
    gh_buf[pos.me] = grad_own[...]
    gather0 = Gather(pos, gh_buf, *side_g)
    scatter1 = Scatter(pos, emb_part, *scatters[0], *main_s)

    def looked_up(h):
        @pl.loop(h * chunks // 2, (h + 1) * chunks // 2)
        def _(j):
            col = pl.multiple_of(j * step, step)
            emb_load(j).wait()
            put_part(scatter1.part, dot(pick_buf[...], emb[:, pl.ds(col, step)]), col)

    with jax.named_scope('lookup_low'):
        local = jnp.transpose(jnp.broadcast_to(tokens[...] - pos.me * rows_local, (seq, seq)))
        lane = lax.broadcasted_iota(jnp.int32, (seq, seq), 1)
        for j in range(rows_local // seq):
            pick_buf[:, j * seq:(j + 1) * seq] = jnp.where(local == lane + j * seq, 1.0, 0.0).astype(BF)
        looked_up(0)
    with jax.named_scope('barrier'):
        pl.semaphore_wait(barrier, 3)
    scatter1.start(0)
    gather0.start()
    with jax.named_scope('lookup_high'):
        looked_up(1)
        scatter1.start(1)
    with jax.named_scope('rs1'):
        scatter1.relay_low()
        scatter1.relay_high()
        gather0.relay()
        scatter1.relay_far()
        gather0.finish()
        cos_ref[...], sin_ref[...] = rope_tables(positions[...], freq[...])
        x0 = scatter1.finish()
    with jax.named_scope('norm1'):
        normed1, inv1 = norm_stats(x0)
        n1_buf[pos.me] = (normed1 * gain_attn[...]).astype(BF)
    with jax.named_scope('ag1'):
        gather1 = Gather(pos, n1_buf, *main_g)
        gather1.start()
        store(gh_buf, gh_out)
    with jax.named_scope('turn_gate'):
        loads[7].wait()
        turn(wg, emb, 0)
    with jax.named_scope('ag1_relay'):
        gather1.relay()
    with jax.named_scope('turn_up'):
        loads[8].wait()
        turn(wu, emb, ffn)
    with jax.named_scope('ag1_finish'):
        gather1.finish()
    store(n1_buf, n1_out)

    with jax.named_scope('qkv'):
        for load in loads[:5]:
            load.wait()
        qkv = dot(full(n1_buf), wqkv[...])
    with jax.named_scope('attention'):
        cos2, sin2 = cos_ref[...], sin_ref[...]
        keys = rope(qkv[:, kq:kq + head_dim], cos2, sin2).astype(BF)
        values = qkv[:, kq + head_dim:].astype(BF)
        causal = lax.broadcasted_iota(jnp.int32, (seq, seq), 0) >= lax.broadcasted_iota(jnp.int32, (seq, seq), 1)
        for h in range(num_heads):
            cols = slice(h * head_dim, (h + 1) * head_dim)
            query = rope(qkv[:, cols], cos2, sin2).astype(BF)
            q_buf[:, cols] = query
            scores = jnp.where(causal, dot_bt(query, keys) * (head_dim ** -0.5), -1e30)
            expd = jnp.exp(scores - jnp.max(scores, axis=-1, keepdims=True))
            probs = expd / jnp.sum(expd, axis=-1, keepdims=True)
            probs_buf[h] = probs
            heads_buf[:, cols] = dot(probs.astype(BF), values).astype(BF)
    store(heads_buf, heads_out)
    with jax.named_scope('w_out'):
        loads[5].wait()
        scatter3 = Scatter(pos, attn_part, *scatters[1], *main_s)
        scatter1.drain()
        halves(scatter3, lambda col: dot(heads_buf[...], wo[:, pl.ds(col, wide)]))

    with jax.named_scope('rs3_a'):
        scatter3.relay_low()
        scatter3.relay_high()

    with jax.named_scope('grad_act'):
        loads[6].wait()

        @pl.loop(0, ffn // 256)
        def _(j):
            cols = pl.ds(pl.multiple_of(j * 256, 256), 256)
            gact[:, cols] = dot_bt(full(gh_buf), wd[cols, :]).astype(BF)

    with jax.named_scope('rs3_b'):
        scatter3.relay_far()
        h1_bf = (x0 + scatter3.finish()).astype(BF)
    with jax.named_scope('norm2'):
        h1 = h1_bf.astype(F32)
        normed2, inv2 = norm_stats(h1)
        n2_buf[pos.me] = (normed2 * gain_mlp[...]).astype(BF)
    with jax.named_scope('ag4'):
        gather4 = Gather(pos, n2_buf, *main_g)
        gather1.drain()
        gather4.start()
        turn(wqkv, wqkv_t, 0)
        gather4.relay()
        gather4.finish()
    store(n2_buf, n2_out)

    with jax.named_scope('gate_up'):
        @pl.loop(0, ffn // 512)
        def _(j):
            cols = pl.ds(pl.multiple_of(j * 512, 512), 512)
            n2 = full(n2_buf)
            gate_pre = dot(n2, wg[:, cols])
            up_pre = dot(n2, wu[:, cols])
            sig = jax.nn.sigmoid(gate_pre)
            gate_act = gate_pre * sig
            act_buf[:, cols] = (gate_act * up_pre).astype(BF)
            grad_act = gact[:, cols].astype(F32)
            dgu_buf[:, pl.ds(pl.multiple_of(ffn + j * 512, 512), 512)] = (grad_act * gate_act).astype(BF)
            dgu_buf[:, cols] = (grad_act * up_pre * sig * (1.0 + gate_pre * (1.0 - sig))).astype(BF)

    store(act_buf, act_out)
    store(dgu_buf, dgu_out)
    with jax.named_scope('dn2'):
        scatter6 = Scatter(pos, dn2_part, *scatters[2], *main_s)
        scatter3.drain()
        halves(scatter6, lambda col: dot(dgu_buf[...], emb[:, pl.ds(col, wide)]))

    with jax.named_scope('rs6'):
        scatter6.relay_low()
        scatter6.relay_high()
        scatter6.relay_far()
        grad_n2 = scatter6.finish().astype(BF).astype(F32)
    with jax.named_scope('norm2_bwd'):
        grad_h1_norm, gain_mlp_part = norm_bwd(grad_n2, normed2, inv2, gain_mlp[...])
        grad_h1 = (grad_own[...].astype(F32) + grad_h1_norm).astype(BF)
        dh1_buf[pos.me] = grad_h1
    gather7 = Gather(pos, dh1_buf, *main_g)
    gather4.drain()
    gather7.start()
    with jax.named_scope('w_down'):
        @pl.loop(0, chunks)
        def _(j):
            col = pl.multiple_of(j * step, step)
            put_part(mlp_part, dot(act_buf[...], wd[:, pl.ds(col, step)]), col)

    scatter5 = Scatter(pos, mlp_part, *scatters[3], *side_s)
    with jax.named_scope('ag7'):
        gather7.relay()
        scatter5.start(0)
        scatter5.start(1)
        gather7.finish()
    with jax.named_scope('rs5_relay'):
        scatter5.relay_low()
        scatter5.relay_high()
    store(dh1_buf, dh1_out)

    with jax.named_scope('dheads'):
        dheads = dot_bt(full(dh1_buf), wo[...]).astype(BF)
    with jax.named_scope('attention_bwd'):
        nsin2 = -sin2
        dkeys = jnp.zeros((seq, head_dim), F32)
        dvalues = jnp.zeros((seq, head_dim), F32)
        for h in range(num_heads):
            cols = slice(h * head_dim, (h + 1) * head_dim)
            dhead = dheads[:, cols]
            probs = probs_buf[h]
            dprobs = dot_bt(dhead, values).astype(BF).astype(F32)
            dvalues += dot_at(probs.astype(BF), dhead)
            inner = jnp.sum(dprobs * probs, axis=-1, keepdims=True)
            dscores = (probs * (dprobs - inner) * (head_dim ** -0.5)).astype(BF)
            dquery = dot(dscores, keys).astype(BF)
            dkeys += dot_at(dscores, q_buf[:, cols])
            dqkv_buf[:, cols] = rope(dquery.astype(F32), cos2, nsin2).astype(BF)
        dqkv_buf[:, kq:kq + head_dim] = rope(dkeys.astype(BF).astype(F32), cos2, nsin2).astype(BF)
        dqkv_buf[:, kq + head_dim:] = dvalues.astype(BF)
    store(dqkv_buf, dqkv_out)

    with jax.named_scope('dn1'):
        scatter8 = Scatter(pos, dn1_part, *scatters[4], *main_s)
        scatter6.drain()
        halves(scatter8, lambda col: dot(dqkv_buf[...], wqkv_t[:, pl.ds(col, wide)]))

    with jax.named_scope('rs8'):
        scatter5.relay_far()
        scatter8.relay_low()
        scatter8.relay_high()
        scatter8.relay_far()
        hidden_buf[...] = (h1 + scatter5.finish()).astype(BF)
        store(hidden_buf, hidden_out)
        grad_n1 = scatter8.finish().astype(BF).astype(F32)
    with jax.named_scope('norm1_bwd'):
        grad_x_norm, gain_attn_part = norm_bwd(grad_n1, normed1, inv1, gain_attn[...])
        dx_pair[pos.core, 0:rows, :] = (grad_h1.astype(F32) + grad_x_norm).astype(BF)
        gain_parts = jnp.concatenate([gain_attn_part, gain_mlp_part], axis=0)
        high = gain_parts.astype(BF)
        dx_pair[pos.core, rows:rows + 2, :] = high
        dx_pair[pos.core, rows + 2:rows + 4, :] = (gain_parts - high.astype(F32)).astype(BF)
    with jax.named_scope('pair'):
        mine = remote(dx_pair.at[pos.core], dx_pair.at[pos.core], *(sem.at[0] for sem in pair_s), pos.partner)
        theirs = remote(dx_pair.at[pos.other], dx_pair.at[pos.other], *(sem.at[0] for sem in pair_s), pos.partner)
        mine.start()
        theirs.wait_recv()
        dx_out[...] = dx_pair[...]
        mine.wait_send()
    with jax.named_scope('tail'):
        for op in (gather0, scatter5, scatter8, gather7):
            op.drain()
        for copy in stores:
            copy.wait()


def layer(tokens, positions, gain_attn, gain_mlp, grad_own, emb, wq, wk, wv, wo, wg, wu, wd):
    num_heads, dim, head_dim = wq.shape
    blocks = CHIPS * CORES
    seq, ffn, rows_local = tokens.shape[1], wg.shape[1], emb.shape[0]
    rows = seq // blocks
    if rows_local != 2 * ffn:
        raise ValueError('shard rows')
    half = head_dim // 2
    freq = np.float32(ROPE_THETA) ** (-np.arange(half, dtype=np.float32) * np.float32(2.0 / head_dim))
    freq = jnp.asarray(np.concatenate([freq, freq])[:, None], F32)
    vmem = pl.BlockSpec(memory_space=pltpu.VMEM)
    hbm = pl.BlockSpec(memory_space=pltpu.HBM)
    width = num_heads * head_dim
    wide = width + 2 * head_dim
    sds = jax.ShapeDtypeStruct
    outs = [sds((CORES, rows + 4, dim), BF), sds((rows, dim), BF)] + [sds((blocks, rows, dim), BF)] * 4
    outs += [sds((seq, width), BF), sds((seq, ffn), BF), sds((seq, 2 * ffn), BF), sds((seq, wide), BF)]
    part = pltpu.VMEM((CORES, CHIPS, rows, dim), BF)
    gathered = pltpu.VMEM((blocks, rows, dim), BF)
    table = pltpu.VMEM((seq, head_dim), F32)
    scratch = [pltpu.VMEM((rows_local, dim), BF), pltpu.VMEM((seq, rows_local), BF), pltpu.VMEM((dim, wide), BF), pltpu.VMEM((wide, dim), BF),
               pltpu.VMEM((width, dim), BF), pltpu.VMEM((dim, ffn), BF),
               pltpu.VMEM((dim, ffn), BF), pltpu.VMEM((ffn, dim), BF), pltpu.SemaphoreType.DMA((15,)), pltpu.SemaphoreType.DMA((9,))]
    scratch += [gathered] * 4 + [part] * 5 + [pltpu.VMEM((seq, width), BF)]
    scratch += [pltpu.VMEM((seq, ffn), BF)] * 2 + [pltpu.VMEM((seq, 2 * ffn), BF), pltpu.VMEM((seq, wide), BF), pltpu.VMEM((seq, width), BF),
                                                   pltpu.VMEM((num_heads, seq, seq), F32), table, table,
                                                   pltpu.VMEM((rows, dim), BF), pltpu.VMEM((CORES, rows + 4, dim), BF)]
    scratch += scatter_scratch(rows, dim) * 5 + SCATTER_SEMS * 2 + GATHER_SEMS * 2 + [pltpu.SemaphoreType.DMA((1,))] * 2
    return pl.pallas_call(
        layer_kernel, out_shape=outs, in_specs=[vmem] * 6 + [hbm] * 8, out_specs=[vmem] + [hbm] * 9,
        scratch_shapes=scratch,
        compiler_params=pltpu.CompilerParams(collective_id=0, has_side_effects=True, vmem_limit_bytes=VMEM_FULL),
        name='layer',
    )(tokens, positions, freq, gain_attn, gain_mlp, grad_own, emb, wq, wk, wv, wo, wg, wu, wd)


def grads_kernel(n1, n2, dqkv, dgate, dup, heads, act, dh1, gh, hidden_in,
                 gw_query, gw_key, gw_value, gw_out, gw_gate, gw_up, gw_down, hidden):
    num_heads, _, head_dim = gw_query.shape
    width = num_heads * head_dim

    @pl.when(pl.program_id(0) == 0)
    def _():
        hidden[...] = hidden_in[...]

    gw_gate[...] = dot_at(n2[...], dgate[...])
    gw_up[...] = dot_at(n2[...], dup[...])
    gw_down[...] = dot_at(act[...], gh[...])
    both = dot_at(n1[...], dqkv[...])
    for h in range(num_heads):
        gw_query[h] = both[:, h * head_dim:(h + 1) * head_dim]
    gw_key[...] = both[:, width:width + head_dim]
    gw_value[...] = both[:, width + head_dim:]
    gw_out[...] = dot_at(heads[...], dh1[...])


def grads(n1, n2, dqkv, dgu, heads, act, dh1, gh, hidden, head_dim):
    seq, dim = n1.shape
    width, ffn = heads.shape[1], act.shape[1]
    num_heads = width // head_dim
    tile = 256
    sds = jax.ShapeDtypeStruct

    def whole(x):
        return pl.BlockSpec(x.shape, lambda i: (0,) * len(x.shape))

    def by_col(n):
        return pl.BlockSpec((n, tile), lambda i: (0, i))

    def by_row(n):
        return pl.BlockSpec((tile, n), lambda i: (i, 0))

    return pl.pallas_call(
        grads_kernel, grid=(dim // tile,),
        out_shape=[sds((num_heads, dim, head_dim), F32), sds((dim, head_dim), F32), sds((dim, head_dim), F32), sds((width, dim), F32),
                   sds((dim, ffn), F32), sds((dim, ffn), F32), sds((ffn, dim), F32), sds(hidden.shape, BF)],
        in_specs=[by_col(seq), by_col(seq), whole(dqkv), pl.BlockSpec((seq, ffn), lambda i: (0, 0)),
                  pl.BlockSpec((seq, ffn), lambda i: (0, 1)), whole(heads), whole(act), by_col(seq), by_col(seq), whole(hidden)],
        out_specs=[pl.BlockSpec((num_heads, tile, head_dim), lambda i: (0, i, 0)), by_row(head_dim), by_row(head_dim), by_col(width),
                   by_row(ffn), by_row(ffn), by_col(ffn), whole(hidden)],
        compiler_params=pltpu.CompilerParams(vmem_limit_bytes=VMEM_FULL),
        cost_estimate=pl.CostEstimate(flops=20_000_000_000, bytes_accessed=50_000_000, transcendentals=0),
        name='grads',
    )(n1, n2, dqkv, dgu, dgu, heads, act, dh1, gh, hidden)


def emb_grad_kernel(tokens, *refs):
    pairs = refs[:CHIPS]
    g_emb, g_attn, g_mlp, dx, gains = refs[CHIPS:]
    rows = dx.shape[0] // (CHIPS * CORES)
    me = lax.axis_index('tp')

    @pl.when(pl.program_id(0) == 0)
    def _():
        for k, pair in enumerate(pairs):
            chip = (me // CORES + CHIPS - k) % CHIPS
            for core in range(CORES):
                source = chip * CORES + core
                dx[pl.ds(pl.multiple_of(source * rows, rows), rows), :] = pair[core, 0:rows, :]
                gains[source] = pair[core, rows:rows + 2, :].astype(F32) + pair[core, rows + 2:rows + 4, :].astype(F32)
        total = gains[0]
        for i in range(1, CHIPS * CORES):
            total = total + gains[i]
        g_attn[...] = total[0:1, :]
        g_mlp[...] = total[1:2, :]

    height, seq = g_emb.shape[0], dx.shape[0]
    first = me * (height * pl.num_programs(0)) + pl.program_id(0) * height
    row = lax.broadcasted_iota(jnp.int32, (height, seq), 0) + first
    g_emb[...] = dot(jnp.where(row == tokens[...], 1.0, 0.0).astype(BF), dx[...])


def emb_grad(tokens, pairs, rows_local):
    seq, dim = tokens.shape[1], pairs[0].shape[2]
    steps = 16
    sds = jax.ShapeDtypeStruct

    def whole(x):
        return pl.BlockSpec(x.shape, lambda i: (0,) * len(x.shape))

    gain = sds((1, dim), F32)
    return pl.pallas_call(
        emb_grad_kernel, grid=(steps,),
        out_shape=[sds((rows_local, dim), F32), gain, gain],
        in_specs=[whole(tokens)] + [whole(x) for x in pairs],
        out_specs=[pl.BlockSpec((rows_local // steps, dim), lambda i: (i, 0)), whole(gain), whole(gain)],
        scratch_shapes=[pltpu.VMEM((seq, dim), BF), pltpu.VMEM((CHIPS * CORES, 2, dim), F32)],
        compiler_params=pltpu.CompilerParams(vmem_limit_bytes=VMEM_FULL),
        name='emb_grad',
    )(tokens, *pairs)


def solution(mesh):
    if mesh.shape['tp'] != CHIPS * CORES:
        raise ValueError('tp size')
    in_specs = (P('dp', None), P('dp', None), P('tp', None), P(None), P(None),
                P(None, 'tp', None), P(None, 'tp', None), P(None, 'tp', None), P('tp', None, None),
                P(None, 'tp'), P(None, 'tp'), P('tp', None), P('dp', 'tp', None))
    out_specs = (P('dp', 'tp', None), P(('dp', 'tp'), None),
                 P('dp', 'tp', None), P('dp', 'tp', None), P('dp', 'tp', None), P(('dp', 'tp'), None, None),
                 P('dp', 'tp'), P('dp', 'tp'), P(('dp', 'tp'), None), P('dp'), P('dp'))

    def device_fn(tokens, positions, emb_shard, gain_attn, gain_mlp, w_query, w_key, w_value, w_out, w_gate, w_up, w_down, grad_hidden):
        rows_local, dim = emb_shard.shape
        seq = tokens.shape[1]
        num_heads, head_dim = w_query.shape[1], w_query.shape[2]
        wq = jnp.transpose(w_query, (1, 0, 2))
        wk, wv = w_key.reshape(dim, head_dim), w_value.reshape(dim, head_dim)
        wo = w_out.reshape(num_heads * head_dim, dim)

        dx_pair, hidden, n1, n2, gh, dh1, heads, act, dgu, dqkv = layer(
            tokens, positions, gain_attn[None, :], gain_mlp[None, :], grad_hidden[0], emb_shard, wq, wk, wv, wo, w_gate, w_up, w_down)
        n = CHIPS * CORES
        arrived = [dx_pair] + [lax.ppermute(dx_pair, 'tp', [(i, (i + k * CORES) % n) for i in range(n)]) for k in range(1, CHIPS)]
        n1, n2, gh, dh1 = (x.reshape(seq, dim) for x in (n1, n2, gh, dh1))
        gw_query, gw_key, gw_value, gw_out, gw_gate, gw_up, gw_down, hidden = grads(
            n1, n2, dqkv, dgu, heads, act, dh1, gh, hidden, head_dim)
        g_emb, g_attn, g_mlp = emb_grad(tokens, arrived, rows_local)
        return (hidden[None], g_emb, jnp.transpose(gw_query, (1, 0, 2)), gw_key.reshape(dim, 1, head_dim),
                gw_value.reshape(dim, 1, head_dim), gw_out.reshape(num_heads, head_dim, dim),
                gw_gate, gw_up, gw_down, g_attn[0], g_mlp[0])

    return jax.shard_map(device_fn, mesh=mesh, in_specs=in_specs, out_specs=out_specs, check_vma=False)
```

```python
import jax
import jax.numpy as jnp
import numpy as np
from jax import lax
from jax.experimental import pallas as pl
from jax.experimental.pallas import tpu as pltpu
from jax.sharding import PartitionSpec as P

ROPE_THETA = 1000000.0
RMS_EPS = 1e-5
BF = jnp.bfloat16
F32 = jnp.float32
VMEM_FULL = 67043328
CHIPS = 4
CORES = 2


def dot(a, b):
    return lax.dot_general(a, b, (((1,), (0,)), ((), ())), preferred_element_type=F32)


def dot_bt(a, b):
    return lax.dot_general(a, b, (((1,), (1,)), ((), ())), preferred_element_type=F32)


def dot_at(a, b):
    return lax.dot_general(a, b, (((0,), (0,)), ((), ())), preferred_element_type=F32)


class Place:
    def __init__(self):
        me = lax.axis_index('tp')
        self.chip, self.core = me // CORES, me % CORES
        self.right_chip = (self.chip + 1) % CHIPS
        self.left_chip = (self.chip + CHIPS - 1) % CHIPS
        self.far_chip = (self.chip + 2) % CHIPS
        self.me = me
        self.other = 1 - self.core
        self.partner = self.chip * CORES + self.other
        self.right = self.right_chip * CORES + self.core
        self.left = self.left_chip * CORES + self.core
        self.far = self.far_chip * CORES + self.core


def remote(src, dst, send, recv, device):
    return pltpu.make_async_remote_copy(src_ref=src, dst_ref=dst, send_sem=send, recv_sem=recv,
                                        device_id={'tp': device}, device_id_type=pl.DeviceIdType.MESH)


def announce(pos):
    barrier = pltpu.get_barrier_semaphore()
    for device in (pos.left, pos.right, pos.partner):
        pl.semaphore_signal(barrier, inc=1, device_id={'tp': device}, device_id_type=pl.DeviceIdType.MESH)
    return barrier


class Gather:
    COPIES = 19

    def __init__(self, pos, buf, send, recv):
        p = pos
        quarter = buf.shape[-1] // 4
        other = p.other - p.core
        low, high, whole = (0, 2), (2, 4), (0, 4)
        pieces = ((0, 1), (1, 2), (2, 3), (3, 4))

        def copy(index, slot, part, device):
            ref = buf.at[slot, :, pl.ds(part[0] * quarter, (part[1] - part[0]) * quarter)]
            return remote(ref, ref, send.at[index], recv.at[index], device)

        plan = [((p.me, pieces[0], p.right), (p.left, pieces[0])), ((p.me, pieces[2], p.left), (p.right, pieces[2])),
                ((p.me, pieces[1], p.right), (p.left, pieces[1])), ((p.me, pieces[3], p.left), (p.right, pieces[3])),
                ((p.me, whole, p.partner), (p.partner, whole)),
                ((p.me, high, p.right), (p.left, high)), ((p.me, low, p.left), (p.right, low)),
                ((p.left, pieces[0], p.right), (p.far, pieces[0])), ((p.right, pieces[2], p.left), (p.far, pieces[2])),
                ((p.left, pieces[1], p.right), (p.far, pieces[1])), ((p.right, pieces[3], p.left), (p.far, pieces[3])),
                ((p.left, low, p.partner), (p.left + other, low)), ((p.right, high, p.partner), (p.right + other, high)),
                ((p.left, high, p.partner), (p.left + other, high)), ((p.right, low, p.partner), (p.right + other, low))]
        plan += [((p.far, pieces[i], p.partner), (p.far + other, pieces[i])) for i in (0, 2, 1, 3)]
        self.out = [copy(i, *sent) for i, (sent, _) in enumerate(plan)]
        self.into = [copy(i, slot, part, p.partner) for i, (_, (slot, part)) in enumerate(plan)]

    def start(self):
        for i in range(7):
            self.out[i].start()

    def pass_on(self, steps):
        for i, onward in steps:
            with jax.named_scope('g%d' % i):
                self.into[i].wait_recv()
            for j in onward:
                self.out[j].start()

    def relay(self):
        self.pass_on(((0, (7,)), (1, (8,)), (2, (9, 11)), (3, (10, 12)), (5, (13,)), (6, (14,))))

    def finish(self):
        self.pass_on(((7, (15,)), (8, (16,)), (9, (17,)), (10, (18,))))
        for i in (4, 11, 12, 13, 14, 15, 16, 17, 18):
            with jax.named_scope('g%d' % i):
                self.into[i].wait_recv()

    def drain(self):
        for copy in self.out:
            copy.wait_send()


class Scatter:
    COPIES = 18

    def __init__(self, pos, part, from_partner, work, arrive, work_half, arrive_half, send, recv):
        p = pos
        self.pos, self.part, self.from_partner = p, part, from_partner
        self.work, self.arrive, self.work_half, self.arrive_half = work, arrive, work_half, arrive_half
        self.quarter = work.shape[-1]
        self.chips = (p.far_chip, p.right_chip, p.left_chip, p.chip)
        self.inner = [[remote(part.at[p.other, y, :, self.cols(2 * h, 2)], from_partner.at[y, :, self.cols(2 * h, 2)],
                              send.at[4 * h + k], recv.at[4 * h + k], p.partner) for k, y in enumerate(self.chips)]
                      for h in range(2)]
        self.outer = [remote(work.at[k], arrive.at[k], send.at[8 + k], recv.at[8 + k], p.right if k % 4 < 2 else p.left)
                      for k in range(8)]
        self.straight = [remote(work_half.at[k], arrive_half.at[k], send.at[16 + k], recv.at[16 + k], device)
                         for k, device in enumerate((p.right, p.left))]

    def cols(self, q, n=1):
        return pl.ds(q * self.quarter, n * self.quarter)

    def pair(self, k, q, n=1):
        y = self.chips[k]
        return self.part[self.pos.core, y, :, self.cols(q, n)].astype(F32) + self.from_partner[y, :, self.cols(q, n)].astype(F32)

    def send_sum(self, k, value):
        self.work[k] = value.astype(BF)
        self.outer[k].start()

    def send_straight(self, k, value):
        self.work_half[k] = value.astype(BF)
        self.straight[k].start()

    def start(self, h):
        for copy in self.inner[h]:
            copy.start()

    def relay_low(self):
        with jax.named_scope('inner00'):
            self.inner[0][0].wait_recv()
        self.send_sum(0, self.pair(0, 0))
        self.send_sum(1, self.pair(0, 1))
        with jax.named_scope('inner02'):
            self.inner[0][2].wait_recv()
        self.send_straight(1, self.pair(2, 0, 2))

    def relay_high(self):
        with jax.named_scope('inner10'):
            self.inner[1][0].wait_recv()
        self.send_sum(2, self.pair(0, 2))
        self.send_sum(3, self.pair(0, 3))
        with jax.named_scope('inner11'):
            self.inner[1][1].wait_recv()
        self.send_straight(0, self.pair(1, 2, 2))

    def relay_far(self):
        with jax.named_scope('inner01'):
            self.inner[0][1].wait_recv()
        with jax.named_scope('inner12'):
            self.inner[1][2].wait_recv()
        for q, k in ((0, 1), (2, 2), (1, 1), (3, 2)):
            with jax.named_scope('s%d' % q):
                self.outer[q].wait_recv()
            self.send_sum(4 + q, self.pair(k, q) + self.arrive[q].astype(F32))

    def finish(self):
        with jax.named_scope('inner03'):
            self.inner[0][3].wait_recv()
        with jax.named_scope('inner13'):
            self.inner[1][3].wait_recv()
        with jax.named_scope('straight0'):
            self.straight[0].wait_recv()
        with jax.named_scope('straight1'):
            self.straight[1].wait_recv()
        low = self.pair(3, 0, 2) + self.arrive_half[1].astype(F32)
        high = self.pair(3, 2, 2) + self.arrive_half[0].astype(F32)
        for k in (4, 6, 5, 7):
            with jax.named_scope('s%d' % k):
                self.outer[k].wait_recv()
        far = [self.arrive[4 + q].astype(F32) for q in range(4)]
        return jnp.concatenate([low, high], axis=-1) + jnp.concatenate(far, axis=-1)

    def drain(self):
        for copy in self.inner[0] + self.inner[1] + self.outer + self.straight:
            copy.wait_send()


GATHER_SEMS = [pltpu.SemaphoreType.DMA((Gather.COPIES,))] * 2
SCATTER_SEMS = [pltpu.SemaphoreType.DMA((Scatter.COPIES,))] * 2


def scatter_scratch(rows, dim):
    return [pltpu.VMEM((CHIPS, rows, dim), BF)] + [pltpu.VMEM((8, rows, dim // 4), BF)] * 2 + [pltpu.VMEM((2, rows, dim // 2), BF)] * 2


def put_part(part, value, col):
    rows, width = part.shape[2], value.shape[1]
    for b in range(CHIPS * CORES):
        part[b % CORES, b // CORES, :, pl.ds(col, width)] = value[b * rows:(b + 1) * rows].astype(BF)


def norm_stats(hidden_f):
    inv_rms = lax.rsqrt(jnp.mean(hidden_f * hidden_f, axis=-1, keepdims=True) + RMS_EPS)
    return hidden_f * inv_rms, inv_rms


def norm_bwd(grad_f, normed, inv_rms, gain):
    gain_part = jnp.sum(grad_f * normed, axis=0, keepdims=True)
    scaled = grad_f * gain
    return inv_rms * (scaled - normed * jnp.mean(scaled * normed, axis=-1, keepdims=True)), gain_part


def rope(values, cos2, sin2):
    return values * cos2 + pltpu.roll(values, values.shape[-1] // 2, axis=1) * sin2


def full(buf):
    blocks, rows, dim = buf.shape
    return buf[...].reshape(blocks * rows, dim)


def rope_tables(pos_row, freq_col):
    angles = jnp.transpose(freq_col * pos_row.astype(F32))
    lane = lax.broadcasted_iota(jnp.int32, angles.shape, 1)
    sin = jnp.sin(angles)
    return jnp.cos(angles), jnp.where(lane < angles.shape[1] // 2, -sin, sin)


def layer_kernel(tokens_hbm, positions_hbm, freq_hbm, gain_attn_hbm, gain_mlp_hbm, grad_hbm, emb_hbm, wq_hbm, wk_hbm, wv_hbm, wo_hbm, wg_hbm, wu_hbm, wd_hbm,
                 dx_out, hidden_out, n1_out, n2_out, gh_out, dh1_out, heads_out, act_out, dgu_out, dqkv_out,
                 emb, pick_buf, wqkv, wqkv_t, wo, wg, wu, wd, wsem, osem, n1_buf, n2_buf, gh_buf, dh1_buf,
                 emb_part, attn_part, dn2_part, mlp_part, dn1_part, heads_buf, gact, act_buf, dgu_buf, dqkv_buf,
                 q_buf, probs_buf, cos_ref, sin_ref, hidden_buf, dx_pair, tokens, positions, freq, gain_attn, gain_mlp, grad_own, small_sem, *comm):
    pos = Place()
    num_heads, dim, head_dim = wq_hbm.shape
    rows_local = emb_hbm.shape[0]
    blocks, rows, _ = n1_buf.shape
    seq, ffn = blocks * rows, wg.shape[1]
    scatters = [comm[5 * i:5 * i + 5] for i in range(5)]
    main_s, side_s, main_g, side_g, pair_s = (comm[25 + 2 * i:27 + 2 * i] for i in range(5))
    kq = num_heads * head_dim
    step = 512
    chunks = dim // step
    wide = dim // 2

    def emb_load(j):
        cols = pl.ds(pl.multiple_of(j * step, step), step)
        return pltpu.make_async_copy(emb_hbm.at[:, cols], emb.at[:, cols], wsem.at[j])

    small = ((tokens_hbm, tokens), (grad_hbm, gh_buf.at[pos.me]), (positions_hbm, positions), (freq_hbm, freq),
             (gain_attn_hbm, gain_attn), (gain_mlp_hbm, gain_mlp), (grad_hbm, grad_own))
    small = [pltpu.make_async_copy(src, dst, small_sem.at[k]) for k, (src, dst) in enumerate(small)]
    small[0].start()
    for j in range(chunks):
        emb_load(j).start()
    for copy in small[1:]:
        copy.start()
    pairs = [(wq_hbm.at[h], wqkv.at[:, pl.ds(h * head_dim, head_dim)]) for h in range(num_heads)]
    pairs += [(wk_hbm, wqkv.at[:, pl.ds(kq, head_dim)]), (wv_hbm, wqkv.at[:, pl.ds(kq + head_dim, head_dim)])]
    pairs += [(wo_hbm, wo), (wd_hbm, wd), (wg_hbm, wg), (wu_hbm, wu)]
    loads = [pltpu.make_async_copy(src, dst, wsem.at[chunks + k]) for k, (src, dst) in enumerate(pairs)]
    for load in loads:
        load.start()
    stores = []

    def store(src, dst):
        stores.append(pltpu.make_async_copy(src, dst, osem.at[len(stores)]))
        stores[-1].start()

    def halves(scatter, product):
        for h in range(2):
            put_part(scatter.part, product(h * wide), h * wide)
            scatter.start(h)

    def turn(src, dst, first):
        @pl.loop(0, src.shape[0] // 128)
        def _(j):
            at = pl.multiple_of(j * 128, 128)
            dst[first:first + src.shape[1], pl.ds(at, 128)] = jnp.transpose(src[pl.ds(at, 128), :])

    barrier = announce(pos)
    gather0 = Gather(pos, gh_buf, *side_g)
    scatter1 = Scatter(pos, emb_part, *scatters[0], *main_s)

    def looked_up(h):
        @pl.loop(h * chunks // 2, (h + 1) * chunks // 2)
        def _(j):
            col = pl.multiple_of(j * step, step)
            emb_load(j).wait()
            put_part(scatter1.part, dot(pick_buf[...], emb[:, pl.ds(col, step)]), col)

    with jax.named_scope('lookup_low'):
        small[0].wait()
        local = jnp.transpose(jnp.broadcast_to(tokens[...] - pos.me * rows_local, (seq, seq)))
        lane = lax.broadcasted_iota(jnp.int32, (seq, seq), 1)
        for j in range(rows_local // seq):
            pick_buf[:, j * seq:(j + 1) * seq] = jnp.where(local == lane + j * seq, 1.0, 0.0).astype(BF)
        looked_up(0)
    with jax.named_scope('barrier'):
        pl.semaphore_wait(barrier, 3)
    scatter1.start(0)
    small[1].wait()
    gather0.start()
    with jax.named_scope('lookup_high'):
        looked_up(1)
        scatter1.start(1)
    with jax.named_scope('rs1'):
        scatter1.relay_low()
        scatter1.relay_high()
        gather0.relay()
        scatter1.relay_far()
        gather0.finish()
        for copy in small[2:]:
            copy.wait()
        cos_ref[...], sin_ref[...] = rope_tables(positions[...], freq[...])
        x0 = scatter1.finish()
    with jax.named_scope('norm1'):
        normed1, inv1 = norm_stats(x0)
        n1_buf[pos.me] = (normed1 * gain_attn[...]).astype(BF)
    with jax.named_scope('ag1'):
        gather1 = Gather(pos, n1_buf, *main_g)
        gather1.start()
        store(gh_buf, gh_out)
    with jax.named_scope('turn_gate'):
        loads[7].wait()
        turn(wg, emb, 0)
    with jax.named_scope('ag1_relay'):
        gather1.relay()
    with jax.named_scope('turn_up'):
        loads[8].wait()
        turn(wu, emb, ffn)
    with jax.named_scope('ag1_finish'):
        gather1.finish()
    store(n1_buf, n1_out)

    with jax.named_scope('qkv'):
        for load in loads[:5]:
            load.wait()
        qkv = dot(full(n1_buf), wqkv[...])
    with jax.named_scope('attention'):
        cos2, sin2 = cos_ref[...], sin_ref[...]
        keys = rope(qkv[:, kq:kq + head_dim], cos2, sin2).astype(BF)
        values = qkv[:, kq + head_dim:].astype(BF)
        causal = lax.broadcasted_iota(jnp.int32, (seq, seq), 0) >= lax.broadcasted_iota(jnp.int32, (seq, seq), 1)
        for h in range(num_heads):
            cols = slice(h * head_dim, (h + 1) * head_dim)
            query = rope(qkv[:, cols], cos2, sin2).astype(BF)
            q_buf[:, cols] = query
            scores = jnp.where(causal, dot_bt(query, keys) * (head_dim ** -0.5), -1e30)
            expd = jnp.exp(scores - jnp.max(scores, axis=-1, keepdims=True))
            probs = expd / jnp.sum(expd, axis=-1, keepdims=True)
            probs_buf[h] = probs
            heads_buf[:, cols] = dot(probs.astype(BF), values).astype(BF)
    store(heads_buf, heads_out)
    with jax.named_scope('w_out'):
        loads[5].wait()
        scatter3 = Scatter(pos, attn_part, *scatters[1], *main_s)
        scatter1.drain()
        halves(scatter3, lambda col: dot(heads_buf[...], wo[:, pl.ds(col, wide)]))

    with jax.named_scope('rs3_a'):
        scatter3.relay_low()
        scatter3.relay_high()

    with jax.named_scope('grad_act'):
        loads[6].wait()

        @pl.loop(0, ffn // 256)
        def _(j):
            cols = pl.ds(pl.multiple_of(j * 256, 256), 256)
            gact[:, cols] = dot_bt(full(gh_buf), wd[cols, :]).astype(BF)

    with jax.named_scope('rs3_b'):
        scatter3.relay_far()
        h1_bf = (x0 + scatter3.finish()).astype(BF)
    with jax.named_scope('norm2'):
        h1 = h1_bf.astype(F32)
        normed2, inv2 = norm_stats(h1)
        n2_buf[pos.me] = (normed2 * gain_mlp[...]).astype(BF)
    with jax.named_scope('ag4'):
        gather4 = Gather(pos, n2_buf, *main_g)
        gather1.drain()
        gather4.start()
        turn(wqkv, wqkv_t, 0)
        gather4.relay()
        gather4.finish()
    store(n2_buf, n2_out)

    with jax.named_scope('gate_up'):
        @pl.loop(0, ffn // 512)
        def _(j):
            cols = pl.ds(pl.multiple_of(j * 512, 512), 512)
            n2 = full(n2_buf)
            gate_pre = dot(n2, wg[:, cols])
            up_pre = dot(n2, wu[:, cols])
            sig = jax.nn.sigmoid(gate_pre)
            gate_act = gate_pre * sig
            act_buf[:, cols] = (gate_act * up_pre).astype(BF)
            grad_act = gact[:, cols].astype(F32)
            dgu_buf[:, pl.ds(pl.multiple_of(ffn + j * 512, 512), 512)] = (grad_act * gate_act).astype(BF)
            dgu_buf[:, cols] = (grad_act * up_pre * sig * (1.0 + gate_pre * (1.0 - sig))).astype(BF)

    store(act_buf, act_out)
    store(dgu_buf, dgu_out)
    with jax.named_scope('dn2'):
        scatter6 = Scatter(pos, dn2_part, *scatters[2], *main_s)
        scatter3.drain()
        halves(scatter6, lambda col: dot(dgu_buf[...], emb[:, pl.ds(col, wide)]))

    with jax.named_scope('rs6'):
        scatter6.relay_low()
        scatter6.relay_high()
        scatter6.relay_far()
        grad_n2 = scatter6.finish().astype(BF).astype(F32)
    with jax.named_scope('norm2_bwd'):
        grad_h1_norm, gain_mlp_part = norm_bwd(grad_n2, normed2, inv2, gain_mlp[...])
        grad_h1 = (grad_own[...].astype(F32) + grad_h1_norm).astype(BF)
        dh1_buf[pos.me] = grad_h1
    gather7 = Gather(pos, dh1_buf, *main_g)
    gather4.drain()
    gather7.start()
    with jax.named_scope('w_down'):
        @pl.loop(0, chunks)
        def _(j):
            col = pl.multiple_of(j * step, step)
            put_part(mlp_part, dot(act_buf[...], wd[:, pl.ds(col, step)]), col)

    scatter5 = Scatter(pos, mlp_part, *scatters[3], *side_s)
    with jax.named_scope('ag7'):
        gather7.relay()
        scatter5.start(0)
        scatter5.start(1)
        gather7.finish()
    with jax.named_scope('rs5_relay'):
        scatter5.relay_low()
        scatter5.relay_high()
    store(dh1_buf, dh1_out)

    with jax.named_scope('dheads'):
        dheads = dot_bt(full(dh1_buf), wo[...]).astype(BF)
    with jax.named_scope('attention_bwd'):
        nsin2 = -sin2
        dkeys = jnp.zeros((seq, head_dim), F32)
        dvalues = jnp.zeros((seq, head_dim), F32)
        for h in range(num_heads):
            cols = slice(h * head_dim, (h + 1) * head_dim)
            dhead = dheads[:, cols]
            probs = probs_buf[h]
            dprobs = dot_bt(dhead, values).astype(BF).astype(F32)
            dvalues += dot_at(probs.astype(BF), dhead)
            inner = jnp.sum(dprobs * probs, axis=-1, keepdims=True)
            dscores = (probs * (dprobs - inner) * (head_dim ** -0.5)).astype(BF)
            dquery = dot(dscores, keys).astype(BF)
            dkeys += dot_at(dscores, q_buf[:, cols])
            dqkv_buf[:, cols] = rope(dquery.astype(F32), cos2, nsin2).astype(BF)
        dqkv_buf[:, kq:kq + head_dim] = rope(dkeys.astype(BF).astype(F32), cos2, nsin2).astype(BF)
        dqkv_buf[:, kq + head_dim:] = dvalues.astype(BF)
    store(dqkv_buf, dqkv_out)

    with jax.named_scope('dn1'):
        scatter8 = Scatter(pos, dn1_part, *scatters[4], *main_s)
        scatter6.drain()
        halves(scatter8, lambda col: dot(dqkv_buf[...], wqkv_t[:, pl.ds(col, wide)]))

    with jax.named_scope('rs8'):
        scatter5.relay_far()
        scatter8.relay_low()
        scatter8.relay_high()
        scatter8.relay_far()
        hidden_buf[...] = (h1 + scatter5.finish()).astype(BF)
        store(hidden_buf, hidden_out)
        grad_n1 = scatter8.finish().astype(BF).astype(F32)
    with jax.named_scope('norm1_bwd'):
        grad_x_norm, gain_attn_part = norm_bwd(grad_n1, normed1, inv1, gain_attn[...])
        dx_pair[pos.core, 0:rows, :] = (grad_h1.astype(F32) + grad_x_norm).astype(BF)
        gain_parts = jnp.concatenate([gain_attn_part, gain_mlp_part], axis=0)
        high = gain_parts.astype(BF)
        dx_pair[pos.core, rows:rows + 2, :] = high
        dx_pair[pos.core, rows + 2:rows + 4, :] = (gain_parts - high.astype(F32)).astype(BF)
    with jax.named_scope('pair'):
        mine = remote(dx_pair.at[pos.core], dx_pair.at[pos.core], *(sem.at[0] for sem in pair_s), pos.partner)
        theirs = remote(dx_pair.at[pos.other], dx_pair.at[pos.other], *(sem.at[0] for sem in pair_s), pos.partner)
        mine.start()
        theirs.wait_recv()
        dx_out[...] = dx_pair[...]
        mine.wait_send()
    with jax.named_scope('tail'):
        for op in (gather0, scatter5, scatter8, gather7):
            op.drain()
        for copy in stores:
            copy.wait()


def layer(tokens, positions, gain_attn, gain_mlp, grad_own, emb, wq, wk, wv, wo, wg, wu, wd):
    num_heads, dim, head_dim = wq.shape
    blocks = CHIPS * CORES
    seq, ffn, rows_local = tokens.shape[1], wg.shape[1], emb.shape[0]
    rows = seq // blocks
    if rows_local != 2 * ffn:
        raise ValueError('shard rows')
    half = head_dim // 2
    freq = np.float32(ROPE_THETA) ** (-np.arange(half, dtype=np.float32) * np.float32(2.0 / head_dim))
    freq = jnp.asarray(np.concatenate([freq, freq])[:, None], F32)
    vmem = pl.BlockSpec(memory_space=pltpu.VMEM)
    hbm = pl.BlockSpec(memory_space=pltpu.HBM)
    width = num_heads * head_dim
    wide = width + 2 * head_dim
    sds = jax.ShapeDtypeStruct
    outs = [sds((CORES, rows + 4, dim), BF), sds((rows, dim), BF)] + [sds((blocks, rows, dim), BF)] * 4
    outs += [sds((seq, width), BF), sds((seq, ffn), BF), sds((seq, 2 * ffn), BF), sds((seq, wide), BF)]
    part = pltpu.VMEM((CORES, CHIPS, rows, dim), BF)
    gathered = pltpu.VMEM((blocks, rows, dim), BF)
    table = pltpu.VMEM((seq, head_dim), F32)
    scratch = [pltpu.VMEM((rows_local, dim), BF), pltpu.VMEM((seq, rows_local), BF), pltpu.VMEM((dim, wide), BF), pltpu.VMEM((wide, dim), BF),
               pltpu.VMEM((width, dim), BF), pltpu.VMEM((dim, ffn), BF),
               pltpu.VMEM((dim, ffn), BF), pltpu.VMEM((ffn, dim), BF), pltpu.SemaphoreType.DMA((15,)), pltpu.SemaphoreType.DMA((9,))]
    scratch += [gathered] * 4 + [part] * 5 + [pltpu.VMEM((seq, width), BF)]
    scratch += [pltpu.VMEM((seq, ffn), BF)] * 2 + [pltpu.VMEM((seq, 2 * ffn), BF), pltpu.VMEM((seq, wide), BF), pltpu.VMEM((seq, width), BF),
                                                   pltpu.VMEM((num_heads, seq, seq), F32), table, table,
                                                   pltpu.VMEM((rows, dim), BF), pltpu.VMEM((CORES, rows + 4, dim), BF),
                                                   pltpu.VMEM((1, seq), jnp.int32), pltpu.VMEM((1, seq), jnp.int32), pltpu.VMEM((head_dim, 1), F32),
                                                   pltpu.VMEM((1, dim), F32), pltpu.VMEM((1, dim), F32), pltpu.VMEM((rows, dim), BF),
                                                   pltpu.SemaphoreType.DMA((7,))]
    scratch += scatter_scratch(rows, dim) * 5 + SCATTER_SEMS * 2 + GATHER_SEMS * 2 + [pltpu.SemaphoreType.DMA((1,))] * 2
    return pl.pallas_call(
        layer_kernel, out_shape=outs, in_specs=[hbm] * 14, out_specs=[vmem] + [hbm] * 9,
        scratch_shapes=scratch,
        compiler_params=pltpu.CompilerParams(collective_id=0, has_side_effects=True, vmem_limit_bytes=VMEM_FULL),
        name='layer',
    )(tokens, positions, freq, gain_attn, gain_mlp, grad_own, emb, wq, wk, wv, wo, wg, wu, wd)


def grads_kernel(n1, n2, dqkv, dgate, dup, heads, act, dh1, gh, hidden_in,
                 gw_query, gw_key, gw_value, gw_out, gw_gate, gw_up, gw_down, hidden):
    num_heads, _, head_dim = gw_query.shape
    width = num_heads * head_dim

    @pl.when(pl.program_id(0) == 0)
    def _():
        hidden[...] = hidden_in[...]

    gw_gate[...] = dot_at(n2[...], dgate[...])
    gw_up[...] = dot_at(n2[...], dup[...])
    gw_down[...] = dot_at(act[...], gh[...])
    both = dot_at(n1[...], dqkv[...])
    for h in range(num_heads):
        gw_query[h] = both[:, h * head_dim:(h + 1) * head_dim]
    gw_key[...] = both[:, width:width + head_dim]
    gw_value[...] = both[:, width + head_dim:]
    gw_out[...] = dot_at(heads[...], dh1[...])


def grads(n1, n2, dqkv, dgu, heads, act, dh1, gh, hidden, head_dim):
    seq, dim = n1.shape
    width, ffn = heads.shape[1], act.shape[1]
    num_heads = width // head_dim
    tile = 256
    sds = jax.ShapeDtypeStruct

    def whole(x):
        return pl.BlockSpec(x.shape, lambda i: (0,) * len(x.shape))

    def by_col(n):
        return pl.BlockSpec((n, tile), lambda i: (0, i))

    def by_row(n):
        return pl.BlockSpec((tile, n), lambda i: (i, 0))

    return pl.pallas_call(
        grads_kernel, grid=(dim // tile,),
        out_shape=[sds((num_heads, dim, head_dim), F32), sds((dim, head_dim), F32), sds((dim, head_dim), F32), sds((width, dim), F32),
                   sds((dim, ffn), F32), sds((dim, ffn), F32), sds((ffn, dim), F32), sds(hidden.shape, BF)],
        in_specs=[by_col(seq), by_col(seq), whole(dqkv), pl.BlockSpec((seq, ffn), lambda i: (0, 0)),
                  pl.BlockSpec((seq, ffn), lambda i: (0, 1)), whole(heads), whole(act), by_col(seq), by_col(seq), whole(hidden)],
        out_specs=[pl.BlockSpec((num_heads, tile, head_dim), lambda i: (0, i, 0)), by_row(head_dim), by_row(head_dim), by_col(width),
                   by_row(ffn), by_row(ffn), by_col(ffn), whole(hidden)],
        compiler_params=pltpu.CompilerParams(vmem_limit_bytes=VMEM_FULL),
        cost_estimate=pl.CostEstimate(flops=20_000_000_000, bytes_accessed=50_000_000, transcendentals=0),
        name='grads',
    )(n1, n2, dqkv, dgu, dgu, heads, act, dh1, gh, hidden)


def emb_grad_kernel(tokens, *refs):
    pairs = refs[:CHIPS]
    g_emb, g_attn, g_mlp, dx, gains, ring, sem = refs[CHIPS:]
    seq, rows = dx.shape[0], dx.shape[0] // (CHIPS * CORES)
    me = lax.axis_index('tp')
    for k, pair in enumerate(pairs):
        chip = (me // CORES + CHIPS - k) % CHIPS
        for core in range(CORES):
            source = chip * CORES + core
            dx[pl.ds(pl.multiple_of(source * rows, rows), rows), :] = pair[core, 0:rows, :]
            gains[source] = pair[core, rows:rows + 2, :].astype(F32) + pair[core, rows + 2:rows + 4, :].astype(F32)

    slots, height = ring.shape[0], ring.shape[1]
    rows_local = g_emb.shape[0]
    local = tokens[...] - me * rows_local
    row = lax.broadcasted_iota(jnp.int32, (height, seq), 0)
    copies = []
    for c in range(rows_local // height):
        slot = c % slots
        if c >= slots:
            copies[c - slots].wait()
        ring[slot] = dot(jnp.where(row + c * height == local, 1.0, 0.0).astype(BF), dx[...])
        copies.append(pltpu.make_async_copy(ring.at[slot], g_emb.at[pl.ds(c * height, height)], sem.at[slot]))
        copies[-1].start()
    total = gains[0]
    for i in range(1, CHIPS * CORES):
        total = total + gains[i]
    g_attn[...] = total[0:1, :]
    g_mlp[...] = total[1:2, :]
    for copy in copies[-slots:]:
        copy.wait()


def emb_grad(tokens, pairs, rows_local):
    seq, dim = tokens.shape[1], pairs[0].shape[2]
    height, slots = 256, 4
    sds = jax.ShapeDtypeStruct
    vmem = pl.BlockSpec(memory_space=pltpu.VMEM)
    gain = sds((1, dim), F32)
    return pl.pallas_call(
        emb_grad_kernel, out_shape=[sds((rows_local, dim), F32), gain, gain],
        in_specs=[vmem] * (1 + len(pairs)), out_specs=[pl.BlockSpec(memory_space=pltpu.HBM), vmem, vmem],
        scratch_shapes=[pltpu.VMEM((seq, dim), BF), pltpu.VMEM((CHIPS * CORES, 2, dim), F32), pltpu.VMEM((slots, height, dim), F32),
                        pltpu.SemaphoreType.DMA((slots,))],
        compiler_params=pltpu.CompilerParams(vmem_limit_bytes=VMEM_FULL),
        name='emb_grad',
    )(tokens, *pairs)


def solution(mesh):
    if mesh.shape['tp'] != CHIPS * CORES:
        raise ValueError('tp size')
    in_specs = (P('dp', None), P('dp', None), P('tp', None), P(None), P(None),
                P(None, 'tp', None), P(None, 'tp', None), P(None, 'tp', None), P('tp', None, None),
                P(None, 'tp'), P(None, 'tp'), P('tp', None), P('dp', 'tp', None))
    out_specs = (P('dp', 'tp', None), P(('dp', 'tp'), None),
                 P('dp', 'tp', None), P('dp', 'tp', None), P('dp', 'tp', None), P(('dp', 'tp'), None, None),
                 P('dp', 'tp'), P('dp', 'tp'), P(('dp', 'tp'), None), P('dp'), P('dp'))

    def device_fn(tokens, positions, emb_shard, gain_attn, gain_mlp, w_query, w_key, w_value, w_out, w_gate, w_up, w_down, grad_hidden):
        rows_local, dim = emb_shard.shape
        seq = tokens.shape[1]
        num_heads, head_dim = w_query.shape[1], w_query.shape[2]
        wq = jnp.transpose(w_query, (1, 0, 2))
        wk, wv = w_key.reshape(dim, head_dim), w_value.reshape(dim, head_dim)
        wo = w_out.reshape(num_heads * head_dim, dim)

        dx_pair, hidden, n1, n2, gh, dh1, heads, act, dgu, dqkv = layer(
            tokens, positions, gain_attn[None, :], gain_mlp[None, :], grad_hidden[0], emb_shard, wq, wk, wv, wo, w_gate, w_up, w_down)
        n = CHIPS * CORES
        arrived = [dx_pair] + [lax.ppermute(dx_pair, 'tp', [(i, (i + k * CORES) % n) for i in range(n)]) for k in range(1, CHIPS)]
        n1, n2, gh, dh1 = (x.reshape(seq, dim) for x in (n1, n2, gh, dh1))
        gw_query, gw_key, gw_value, gw_out, gw_gate, gw_up, gw_down, hidden = grads(
            n1, n2, dqkv, dgu, heads, act, dh1, gh, hidden, head_dim)
        g_emb, g_attn, g_mlp = emb_grad(tokens, arrived, rows_local)
        return (hidden[None], g_emb, jnp.transpose(gw_query, (1, 0, 2)), gw_key.reshape(dim, 1, head_dim),
                gw_value.reshape(dim, 1, head_dim), gw_out.reshape(num_heads, head_dim, dim),
                gw_gate, gw_up, gw_down, g_attn[0], g_mlp[0])

    return jax.shard_map(device_fn, mesh=mesh, in_specs=in_specs, out_specs=out_specs, check_vma=False)
```

```python
import jax
import jax.numpy as jnp
import numpy as np
from jax import lax
from jax.experimental import pallas as pl
from jax.experimental.pallas import tpu as pltpu
from jax.sharding import PartitionSpec as P

ROPE_THETA = 1000000.0
RMS_EPS = 1e-5
BF = jnp.bfloat16
F32 = jnp.float32
VMEM_FULL = 67043328
CHIPS = 4
CORES = 2


def dot(a, b):
    return lax.dot_general(a, b, (((1,), (0,)), ((), ())), preferred_element_type=F32)


def dot_bt(a, b):
    return lax.dot_general(a, b, (((1,), (1,)), ((), ())), preferred_element_type=F32)


def dot_at(a, b):
    return lax.dot_general(a, b, (((0,), (0,)), ((), ())), preferred_element_type=F32)


class Place:
    def __init__(self):
        me = lax.axis_index('tp')
        self.chip, self.core = me // CORES, me % CORES
        self.right_chip = (self.chip + 1) % CHIPS
        self.left_chip = (self.chip + CHIPS - 1) % CHIPS
        self.far_chip = (self.chip + 2) % CHIPS
        self.me = me
        self.other = 1 - self.core
        self.partner = self.chip * CORES + self.other
        self.right = self.right_chip * CORES + self.core
        self.left = self.left_chip * CORES + self.core
        self.far = self.far_chip * CORES + self.core


def remote(src, dst, send, recv, device):
    return pltpu.make_async_remote_copy(src_ref=src, dst_ref=dst, send_sem=send, recv_sem=recv,
                                        device_id={'tp': device}, device_id_type=pl.DeviceIdType.MESH)


def announce(pos):
    barrier = pltpu.get_barrier_semaphore()
    for device in (pos.left, pos.right, pos.partner):
        pl.semaphore_signal(barrier, inc=1, device_id={'tp': device}, device_id_type=pl.DeviceIdType.MESH)
    return barrier


class Gather:
    COPIES = 19

    def __init__(self, pos, buf, send, recv):
        p = pos
        quarter = buf.shape[-1] // 4
        other = p.other - p.core
        low, high, whole = (0, 2), (2, 4), (0, 4)
        pieces = ((0, 1), (1, 2), (2, 3), (3, 4))

        def copy(index, slot, part, device):
            ref = buf.at[slot, :, pl.ds(part[0] * quarter, (part[1] - part[0]) * quarter)]
            return remote(ref, ref, send.at[index], recv.at[index], device)

        plan = [((p.me, pieces[0], p.right), (p.left, pieces[0])), ((p.me, pieces[2], p.left), (p.right, pieces[2])),
                ((p.me, pieces[1], p.right), (p.left, pieces[1])), ((p.me, pieces[3], p.left), (p.right, pieces[3])),
                ((p.me, whole, p.partner), (p.partner, whole)),
                ((p.me, high, p.right), (p.left, high)), ((p.me, low, p.left), (p.right, low)),
                ((p.left, pieces[0], p.right), (p.far, pieces[0])), ((p.right, pieces[2], p.left), (p.far, pieces[2])),
                ((p.left, pieces[1], p.right), (p.far, pieces[1])), ((p.right, pieces[3], p.left), (p.far, pieces[3])),
                ((p.left, low, p.partner), (p.left + other, low)), ((p.right, high, p.partner), (p.right + other, high)),
                ((p.left, high, p.partner), (p.left + other, high)), ((p.right, low, p.partner), (p.right + other, low))]
        plan += [((p.far, pieces[i], p.partner), (p.far + other, pieces[i])) for i in (0, 2, 1, 3)]
        self.out = [copy(i, *sent) for i, (sent, _) in enumerate(plan)]
        self.into = [copy(i, slot, part, p.partner) for i, (_, (slot, part)) in enumerate(plan)]

    def start(self):
        for i in range(7):
            self.out[i].start()

    def pass_on(self, steps):
        for i, onward in steps:
            with jax.named_scope('g%d' % i):
                self.into[i].wait_recv()
            for j in onward:
                self.out[j].start()

    def relay(self):
        self.pass_on(((0, (7,)), (1, (8,)), (2, (9, 11)), (3, (10, 12)), (5, (13,)), (6, (14,))))

    def finish(self):
        self.pass_on(((7, (15,)), (8, (16,)), (9, (17,)), (10, (18,))))
        for i in (4, 11, 12, 13, 14, 15, 16, 17, 18):
            with jax.named_scope('g%d' % i):
                self.into[i].wait_recv()

    def drain(self):
        for copy in self.out:
            copy.wait_send()


class Scatter:
    COPIES = 18

    def __init__(self, pos, part, from_partner, work, arrive, work_half, arrive_half, send, recv):
        p = pos
        self.pos, self.part, self.from_partner = p, part, from_partner
        self.work, self.arrive, self.work_half, self.arrive_half = work, arrive, work_half, arrive_half
        self.quarter = work.shape[-1]
        self.chips = (p.far_chip, p.right_chip, p.left_chip, p.chip)
        self.inner = [[remote(part.at[p.other, y, :, self.cols(2 * h, 2)], from_partner.at[y, :, self.cols(2 * h, 2)],
                              send.at[4 * h + k], recv.at[4 * h + k], p.partner) for k, y in enumerate(self.chips)]
                      for h in range(2)]
        self.outer = [remote(work.at[k], arrive.at[k], send.at[8 + k], recv.at[8 + k], p.right if k % 4 < 2 else p.left)
                      for k in range(8)]
        self.straight = [remote(work_half.at[k], arrive_half.at[k], send.at[16 + k], recv.at[16 + k], device)
                         for k, device in enumerate((p.right, p.left))]

    def cols(self, q, n=1):
        return pl.ds(q * self.quarter, n * self.quarter)

    def pair(self, k, q, n=1):
        y = self.chips[k]
        return self.part[self.pos.core, y, :, self.cols(q, n)].astype(F32) + self.from_partner[y, :, self.cols(q, n)].astype(F32)

    def send_sum(self, k, value):
        self.work[k] = value.astype(BF)
        self.outer[k].start()

    def send_straight(self, k, value):
        self.work_half[k] = value.astype(BF)
        self.straight[k].start()

    def start(self, h):
        for copy in self.inner[h]:
            copy.start()

    def relay_low(self):
        with jax.named_scope('inner00'):
            self.inner[0][0].wait_recv()
        self.send_sum(0, self.pair(0, 0))
        self.send_sum(1, self.pair(0, 1))
        with jax.named_scope('inner02'):
            self.inner[0][2].wait_recv()
        self.send_straight(1, self.pair(2, 0, 2))

    def relay_high(self):
        with jax.named_scope('inner10'):
            self.inner[1][0].wait_recv()
        self.send_sum(2, self.pair(0, 2))
        self.send_sum(3, self.pair(0, 3))
        with jax.named_scope('inner11'):
            self.inner[1][1].wait_recv()
        self.send_straight(0, self.pair(1, 2, 2))

    def relay_far(self):
        with jax.named_scope('inner01'):
            self.inner[0][1].wait_recv()
        with jax.named_scope('inner12'):
            self.inner[1][2].wait_recv()
        for q, k in ((0, 1), (2, 2), (1, 1), (3, 2)):
            with jax.named_scope('s%d' % q):
                self.outer[q].wait_recv()
            self.send_sum(4 + q, self.pair(k, q) + self.arrive[q].astype(F32))

    def finish(self):
        with jax.named_scope('inner03'):
            self.inner[0][3].wait_recv()
        with jax.named_scope('inner13'):
            self.inner[1][3].wait_recv()
        with jax.named_scope('straight0'):
            self.straight[0].wait_recv()
        with jax.named_scope('straight1'):
            self.straight[1].wait_recv()
        low = self.pair(3, 0, 2) + self.arrive_half[1].astype(F32)
        high = self.pair(3, 2, 2) + self.arrive_half[0].astype(F32)
        for k in (4, 6, 5, 7):
            with jax.named_scope('s%d' % k):
                self.outer[k].wait_recv()
        far = [self.arrive[4 + q].astype(F32) for q in range(4)]
        return jnp.concatenate([low, high], axis=-1) + jnp.concatenate(far, axis=-1)

    def drain(self):
        for copy in self.inner[0] + self.inner[1] + self.outer + self.straight:
            copy.wait_send()


GATHER_SEMS = [pltpu.SemaphoreType.DMA((Gather.COPIES,))] * 2
SCATTER_SEMS = [pltpu.SemaphoreType.DMA((Scatter.COPIES,))] * 2


def scatter_scratch(rows, dim):
    return [pltpu.VMEM((CHIPS, rows, dim), BF)] + [pltpu.VMEM((8, rows, dim // 4), BF)] * 2 + [pltpu.VMEM((2, rows, dim // 2), BF)] * 2


def put_part(part, value, col):
    rows, width = part.shape[2], value.shape[1]
    for b in range(CHIPS * CORES):
        part[b % CORES, b // CORES, :, pl.ds(col, width)] = value[b * rows:(b + 1) * rows].astype(BF)


def norm_stats(hidden_f):
    inv_rms = lax.rsqrt(jnp.mean(hidden_f * hidden_f, axis=-1, keepdims=True) + RMS_EPS)
    return hidden_f * inv_rms, inv_rms


def norm_bwd(grad_f, normed, inv_rms, gain):
    gain_part = jnp.sum(grad_f * normed, axis=0, keepdims=True)
    scaled = grad_f * gain
    return inv_rms * (scaled - normed * jnp.mean(scaled * normed, axis=-1, keepdims=True)), gain_part


def rope(values, cos2, sin2):
    return values * cos2 + pltpu.roll(values, values.shape[-1] // 2, axis=1) * sin2


def full(buf):
    blocks, rows, dim = buf.shape
    return buf[...].reshape(blocks * rows, dim)


def rope_tables(pos_row, freq_col):
    angles = jnp.transpose(freq_col * pos_row.astype(F32))
    lane = lax.broadcasted_iota(jnp.int32, angles.shape, 1)
    sin = jnp.sin(angles)
    return jnp.cos(angles), jnp.where(lane < angles.shape[1] // 2, -sin, sin)


def layer_kernel(tokens_hbm, positions_hbm, freq_hbm, gain_attn_hbm, gain_mlp_hbm, grad_hbm, emb_hbm, wq_hbm, wk_hbm, wv_hbm, wo_hbm, wg_hbm, wu_hbm, wd_hbm,
                 dx_out, hidden_out, n1_out, n2_out, gh_out, dh1_out, heads_out, act_out, dgu_out, dqkv_out,
                 emb, pick_buf, wqkv, wqkv_t, wo, wg, wu, wd, wsem, osem, n1_buf, n2_buf, gh_buf, dh1_buf,
                 emb_part, attn_part, dn2_part, mlp_part, dn1_part, heads_buf, gact, act_buf, dgu_buf, dqkv_buf,
                 q_buf, probs_buf, cos_ref, sin_ref, hidden_buf, dx_pair, tokens, positions, freq, gain_attn, gain_mlp, grad_own, small_sem, *comm):
    pos = Place()
    num_heads, dim, head_dim = wq_hbm.shape
    rows_local = emb_hbm.shape[0]
    blocks, rows, _ = n1_buf.shape
    seq, ffn = blocks * rows, wg.shape[1]
    scatters = [comm[5 * i:5 * i + 5] for i in range(5)]
    main_s, main_g, side, pair_s = (comm[25 + 2 * i:27 + 2 * i] for i in range(4))
    kq = num_heads * head_dim
    step = 512
    chunks = dim // step
    wide = dim // 2

    def emb_load(j):
        cols = pl.ds(pl.multiple_of(j * step, step), step)
        return pltpu.make_async_copy(emb_hbm.at[:, cols], emb.at[:, cols], wsem.at[j])

    small = ((tokens_hbm, tokens), (grad_hbm, gh_buf.at[pos.me]), (positions_hbm, positions), (freq_hbm, freq),
             (gain_attn_hbm, gain_attn), (gain_mlp_hbm, gain_mlp), (grad_hbm, grad_own))
    small = [pltpu.make_async_copy(src, dst, small_sem.at[k]) for k, (src, dst) in enumerate(small)]
    small[0].start()
    for j in range(chunks):
        emb_load(j).start()
    for copy in small[1:]:
        copy.start()
    pairs = [(wq_hbm.at[h], wqkv.at[:, pl.ds(h * head_dim, head_dim)]) for h in range(num_heads)]
    pairs += [(wk_hbm, wqkv.at[:, pl.ds(kq, head_dim)]), (wv_hbm, wqkv.at[:, pl.ds(kq + head_dim, head_dim)])]
    pairs += [(wo_hbm, wo), (wd_hbm, wd), (wg_hbm, wg), (wu_hbm, wu)]
    loads = [pltpu.make_async_copy(src, dst, wsem.at[chunks + k]) for k, (src, dst) in enumerate(pairs)]
    stores = []

    def store(src, dst):
        stores.append(pltpu.make_async_copy(src, dst, osem.at[len(stores)]))
        stores[-1].start()

    def halves(scatter, product):
        for h in range(2):
            put_part(scatter.part, product(h * wide), h * wide)
            scatter.start(h)

    def turn(src, dst, first):
        @pl.loop(0, src.shape[0] // 128)
        def _(j):
            at = pl.multiple_of(j * 128, 128)
            dst[first:first + src.shape[1], pl.ds(at, 128)] = jnp.transpose(src[pl.ds(at, 128), :])

    barrier = announce(pos)
    gather0 = Gather(pos, gh_buf, *side)
    scatter1 = Scatter(pos, emb_part, *scatters[0], *main_s)

    def looked_up(h):
        @pl.loop(h * chunks // 2, (h + 1) * chunks // 2)
        def _(j):
            col = pl.multiple_of(j * step, step)
            emb_load(j).wait()
            put_part(scatter1.part, dot(pick_buf[...], emb[:, pl.ds(col, step)]), col)

    with jax.named_scope('lookup_low'):
        small[0].wait()
        local = jnp.transpose(jnp.broadcast_to(tokens[...] - pos.me * rows_local, (seq, seq)))
        lane = lax.broadcasted_iota(jnp.int32, (seq, seq), 1)
        for j in range(rows_local // seq):
            pick_buf[:, j * seq:(j + 1) * seq] = jnp.where(local == lane + j * seq, 1.0, 0.0).astype(BF)
        looked_up(0)
        for load in loads:
            load.start()
    with jax.named_scope('barrier'):
        pl.semaphore_wait(barrier, 3)
    scatter1.start(0)
    small[1].wait()
    gather0.start()
    with jax.named_scope('lookup_high'):
        looked_up(1)
        scatter1.start(1)
    with jax.named_scope('rs1'):
        scatter1.relay_low()
        scatter1.relay_high()
        gather0.relay()
        scatter1.relay_far()
        gather0.finish()
        for copy in small[2:]:
            copy.wait()
        cos_ref[...], sin_ref[...] = rope_tables(positions[...], freq[...])
        x0 = scatter1.finish()
    with jax.named_scope('norm1'):
        normed1, inv1 = norm_stats(x0)
        n1_buf[pos.me] = (normed1 * gain_attn[...]).astype(BF)
    with jax.named_scope('ag1'):
        gather1 = Gather(pos, n1_buf, *main_g)
        gather1.start()
        store(gh_buf, gh_out)
    with jax.named_scope('turn_gate'):
        loads[7].wait()
        turn(wg, emb, 0)
    with jax.named_scope('ag1_relay'):
        gather1.relay()
    with jax.named_scope('turn_up'):
        loads[8].wait()
        turn(wu, emb, ffn)
    with jax.named_scope('ag1_finish'):
        gather1.finish()
    store(n1_buf, n1_out)

    with jax.named_scope('qkv'):
        for load in loads[:5]:
            load.wait()
        qkv = dot(full(n1_buf), wqkv[...])
    with jax.named_scope('attention'):
        cos2, sin2 = cos_ref[...], sin_ref[...]
        keys = rope(qkv[:, kq:kq + head_dim], cos2, sin2).astype(BF)
        values = qkv[:, kq + head_dim:].astype(BF)
        causal = lax.broadcasted_iota(jnp.int32, (seq, seq), 0) >= lax.broadcasted_iota(jnp.int32, (seq, seq), 1)
        for h in range(num_heads):
            cols = slice(h * head_dim, (h + 1) * head_dim)
            query = rope(qkv[:, cols], cos2, sin2).astype(BF)
            q_buf[:, cols] = query
            scores = jnp.where(causal, dot_bt(query, keys) * (head_dim ** -0.5), -1e30)
            expd = jnp.exp(scores - jnp.max(scores, axis=-1, keepdims=True))
            probs = expd / jnp.sum(expd, axis=-1, keepdims=True)
            probs_buf[h] = probs
            heads_buf[:, cols] = dot(probs.astype(BF), values).astype(BF)
    store(heads_buf, heads_out)
    with jax.named_scope('w_out'):
        loads[5].wait()
        scatter3 = Scatter(pos, attn_part, *scatters[1], *main_s)
        scatter1.drain()
        halves(scatter3, lambda col: dot(heads_buf[...], wo[:, pl.ds(col, wide)]))

    with jax.named_scope('rs3_a'):
        scatter3.relay_low()
        scatter3.relay_high()

    with jax.named_scope('grad_act'):
        loads[6].wait()

        @pl.loop(0, ffn // 256)
        def _(j):
            cols = pl.ds(pl.multiple_of(j * 256, 256), 256)
            gact[:, cols] = dot_bt(full(gh_buf), wd[cols, :]).astype(BF)

    with jax.named_scope('rs3_b'):
        scatter3.relay_far()
        h1_bf = (x0 + scatter3.finish()).astype(BF)
    with jax.named_scope('norm2'):
        h1 = h1_bf.astype(F32)
        normed2, inv2 = norm_stats(h1)
        n2_buf[pos.me] = (normed2 * gain_mlp[...]).astype(BF)
    with jax.named_scope('ag4'):
        gather4 = Gather(pos, n2_buf, *main_g)
        gather1.drain()
        gather4.start()
        turn(wqkv, wqkv_t, 0)
        gather4.relay()
        gather4.finish()
    store(n2_buf, n2_out)

    with jax.named_scope('gate_up'):
        @pl.loop(0, ffn // 512)
        def _(j):
            cols = pl.ds(pl.multiple_of(j * 512, 512), 512)
            n2 = full(n2_buf)
            gate_pre = dot(n2, wg[:, cols])
            up_pre = dot(n2, wu[:, cols])
            sig = jax.nn.sigmoid(gate_pre)
            gate_act = gate_pre * sig
            act_buf[:, cols] = (gate_act * up_pre).astype(BF)
            grad_act = gact[:, cols].astype(F32)
            dgu_buf[:, pl.ds(pl.multiple_of(ffn + j * 512, 512), 512)] = (grad_act * gate_act).astype(BF)
            dgu_buf[:, cols] = (grad_act * up_pre * sig * (1.0 + gate_pre * (1.0 - sig))).astype(BF)

    store(act_buf, act_out)
    store(dgu_buf, dgu_out)
    with jax.named_scope('dn2'):
        scatter6 = Scatter(pos, dn2_part, *scatters[2], *main_s)
        scatter3.drain()
        halves(scatter6, lambda col: dot(dgu_buf[...], emb[:, pl.ds(col, wide)]))

    with jax.named_scope('rs6_a'):
        scatter6.relay_low()
        scatter6.relay_high()
    with jax.named_scope('w_down'):
        for h in range(2):
            put_part(mlp_part, dot(act_buf[...], wd[:, h * wide:(h + 1) * wide]), h * wide)
        gather0.drain()
        scatter5 = Scatter(pos, mlp_part, *scatters[3], *side)
        scatter5.start(0)
        scatter5.start(1)
    with jax.named_scope('rs6_b'):
        scatter6.relay_far()
        scatter5.relay_low()
        scatter5.relay_high()
        grad_n2 = scatter6.finish().astype(BF).astype(F32)
    with jax.named_scope('norm2_bwd'):
        grad_h1_norm, gain_mlp_part = norm_bwd(grad_n2, normed2, inv2, gain_mlp[...])
        grad_h1 = (grad_own[...].astype(F32) + grad_h1_norm).astype(BF)
        dh1_buf[pos.me] = grad_h1
    gather7 = Gather(pos, dh1_buf, *main_g)
    gather4.drain()
    gather7.start()
    with jax.named_scope('ag7'):
        gather7.relay()
        scatter5.relay_far()
        gather7.finish()
    store(dh1_buf, dh1_out)

    with jax.named_scope('dheads'):
        dheads = dot_bt(full(dh1_buf), wo[...]).astype(BF)
    with jax.named_scope('attention_bwd'):
        nsin2 = -sin2
        dkeys = jnp.zeros((seq, head_dim), F32)
        dvalues = jnp.zeros((seq, head_dim), F32)
        for h in range(num_heads):
            cols = slice(h * head_dim, (h + 1) * head_dim)
            dhead = dheads[:, cols]
            probs = probs_buf[h]
            dprobs = dot_bt(dhead, values).astype(BF).astype(F32)
            dvalues += dot_at(probs.astype(BF), dhead)
            inner = jnp.sum(dprobs * probs, axis=-1, keepdims=True)
            dscores = (probs * (dprobs - inner) * (head_dim ** -0.5)).astype(BF)
            dquery = dot(dscores, keys).astype(BF)
            dkeys += dot_at(dscores, q_buf[:, cols])
            dqkv_buf[:, cols] = rope(dquery.astype(F32), cos2, nsin2).astype(BF)
        dqkv_buf[:, kq:kq + head_dim] = rope(dkeys.astype(BF).astype(F32), cos2, nsin2).astype(BF)
        dqkv_buf[:, kq + head_dim:] = dvalues.astype(BF)
    store(dqkv_buf, dqkv_out)

    with jax.named_scope('dn1'):
        scatter8 = Scatter(pos, dn1_part, *scatters[4], *main_s)
        scatter6.drain()
        halves(scatter8, lambda col: dot(dqkv_buf[...], wqkv_t[:, pl.ds(col, wide)]))

    with jax.named_scope('rs8'):
        scatter8.relay_low()
        scatter8.relay_high()
        hidden_buf[...] = (h1 + scatter5.finish()).astype(BF)
        store(hidden_buf, hidden_out)
        scatter8.relay_far()
        grad_n1 = scatter8.finish().astype(BF).astype(F32)
    with jax.named_scope('norm1_bwd'):
        grad_x_norm, gain_attn_part = norm_bwd(grad_n1, normed1, inv1, gain_attn[...])
        dx_pair[pos.core, 0:rows, :] = (grad_h1.astype(F32) + grad_x_norm).astype(BF)
        gain_parts = jnp.concatenate([gain_attn_part, gain_mlp_part], axis=0)
        high = gain_parts.astype(BF)
        dx_pair[pos.core, rows:rows + 2, :] = high
        dx_pair[pos.core, rows + 2:rows + 4, :] = (gain_parts - high.astype(F32)).astype(BF)
    with jax.named_scope('pair'):
        mine = remote(dx_pair.at[pos.core], dx_pair.at[pos.core], *(sem.at[0] for sem in pair_s), pos.partner)
        theirs = remote(dx_pair.at[pos.other], dx_pair.at[pos.other], *(sem.at[0] for sem in pair_s), pos.partner)
        mine.start()
        theirs.wait_recv()
        dx_out[...] = dx_pair[...]
        mine.wait_send()
    with jax.named_scope('tail'):
        for op in (scatter5, scatter8, gather7):
            op.drain()
        for copy in stores:
            copy.wait()


def layer(tokens, positions, gain_attn, gain_mlp, grad_own, emb, wq, wk, wv, wo, wg, wu, wd):
    num_heads, dim, head_dim = wq.shape
    blocks = CHIPS * CORES
    seq, ffn, rows_local = tokens.shape[1], wg.shape[1], emb.shape[0]
    rows = seq // blocks
    if rows_local != 2 * ffn:
        raise ValueError('shard rows')
    half = head_dim // 2
    freq = np.float32(ROPE_THETA) ** (-np.arange(half, dtype=np.float32) * np.float32(2.0 / head_dim))
    freq = jnp.asarray(np.concatenate([freq, freq])[:, None], F32)
    vmem = pl.BlockSpec(memory_space=pltpu.VMEM)
    hbm = pl.BlockSpec(memory_space=pltpu.HBM)
    width = num_heads * head_dim
    wide = width + 2 * head_dim
    sds = jax.ShapeDtypeStruct
    outs = [sds((CORES, rows + 4, dim), BF), sds((rows, dim), BF)] + [sds((blocks, rows, dim), BF)] * 4
    outs += [sds((seq, width), BF), sds((seq, ffn), BF), sds((seq, 2 * ffn), BF), sds((seq, wide), BF)]
    part = pltpu.VMEM((CORES, CHIPS, rows, dim), BF)
    gathered = pltpu.VMEM((blocks, rows, dim), BF)
    table = pltpu.VMEM((seq, head_dim), F32)
    scratch = [pltpu.VMEM((rows_local, dim), BF), pltpu.VMEM((seq, rows_local), BF), pltpu.VMEM((dim, wide), BF), pltpu.VMEM((wide, dim), BF),
               pltpu.VMEM((width, dim), BF), pltpu.VMEM((dim, ffn), BF),
               pltpu.VMEM((dim, ffn), BF), pltpu.VMEM((ffn, dim), BF), pltpu.SemaphoreType.DMA((15,)), pltpu.SemaphoreType.DMA((9,))]
    scratch += [gathered] * 4 + [part] * 5 + [pltpu.VMEM((seq, width), BF)]
    scratch += [pltpu.VMEM((seq, ffn), BF)] * 2 + [pltpu.VMEM((seq, 2 * ffn), BF), pltpu.VMEM((seq, wide), BF), pltpu.VMEM((seq, width), BF),
                                                   pltpu.VMEM((num_heads, seq, seq), F32), table, table,
                                                   pltpu.VMEM((rows, dim), BF), pltpu.VMEM((CORES, rows + 4, dim), BF),
                                                   pltpu.VMEM((1, seq), jnp.int32), pltpu.VMEM((1, seq), jnp.int32), pltpu.VMEM((head_dim, 1), F32),
                                                   pltpu.VMEM((1, dim), F32), pltpu.VMEM((1, dim), F32), pltpu.VMEM((rows, dim), BF),
                                                   pltpu.SemaphoreType.DMA((7,))]
    scratch += scatter_scratch(rows, dim) * 5 + SCATTER_SEMS + GATHER_SEMS * 2 + [pltpu.SemaphoreType.DMA((1,))] * 2
    return pl.pallas_call(
        layer_kernel, out_shape=outs, in_specs=[hbm] * 14, out_specs=[vmem] + [hbm] * 9,
        scratch_shapes=scratch,
        compiler_params=pltpu.CompilerParams(collective_id=0, has_side_effects=True, vmem_limit_bytes=VMEM_FULL),
        name='layer',
    )(tokens, positions, freq, gain_attn, gain_mlp, grad_own, emb, wq, wk, wv, wo, wg, wu, wd)


def grads_kernel(n1, n2, dqkv, dgate, dup, heads, act, dh1, gh, hidden_in,
                 gw_query, gw_key, gw_value, gw_out, gw_gate, gw_up, gw_down, hidden):
    num_heads, _, head_dim = gw_query.shape
    width = num_heads * head_dim

    @pl.when(pl.program_id(0) == 0)
    def _():
        hidden[...] = hidden_in[...]

    gw_gate[...] = dot_at(n2[...], dgate[...])
    gw_up[...] = dot_at(n2[...], dup[...])
    gw_down[...] = dot_at(act[...], gh[...])
    both = dot_at(n1[...], dqkv[...])
    for h in range(num_heads):
        gw_query[h] = both[:, h * head_dim:(h + 1) * head_dim]
    gw_key[...] = both[:, width:width + head_dim]
    gw_value[...] = both[:, width + head_dim:]
    gw_out[...] = dot_at(heads[...], dh1[...])


def grads(n1, n2, dqkv, dgu, heads, act, dh1, gh, hidden, head_dim):
    seq, dim = n1.shape
    width, ffn = heads.shape[1], act.shape[1]
    num_heads = width // head_dim
    tile = 256
    sds = jax.ShapeDtypeStruct

    def whole(x):
        return pl.BlockSpec(x.shape, lambda i: (0,) * len(x.shape))

    def by_col(n):
        return pl.BlockSpec((n, tile), lambda i: (0, i))

    def by_row(n):
        return pl.BlockSpec((tile, n), lambda i: (i, 0))

    return pl.pallas_call(
        grads_kernel, grid=(dim // tile,),
        out_shape=[sds((num_heads, dim, head_dim), F32), sds((dim, head_dim), F32), sds((dim, head_dim), F32), sds((width, dim), F32),
                   sds((dim, ffn), F32), sds((dim, ffn), F32), sds((ffn, dim), F32), sds(hidden.shape, BF)],
        in_specs=[by_col(seq), by_col(seq), whole(dqkv), pl.BlockSpec((seq, ffn), lambda i: (0, 0)),
                  pl.BlockSpec((seq, ffn), lambda i: (0, 1)), whole(heads), whole(act), by_col(seq), by_col(seq), whole(hidden)],
        out_specs=[pl.BlockSpec((num_heads, tile, head_dim), lambda i: (0, i, 0)), by_row(head_dim), by_row(head_dim), by_col(width),
                   by_row(ffn), by_row(ffn), by_col(ffn), whole(hidden)],
        compiler_params=pltpu.CompilerParams(vmem_limit_bytes=VMEM_FULL),
        cost_estimate=pl.CostEstimate(flops=20_000_000_000, bytes_accessed=50_000_000, transcendentals=0),
        name='grads',
    )(n1, n2, dqkv, dgu, dgu, heads, act, dh1, gh, hidden)


def emb_grad_kernel(tokens, *refs):
    pairs = refs[:CHIPS]
    g_emb, g_attn, g_mlp, dx, gains, ring, sem = refs[CHIPS:]
    seq, rows = dx.shape[0], dx.shape[0] // (CHIPS * CORES)
    me = lax.axis_index('tp')
    for k, pair in enumerate(pairs):
        chip = (me // CORES + CHIPS - k) % CHIPS
        for core in range(CORES):
            source = chip * CORES + core
            dx[pl.ds(pl.multiple_of(source * rows, rows), rows), :] = pair[core, 0:rows, :]
            gains[source] = pair[core, rows:rows + 2, :].astype(F32) + pair[core, rows + 2:rows + 4, :].astype(F32)

    slots, height = ring.shape[0], ring.shape[1]
    rows_local = g_emb.shape[0]
    local = tokens[...] - me * rows_local
    row = lax.broadcasted_iota(jnp.int32, (height, seq), 0)
    copies = []
    for c in range(rows_local // height):
        slot = c % slots
        if c >= slots:
            copies[c - slots].wait()
        ring[slot] = dot(jnp.where(row + c * height == local, 1.0, 0.0).astype(BF), dx[...])
        copies.append(pltpu.make_async_copy(ring.at[slot], g_emb.at[pl.ds(c * height, height)], sem.at[slot]))
        copies[-1].start()
    total = gains[0]
    for i in range(1, CHIPS * CORES):
        total = total + gains[i]
    g_attn[...] = total[0:1, :]
    g_mlp[...] = total[1:2, :]
    for copy in copies[-slots:]:
        copy.wait()


def emb_grad(tokens, pairs, rows_local):
    seq, dim = tokens.shape[1], pairs[0].shape[2]
    height, slots = 256, 4
    sds = jax.ShapeDtypeStruct
    vmem = pl.BlockSpec(memory_space=pltpu.VMEM)
    gain = sds((1, dim), F32)
    return pl.pallas_call(
        emb_grad_kernel, out_shape=[sds((rows_local, dim), F32), gain, gain],
        in_specs=[vmem] * (1 + len(pairs)), out_specs=[pl.BlockSpec(memory_space=pltpu.HBM), vmem, vmem],
        scratch_shapes=[pltpu.VMEM((seq, dim), BF), pltpu.VMEM((CHIPS * CORES, 2, dim), F32), pltpu.VMEM((slots, height, dim), F32),
                        pltpu.SemaphoreType.DMA((slots,))],
        compiler_params=pltpu.CompilerParams(vmem_limit_bytes=VMEM_FULL),
        name='emb_grad',
    )(tokens, *pairs)


def solution(mesh):
    if mesh.shape['tp'] != CHIPS * CORES:
        raise ValueError('tp size')
    in_specs = (P('dp', None), P('dp', None), P('tp', None), P(None), P(None),
                P(None, 'tp', None), P(None, 'tp', None), P(None, 'tp', None), P('tp', None, None),
                P(None, 'tp'), P(None, 'tp'), P('tp', None), P('dp', 'tp', None))
    out_specs = (P('dp', 'tp', None), P(('dp', 'tp'), None),
                 P('dp', 'tp', None), P('dp', 'tp', None), P('dp', 'tp', None), P(('dp', 'tp'), None, None),
                 P('dp', 'tp'), P('dp', 'tp'), P(('dp', 'tp'), None), P('dp'), P('dp'))

    def device_fn(tokens, positions, emb_shard, gain_attn, gain_mlp, w_query, w_key, w_value, w_out, w_gate, w_up, w_down, grad_hidden):
        rows_local, dim = emb_shard.shape
        seq = tokens.shape[1]
        num_heads, head_dim = w_query.shape[1], w_query.shape[2]
        wq = jnp.transpose(w_query, (1, 0, 2))
        wk, wv = w_key.reshape(dim, head_dim), w_value.reshape(dim, head_dim)
        wo = w_out.reshape(num_heads * head_dim, dim)

        dx_pair, hidden, n1, n2, gh, dh1, heads, act, dgu, dqkv = layer(
            tokens, positions, gain_attn[None, :], gain_mlp[None, :], grad_hidden[0], emb_shard, wq, wk, wv, wo, w_gate, w_up, w_down)
        n = CHIPS * CORES
        arrived = [dx_pair] + [lax.ppermute(dx_pair, 'tp', [(i, (i + k * CORES) % n) for i in range(n)]) for k in range(1, CHIPS)]
        n1, n2, gh, dh1 = (x.reshape(seq, dim) for x in (n1, n2, gh, dh1))
        gw_query, gw_key, gw_value, gw_out, gw_gate, gw_up, gw_down, hidden = grads(
            n1, n2, dqkv, dgu, heads, act, dh1, gh, hidden, head_dim)
        g_emb, g_attn, g_mlp = emb_grad(tokens, arrived, rows_local)
        return (hidden[None], g_emb, jnp.transpose(gw_query, (1, 0, 2)), gw_key.reshape(dim, 1, head_dim),
                gw_value.reshape(dim, 1, head_dim), gw_out.reshape(num_heads, head_dim, dim),
                gw_gate, gw_up, gw_down, g_attn[0], g_mlp[0])

    return jax.shard_map(device_fn, mesh=mesh, in_specs=in_specs, out_specs=out_specs, check_vma=False)
```

```python
import jax
import jax.numpy as jnp
import numpy as np
from jax import lax
from jax.experimental import pallas as pl
from jax.experimental.pallas import tpu as pltpu
from jax.sharding import PartitionSpec as P

ROPE_THETA = 1000000.0
RMS_EPS = 1e-5
BF = jnp.bfloat16
F32 = jnp.float32
VMEM_FULL = 67043328
CHIPS = 4
CORES = 2


def dot(a, b):
    return lax.dot_general(a, b, (((1,), (0,)), ((), ())), preferred_element_type=F32)


def dot_bt(a, b):
    return lax.dot_general(a, b, (((1,), (1,)), ((), ())), preferred_element_type=F32)


def dot_at(a, b):
    return lax.dot_general(a, b, (((0,), (0,)), ((), ())), preferred_element_type=F32)


class Place:
    def __init__(self):
        me = lax.axis_index('tp')
        self.chip, self.core = me // CORES, me % CORES
        self.right_chip = (self.chip + 1) % CHIPS
        self.left_chip = (self.chip + CHIPS - 1) % CHIPS
        self.far_chip = (self.chip + 2) % CHIPS
        self.me = me
        self.other = 1 - self.core
        self.partner = self.chip * CORES + self.other
        self.right = self.right_chip * CORES + self.core
        self.left = self.left_chip * CORES + self.core
        self.far = self.far_chip * CORES + self.core


def remote(src, dst, send, recv, device):
    return pltpu.make_async_remote_copy(src_ref=src, dst_ref=dst, send_sem=send, recv_sem=recv,
                                        device_id={'tp': device}, device_id_type=pl.DeviceIdType.MESH)


def announce(pos):
    barrier = pltpu.get_barrier_semaphore()
    for device in (pos.left, pos.right, pos.partner):
        pl.semaphore_signal(barrier, inc=1, device_id={'tp': device}, device_id_type=pl.DeviceIdType.MESH)
    return barrier


def all_sends(buf, send):
    return pltpu.make_async_copy(buf.at[pl.ds(0, 7)], buf.at[pl.ds(0, 7)], send.at[0])


class Gather:
    COPIES = 19

    def __init__(self, pos, buf, send, recv):
        p = pos
        quarter = buf.shape[-1] // 4
        other = p.other - p.core
        low, high, whole = (0, 2), (2, 4), (0, 4)
        pieces = ((0, 1), (1, 2), (2, 3), (3, 4))

        def copy(index, slot, part, device):
            ref = buf.at[slot, :, pl.ds(part[0] * quarter, (part[1] - part[0]) * quarter)]
            return remote(ref, ref, send.at[0], recv.at[index], device)

        self.send, self.buf = send, buf
        plan = [((p.me, pieces[0], p.right), (p.left, pieces[0])), ((p.me, pieces[2], p.left), (p.right, pieces[2])),
                ((p.me, pieces[1], p.right), (p.left, pieces[1])), ((p.me, pieces[3], p.left), (p.right, pieces[3])),
                ((p.me, whole, p.partner), (p.partner, whole)),
                ((p.me, high, p.right), (p.left, high)), ((p.me, low, p.left), (p.right, low)),
                ((p.left, pieces[0], p.right), (p.far, pieces[0])), ((p.right, pieces[2], p.left), (p.far, pieces[2])),
                ((p.left, pieces[1], p.right), (p.far, pieces[1])), ((p.right, pieces[3], p.left), (p.far, pieces[3])),
                ((p.left, low, p.partner), (p.left + other, low)), ((p.right, high, p.partner), (p.right + other, high)),
                ((p.left, high, p.partner), (p.left + other, high)), ((p.right, low, p.partner), (p.right + other, low))]
        plan += [((p.far, pieces[i], p.partner), (p.far + other, pieces[i])) for i in (0, 2, 1, 3)]
        self.out = [copy(i, *sent) for i, (sent, _) in enumerate(plan)]
        self.into = [copy(i, slot, part, p.partner) for i, (_, (slot, part)) in enumerate(plan)]

    def start(self):
        for i in range(7):
            self.out[i].start()

    def pass_on(self, steps):
        for i, onward in steps:
            with jax.named_scope('g%d' % i):
                self.into[i].wait_recv()
            for j in onward:
                self.out[j].start()

    def relay(self):
        self.pass_on(((0, (7,)), (1, (8,)), (2, (9, 11)), (3, (10, 12)), (5, (13,)), (6, (14,))))

    def finish(self):
        self.pass_on(((7, (15,)), (8, (16,)), (9, (17,)), (10, (18,))))
        for i in (4, 11, 12, 13, 14, 15, 16, 17, 18):
            with jax.named_scope('g%d' % i):
                self.into[i].wait_recv()

    def drain(self):
        all_sends(self.buf, self.send).wait()


class Scatter:
    COPIES = 18

    def __init__(self, pos, blocks, part, from_partner, work, arrive, work_half, arrive_half, send, recv):
        p = pos
        self.blocks, self.send = blocks, send
        self.pos, self.part, self.from_partner = p, part, from_partner
        self.work, self.arrive, self.work_half, self.arrive_half = work, arrive, work_half, arrive_half
        self.quarter = work.shape[-1]
        self.chips = (p.far_chip, p.right_chip, p.left_chip, p.chip)
        self.inner = [[remote(part.at[p.other, y, :, self.cols(2 * h, 2)], from_partner.at[y, :, self.cols(2 * h, 2)],
                              send.at[0], recv.at[4 * h + k], p.partner) for k, y in enumerate(self.chips)]
                      for h in range(2)]
        self.outer = [remote(work.at[k], arrive.at[k], send.at[0], recv.at[8 + k], p.right if k % 4 < 2 else p.left)
                      for k in range(8)]
        self.straight = [remote(work_half.at[k], arrive_half.at[k], send.at[0], recv.at[16 + k], device)
                         for k, device in enumerate((p.right, p.left))]

    def cols(self, q, n=1):
        return pl.ds(q * self.quarter, n * self.quarter)

    def pair(self, k, q, n=1):
        y = self.chips[k]
        return self.part[self.pos.core, y, :, self.cols(q, n)].astype(F32) + self.from_partner[y, :, self.cols(q, n)].astype(F32)

    def send_sum(self, k, value):
        self.work[k] = value.astype(BF)
        self.outer[k].start()

    def send_straight(self, k, value):
        self.work_half[k] = value.astype(BF)
        self.straight[k].start()

    def start(self, h):
        for copy in self.inner[h]:
            copy.start()

    def relay_low(self):
        with jax.named_scope('inner00'):
            self.inner[0][0].wait_recv()
        self.send_sum(0, self.pair(0, 0))
        self.send_sum(1, self.pair(0, 1))
        with jax.named_scope('inner02'):
            self.inner[0][2].wait_recv()
        self.send_straight(1, self.pair(2, 0, 2))

    def relay_high(self):
        with jax.named_scope('inner10'):
            self.inner[1][0].wait_recv()
        self.send_sum(2, self.pair(0, 2))
        self.send_sum(3, self.pair(0, 3))
        with jax.named_scope('inner11'):
            self.inner[1][1].wait_recv()
        self.send_straight(0, self.pair(1, 2, 2))

    def relay_far(self):
        with jax.named_scope('inner01'):
            self.inner[0][1].wait_recv()
        with jax.named_scope('inner12'):
            self.inner[1][2].wait_recv()
        for q, k in ((0, 1), (2, 2), (1, 1), (3, 2)):
            with jax.named_scope('s%d' % q):
                self.outer[q].wait_recv()
            self.send_sum(4 + q, self.pair(k, q) + self.arrive[q].astype(F32))

    def finish(self):
        with jax.named_scope('inner03'):
            self.inner[0][3].wait_recv()
        with jax.named_scope('inner13'):
            self.inner[1][3].wait_recv()
        with jax.named_scope('straight0'):
            self.straight[0].wait_recv()
        with jax.named_scope('straight1'):
            self.straight[1].wait_recv()
        low = self.pair(3, 0, 2) + self.arrive_half[1].astype(F32)
        high = self.pair(3, 2, 2) + self.arrive_half[0].astype(F32)
        for k in (4, 6, 5, 7):
            with jax.named_scope('s%d' % k):
                self.outer[k].wait_recv()
        far = [self.arrive[4 + q].astype(F32) for q in range(4)]
        return jnp.concatenate([low, high], axis=-1) + jnp.concatenate(far, axis=-1)

    def drain(self):
        all_sends(self.blocks, self.send).wait()


GATHER_SEMS = [pltpu.SemaphoreType.DMA((1,)), pltpu.SemaphoreType.DMA((Gather.COPIES,))]
SCATTER_SEMS = [pltpu.SemaphoreType.DMA((1,)), pltpu.SemaphoreType.DMA((Scatter.COPIES,))]


def scatter_scratch(rows, dim):
    return [pltpu.VMEM((CHIPS, rows, dim), BF)] + [pltpu.VMEM((8, rows, dim // 4), BF)] * 2 + [pltpu.VMEM((2, rows, dim // 2), BF)] * 2


def put_part(part, value, col):
    rows, width = part.shape[2], value.shape[1]
    for b in range(CHIPS * CORES):
        part[b % CORES, b // CORES, :, pl.ds(col, width)] = value[b * rows:(b + 1) * rows].astype(BF)


def norm_stats(hidden_f):
    inv_rms = lax.rsqrt(jnp.mean(hidden_f * hidden_f, axis=-1, keepdims=True) + RMS_EPS)
    return hidden_f * inv_rms, inv_rms


def norm_bwd(grad_f, normed, inv_rms, gain):
    gain_part = jnp.sum(grad_f * normed, axis=0, keepdims=True)
    scaled = grad_f * gain
    return inv_rms * (scaled - normed * jnp.mean(scaled * normed, axis=-1, keepdims=True)), gain_part


def rope(values, cos2, sin2):
    return values * cos2 + pltpu.roll(values, values.shape[-1] // 2, axis=1) * sin2


def full(buf):
    blocks, rows, dim = buf.shape
    return buf[...].reshape(blocks * rows, dim)


def rope_tables(pos_row, freq_col):
    angles = jnp.transpose(freq_col * pos_row.astype(F32))
    lane = lax.broadcasted_iota(jnp.int32, angles.shape, 1)
    sin = jnp.sin(angles)
    return jnp.cos(angles), jnp.where(lane < angles.shape[1] // 2, -sin, sin)


def layer_kernel(tokens_hbm, positions_hbm, freq_hbm, gain_attn_hbm, gain_mlp_hbm, grad_hbm, emb_hbm, wq_hbm, wk_hbm, wv_hbm, wo_hbm, wg_hbm, wu_hbm, wd_hbm,
                 dx_out, hidden_out, n1_out, n2_out, gh_out, dh1_out, heads_out, act_out, dgu_out, dqkv_out,
                 emb, pick_buf, wqkv, wqkv_t, wo, wg, wu, wd, wsem, osem, n1_buf, n2_buf, gh_buf, dh1_buf,
                 emb_part, attn_part, dn2_part, mlp_part, dn1_part, heads_buf, gact, act_buf, dgu_buf, dqkv_buf,
                 q_buf, probs_buf, cos_ref, sin_ref, hidden_buf, dx_pair, tokens, positions, freq, gain_attn, gain_mlp, grad_own, small_sem, *comm):
    pos = Place()
    num_heads, dim, head_dim = wq_hbm.shape
    rows_local = emb_hbm.shape[0]
    blocks, rows, _ = n1_buf.shape
    seq, ffn = blocks * rows, wg.shape[1]
    scatters = [comm[5 * i:5 * i + 5] for i in range(5)]
    main_s, main_g, side, pair_s = (comm[25 + 2 * i:27 + 2 * i] for i in range(4))
    kq = num_heads * head_dim
    step = 512
    chunks = dim // step
    wide = dim // 2

    def emb_load(j):
        cols = pl.ds(pl.multiple_of(j * step, step), step)
        return pltpu.make_async_copy(emb_hbm.at[:, cols], emb.at[:, cols], wsem.at[j])

    small = ((tokens_hbm, tokens), (grad_hbm, gh_buf.at[pos.me]), (positions_hbm, positions), (freq_hbm, freq),
             (gain_attn_hbm, gain_attn), (gain_mlp_hbm, gain_mlp), (grad_hbm, grad_own))
    small = [pltpu.make_async_copy(src, dst, small_sem.at[k]) for k, (src, dst) in enumerate(small)]
    small[0].start()
    for j in range(chunks):
        emb_load(j).start()
    for copy in small[1:]:
        copy.start()
    pairs = [(wq_hbm.at[h], wqkv.at[:, pl.ds(h * head_dim, head_dim)]) for h in range(num_heads)]
    pairs += [(wk_hbm, wqkv.at[:, pl.ds(kq, head_dim)]), (wv_hbm, wqkv.at[:, pl.ds(kq + head_dim, head_dim)])]
    pairs += [(wo_hbm, wo), (wd_hbm, wd), (wg_hbm, wg), (wu_hbm, wu)]
    loads = [pltpu.make_async_copy(src, dst, wsem.at[chunks + k]) for k, (src, dst) in enumerate(pairs)]
    stores = []

    def store(src, dst):
        stores.append(pltpu.make_async_copy(src, dst, osem.at[len(stores)]))
        stores[-1].start()

    def halves(scatter, product):
        for h in range(2):
            put_part(scatter.part, product(h * wide), h * wide)
            scatter.start(h)

    def turn(src, dst, first):
        @pl.loop(0, src.shape[0] // 128)
        def _(j):
            at = pl.multiple_of(j * 128, 128)
            dst[first:first + src.shape[1], pl.ds(at, 128)] = jnp.transpose(src[pl.ds(at, 128), :])

    barrier = announce(pos)
    gather0 = Gather(pos, gh_buf, *side)
    scatter1 = Scatter(pos, n1_buf, emb_part, *scatters[0], *main_s)

    def looked_up(h):
        @pl.loop(h * chunks // 2, (h + 1) * chunks // 2)
        def _(j):
            col = pl.multiple_of(j * step, step)
            emb_load(j).wait()
            put_part(scatter1.part, dot(pick_buf[...], emb[:, pl.ds(col, step)]), col)

    with jax.named_scope('lookup_low'):
        small[0].wait()
        local = jnp.transpose(jnp.broadcast_to(tokens[...] - pos.me * rows_local, (seq, seq)))
        lane = lax.broadcasted_iota(jnp.int32, (seq, seq), 1)
        for j in range(rows_local // seq):
            pick_buf[:, j * seq:(j + 1) * seq] = jnp.where(local == lane + j * seq, 1.0, 0.0).astype(BF)
        looked_up(0)
        for load in loads:
            load.start()
    with jax.named_scope('barrier'):
        pl.semaphore_wait(barrier, 3)
    scatter1.start(0)
    small[1].wait()
    gather0.start()
    with jax.named_scope('lookup_high'):
        looked_up(1)
        scatter1.start(1)
    with jax.named_scope('rs1'):
        scatter1.relay_low()
        scatter1.relay_high()
        gather0.relay()
        scatter1.relay_far()
        gather0.finish()
        for copy in small[2:]:
            copy.wait()
        cos_ref[...], sin_ref[...] = rope_tables(positions[...], freq[...])
        x0 = scatter1.finish()
    with jax.named_scope('norm1'):
        normed1, inv1 = norm_stats(x0)
        n1_buf[pos.me] = (normed1 * gain_attn[...]).astype(BF)
    with jax.named_scope('ag1'):
        gather1 = Gather(pos, n1_buf, *main_g)
        gather1.start()
        store(gh_buf, gh_out)
    with jax.named_scope('turn_gate'):
        loads[7].wait()
        turn(wg, emb, 0)
    with jax.named_scope('ag1_relay'):
        gather1.relay()
    with jax.named_scope('turn_up'):
        loads[8].wait()
        turn(wu, emb, ffn)
    with jax.named_scope('ag1_finish'):
        gather1.finish()
    store(n1_buf, n1_out)

    with jax.named_scope('qkv'):
        for load in loads[:5]:
            load.wait()
        qkv = dot(full(n1_buf), wqkv[...])
    with jax.named_scope('attention'):
        cos2, sin2 = cos_ref[...], sin_ref[...]
        keys = rope(qkv[:, kq:kq + head_dim], cos2, sin2).astype(BF)
        values = qkv[:, kq + head_dim:].astype(BF)
        causal = lax.broadcasted_iota(jnp.int32, (seq, seq), 0) >= lax.broadcasted_iota(jnp.int32, (seq, seq), 1)
        for h in range(num_heads):
            cols = slice(h * head_dim, (h + 1) * head_dim)
            query = rope(qkv[:, cols], cos2, sin2).astype(BF)
            q_buf[:, cols] = query
            scores = jnp.where(causal, dot_bt(query, keys) * (head_dim ** -0.5), -1e30)
            expd = jnp.exp(scores - jnp.max(scores, axis=-1, keepdims=True))
            probs = expd / jnp.sum(expd, axis=-1, keepdims=True)
            probs_buf[h] = probs
            heads_buf[:, cols] = dot(probs.astype(BF), values).astype(BF)
    store(heads_buf, heads_out)
    with jax.named_scope('w_out'):
        loads[5].wait()
        scatter3 = Scatter(pos, n1_buf, attn_part, *scatters[1], *main_s)
        scatter1.drain()
        halves(scatter3, lambda col: dot(heads_buf[...], wo[:, pl.ds(col, wide)]))

    with jax.named_scope('rs3_a'):
        scatter3.relay_low()
        scatter3.relay_high()

    with jax.named_scope('grad_act'):
        loads[6].wait()

        @pl.loop(0, ffn // 256)
        def _(j):
            cols = pl.ds(pl.multiple_of(j * 256, 256), 256)
            gact[:, cols] = dot_bt(full(gh_buf), wd[cols, :]).astype(BF)

    with jax.named_scope('rs3_b'):
        scatter3.relay_far()
        h1_bf = (x0 + scatter3.finish()).astype(BF)
    with jax.named_scope('norm2'):
        h1 = h1_bf.astype(F32)
        normed2, inv2 = norm_stats(h1)
        n2_buf[pos.me] = (normed2 * gain_mlp[...]).astype(BF)
    with jax.named_scope('ag4'):
        gather4 = Gather(pos, n2_buf, *main_g)
        gather1.drain()
        gather4.start()
        turn(wqkv, wqkv_t, 0)
        gather4.relay()
        gather4.finish()
    store(n2_buf, n2_out)

    with jax.named_scope('gate_up'):
        @pl.loop(0, ffn // 512)
        def _(j):
            cols = pl.ds(pl.multiple_of(j * 512, 512), 512)
            n2 = full(n2_buf)
            gate_pre = dot(n2, wg[:, cols])
            up_pre = dot(n2, wu[:, cols])
            sig = jax.nn.sigmoid(gate_pre)
            gate_act = gate_pre * sig
            act_buf[:, cols] = (gate_act * up_pre).astype(BF)
            grad_act = gact[:, cols].astype(F32)
            dgu_buf[:, pl.ds(pl.multiple_of(ffn + j * 512, 512), 512)] = (grad_act * gate_act).astype(BF)
            dgu_buf[:, cols] = (grad_act * up_pre * sig * (1.0 + gate_pre * (1.0 - sig))).astype(BF)

    store(act_buf, act_out)
    store(dgu_buf, dgu_out)
    with jax.named_scope('dn2'):
        scatter6 = Scatter(pos, n1_buf, dn2_part, *scatters[2], *main_s)
        scatter3.drain()
        halves(scatter6, lambda col: dot(dgu_buf[...], emb[:, pl.ds(col, wide)]))

    with jax.named_scope('rs6_a'):
        scatter6.relay_low()
        scatter6.relay_high()
    with jax.named_scope('w_down'):
        for h in range(2):
            put_part(mlp_part, dot(act_buf[...], wd[:, h * wide:(h + 1) * wide]), h * wide)
        gather0.drain()
        scatter5 = Scatter(pos, n1_buf, mlp_part, *scatters[3], *side)
        scatter5.start(0)
        scatter5.start(1)
    with jax.named_scope('rs6_b'):
        scatter6.relay_far()
        scatter5.relay_low()
        scatter5.relay_high()
        grad_n2 = scatter6.finish().astype(BF).astype(F32)
    with jax.named_scope('norm2_bwd'):
        grad_h1_norm, gain_mlp_part = norm_bwd(grad_n2, normed2, inv2, gain_mlp[...])
        grad_h1 = (grad_own[...].astype(F32) + grad_h1_norm).astype(BF)
        dh1_buf[pos.me] = grad_h1
    gather7 = Gather(pos, dh1_buf, *main_g)
    gather4.drain()
    gather7.start()
    with jax.named_scope('ag7'):
        gather7.relay()
        scatter5.relay_far()
        gather7.finish()
    store(dh1_buf, dh1_out)

    with jax.named_scope('dheads'):
        dheads = dot_bt(full(dh1_buf), wo[...]).astype(BF)
    with jax.named_scope('attention_bwd'):
        nsin2 = -sin2
        dkeys = jnp.zeros((seq, head_dim), F32)
        dvalues = jnp.zeros((seq, head_dim), F32)
        for h in range(num_heads):
            cols = slice(h * head_dim, (h + 1) * head_dim)
            dhead = dheads[:, cols]
            probs = probs_buf[h]
            dprobs = dot_bt(dhead, values).astype(BF).astype(F32)
            dvalues += dot_at(probs.astype(BF), dhead)
            inner = jnp.sum(dprobs * probs, axis=-1, keepdims=True)
            dscores = (probs * (dprobs - inner) * (head_dim ** -0.5)).astype(BF)
            dquery = dot(dscores, keys).astype(BF)
            dkeys += dot_at(dscores, q_buf[:, cols])
            dqkv_buf[:, cols] = rope(dquery.astype(F32), cos2, nsin2).astype(BF)
        dqkv_buf[:, kq:kq + head_dim] = rope(dkeys.astype(BF).astype(F32), cos2, nsin2).astype(BF)
        dqkv_buf[:, kq + head_dim:] = dvalues.astype(BF)
    store(dqkv_buf, dqkv_out)

    with jax.named_scope('dn1'):
        scatter8 = Scatter(pos, n1_buf, dn1_part, *scatters[4], *main_s)
        scatter6.drain()
        halves(scatter8, lambda col: dot(dqkv_buf[...], wqkv_t[:, pl.ds(col, wide)]))

    with jax.named_scope('rs8'):
        scatter8.relay_low()
        scatter8.relay_high()
        hidden_buf[...] = (h1 + scatter5.finish()).astype(BF)
        store(hidden_buf, hidden_out)
        scatter8.relay_far()
        grad_n1 = scatter8.finish().astype(BF).astype(F32)
    with jax.named_scope('norm1_bwd'):
        grad_x_norm, gain_attn_part = norm_bwd(grad_n1, normed1, inv1, gain_attn[...])
        dx_pair[pos.core, 0:rows, :] = (grad_h1.astype(F32) + grad_x_norm).astype(BF)
        gain_parts = jnp.concatenate([gain_attn_part, gain_mlp_part], axis=0)
        high = gain_parts.astype(BF)
        dx_pair[pos.core, rows:rows + 2, :] = high
        dx_pair[pos.core, rows + 2:rows + 4, :] = (gain_parts - high.astype(F32)).astype(BF)
    with jax.named_scope('pair'):
        mine = remote(dx_pair.at[pos.core], dx_out.at[pos.core], *(sem.at[0] for sem in pair_s), pos.partner)
        theirs = remote(dx_pair.at[pos.core], dx_out.at[pos.other], *(sem.at[0] for sem in pair_s), pos.partner)
        mine.start()
        store(dx_pair.at[pos.core], dx_out.at[pos.core])
        mine.wait_send()
        theirs.wait_recv()
    with jax.named_scope('tail'):
        for op in (scatter5, scatter8, gather7):
            op.drain()
        for copy in stores:
            copy.wait()


def layer(tokens, positions, gain_attn, gain_mlp, grad_own, emb, wq, wk, wv, wo, wg, wu, wd):
    num_heads, dim, head_dim = wq.shape
    blocks = CHIPS * CORES
    seq, ffn, rows_local = tokens.shape[1], wg.shape[1], emb.shape[0]
    rows = seq // blocks
    if rows_local != 2 * ffn:
        raise ValueError('shard rows')
    half = head_dim // 2
    freq = np.float32(ROPE_THETA) ** (-np.arange(half, dtype=np.float32) * np.float32(2.0 / head_dim))
    freq = jnp.asarray(np.concatenate([freq, freq])[:, None], F32)
    vmem = pl.BlockSpec(memory_space=pltpu.VMEM)
    hbm = pl.BlockSpec(memory_space=pltpu.HBM)
    width = num_heads * head_dim
    wide = width + 2 * head_dim
    sds = jax.ShapeDtypeStruct
    outs = [sds((CORES, rows + 4, dim), BF), sds((rows, dim), BF)] + [sds((blocks, rows, dim), BF)] * 4
    outs += [sds((seq, width), BF), sds((seq, ffn), BF), sds((seq, 2 * ffn), BF), sds((seq, wide), BF)]
    part = pltpu.VMEM((CORES, CHIPS, rows, dim), BF)
    gathered = pltpu.VMEM((blocks, rows, dim), BF)
    table = pltpu.VMEM((seq, head_dim), F32)
    scratch = [pltpu.VMEM((rows_local, dim), BF), pltpu.VMEM((seq, rows_local), BF), pltpu.VMEM((dim, wide), BF), pltpu.VMEM((wide, dim), BF),
               pltpu.VMEM((width, dim), BF), pltpu.VMEM((dim, ffn), BF),
               pltpu.VMEM((dim, ffn), BF), pltpu.VMEM((ffn, dim), BF), pltpu.SemaphoreType.DMA((15,)), pltpu.SemaphoreType.DMA((10,))]
    scratch += [gathered] * 4 + [part] * 5 + [pltpu.VMEM((seq, width), BF)]
    scratch += [pltpu.VMEM((seq, ffn), BF)] * 2 + [pltpu.VMEM((seq, 2 * ffn), BF), pltpu.VMEM((seq, wide), BF), pltpu.VMEM((seq, width), BF),
                                                   pltpu.VMEM((num_heads, seq, seq), F32), table, table,
                                                   pltpu.VMEM((rows, dim), BF), pltpu.VMEM((CORES, rows + 4, dim), BF),
                                                   pltpu.VMEM((1, seq), jnp.int32), pltpu.VMEM((1, seq), jnp.int32), pltpu.VMEM((head_dim, 1), F32),
                                                   pltpu.VMEM((1, dim), F32), pltpu.VMEM((1, dim), F32), pltpu.VMEM((rows, dim), BF),
                                                   pltpu.SemaphoreType.DMA((7,))]
    scratch += scatter_scratch(rows, dim) * 5 + SCATTER_SEMS + GATHER_SEMS * 2 + [pltpu.SemaphoreType.DMA((1,))] * 2
    return pl.pallas_call(
        layer_kernel, out_shape=outs, in_specs=[hbm] * 14, out_specs=[hbm] * 10,
        scratch_shapes=scratch,
        compiler_params=pltpu.CompilerParams(collective_id=0, has_side_effects=True, vmem_limit_bytes=VMEM_FULL),
        name='layer',
    )(tokens, positions, freq, gain_attn, gain_mlp, grad_own, emb, wq, wk, wv, wo, wg, wu, wd)


def grads_kernel(n1, n2, dqkv, dgate, dup, heads, act, dh1, gh, hidden_in,
                 gw_query, gw_key, gw_value, gw_out, gw_gate, gw_up, gw_down, hidden):
    num_heads, _, head_dim = gw_query.shape
    width = num_heads * head_dim

    @pl.when(pl.program_id(0) == 0)
    def _():
        hidden[...] = hidden_in[...]

    gw_gate[...] = dot_at(n2[...], dgate[...])
    gw_up[...] = dot_at(n2[...], dup[...])
    gw_down[...] = dot_at(act[...], gh[...])
    both = dot_at(n1[...], dqkv[...])
    for h in range(num_heads):
        gw_query[h] = both[:, h * head_dim:(h + 1) * head_dim]
    gw_key[...] = both[:, width:width + head_dim]
    gw_value[...] = both[:, width + head_dim:]
    gw_out[...] = dot_at(heads[...], dh1[...])


def grads(n1, n2, dqkv, dgu, heads, act, dh1, gh, hidden, head_dim):
    seq, dim = n1.shape
    width, ffn = heads.shape[1], act.shape[1]
    num_heads = width // head_dim
    tile = 256
    sds = jax.ShapeDtypeStruct

    def whole(x):
        return pl.BlockSpec(x.shape, lambda i: (0,) * len(x.shape))

    def by_col(n):
        return pl.BlockSpec((n, tile), lambda i: (0, i))

    def by_row(n):
        return pl.BlockSpec((tile, n), lambda i: (i, 0))

    return pl.pallas_call(
        grads_kernel, grid=(dim // tile,),
        out_shape=[sds((num_heads, dim, head_dim), F32), sds((dim, head_dim), F32), sds((dim, head_dim), F32), sds((width, dim), F32),
                   sds((dim, ffn), F32), sds((dim, ffn), F32), sds((ffn, dim), F32), sds(hidden.shape, BF)],
        in_specs=[by_col(seq), by_col(seq), whole(dqkv), pl.BlockSpec((seq, ffn), lambda i: (0, 0)),
                  pl.BlockSpec((seq, ffn), lambda i: (0, 1)), whole(heads), whole(act), by_col(seq), by_col(seq), whole(hidden)],
        out_specs=[pl.BlockSpec((num_heads, tile, head_dim), lambda i: (0, i, 0)), by_row(head_dim), by_row(head_dim), by_col(width),
                   by_row(ffn), by_row(ffn), by_col(ffn), whole(hidden)],
        compiler_params=pltpu.CompilerParams(vmem_limit_bytes=VMEM_FULL),
        cost_estimate=pl.CostEstimate(flops=20_000_000_000, bytes_accessed=50_000_000, transcendentals=0),
        name='grads',
    )(n1, n2, dqkv, dgu, dgu, heads, act, dh1, gh, hidden)


def emb_grad_kernel(tokens, *refs):
    pairs = refs[:CHIPS]
    g_emb, g_attn, g_mlp, dx, gains, ring, sem = refs[CHIPS:]
    seq, rows = dx.shape[0], dx.shape[0] // (CHIPS * CORES)
    me = lax.axis_index('tp')
    for k, pair in enumerate(pairs):
        chip = (me // CORES + CHIPS - k) % CHIPS
        for core in range(CORES):
            source = chip * CORES + core
            dx[pl.ds(pl.multiple_of(source * rows, rows), rows), :] = pair[core, 0:rows, :]
            gains[source] = pair[core, rows:rows + 2, :].astype(F32) + pair[core, rows + 2:rows + 4, :].astype(F32)

    slots, height = ring.shape[0], ring.shape[1]
    rows_local = g_emb.shape[0]
    local = tokens[...] - me * rows_local
    row = lax.broadcasted_iota(jnp.int32, (height, seq), 0)
    copies = []
    for c in range(rows_local // height):
        slot = c % slots
        if c >= slots:
            copies[c - slots].wait()
        ring[slot] = dot(jnp.where(row + c * height == local, 1.0, 0.0).astype(BF), dx[...])
        copies.append(pltpu.make_async_copy(ring.at[slot], g_emb.at[pl.ds(c * height, height)], sem.at[slot]))
        copies[-1].start()
    total = gains[0]
    for i in range(1, CHIPS * CORES):
        total = total + gains[i]
    g_attn[...] = total[0:1, :]
    g_mlp[...] = total[1:2, :]
    for copy in copies[-slots:]:
        copy.wait()


def emb_grad(tokens, pairs, rows_local):
    seq, dim = tokens.shape[1], pairs[0].shape[2]
    height, slots = 128, 8
    sds = jax.ShapeDtypeStruct
    vmem = pl.BlockSpec(memory_space=pltpu.VMEM)
    gain = sds((1, dim), F32)
    return pl.pallas_call(
        emb_grad_kernel, out_shape=[sds((rows_local, dim), F32), gain, gain],
        in_specs=[vmem] * (1 + len(pairs)), out_specs=[pl.BlockSpec(memory_space=pltpu.HBM), vmem, vmem],
        scratch_shapes=[pltpu.VMEM((seq, dim), BF), pltpu.VMEM((CHIPS * CORES, 2, dim), F32), pltpu.VMEM((slots, height, dim), F32),
                        pltpu.SemaphoreType.DMA((slots,))],
        compiler_params=pltpu.CompilerParams(vmem_limit_bytes=VMEM_FULL),
        name='emb_grad',
    )(tokens, *pairs)


def solution(mesh):
    if mesh.shape['tp'] != CHIPS * CORES:
        raise ValueError('tp size')
    in_specs = (P('dp', None), P('dp', None), P('tp', None), P(None), P(None),
                P(None, 'tp', None), P(None, 'tp', None), P(None, 'tp', None), P('tp', None, None),
                P(None, 'tp'), P(None, 'tp'), P('tp', None), P('dp', 'tp', None))
    out_specs = (P('dp', 'tp', None), P(('dp', 'tp'), None),
                 P('dp', 'tp', None), P('dp', 'tp', None), P('dp', 'tp', None), P(('dp', 'tp'), None, None),
                 P('dp', 'tp'), P('dp', 'tp'), P(('dp', 'tp'), None), P('dp'), P('dp'))

    def device_fn(tokens, positions, emb_shard, gain_attn, gain_mlp, w_query, w_key, w_value, w_out, w_gate, w_up, w_down, grad_hidden):
        rows_local, dim = emb_shard.shape
        seq = tokens.shape[1]
        num_heads, head_dim = w_query.shape[1], w_query.shape[2]
        wq = jnp.transpose(w_query, (1, 0, 2))
        wk, wv = w_key.reshape(dim, head_dim), w_value.reshape(dim, head_dim)
        wo = w_out.reshape(num_heads * head_dim, dim)

        dx_pair, hidden, n1, n2, gh, dh1, heads, act, dgu, dqkv = layer(
            tokens, positions, gain_attn[None, :], gain_mlp[None, :], grad_hidden[0], emb_shard, wq, wk, wv, wo, w_gate, w_up, w_down)
        n = CHIPS * CORES
        arrived = [dx_pair] + [lax.ppermute(dx_pair, 'tp', [(i, (i + k * CORES) % n) for i in range(n)]) for k in range(1, CHIPS)]
        n1, n2, gh, dh1 = (x.reshape(seq, dim) for x in (n1, n2, gh, dh1))
        gw_query, gw_key, gw_value, gw_out, gw_gate, gw_up, gw_down, hidden = grads(
            n1, n2, dqkv, dgu, heads, act, dh1, gh, hidden, head_dim)
        g_emb, g_attn, g_mlp = emb_grad(tokens, arrived, rows_local)
        return (hidden[None], g_emb, jnp.transpose(gw_query, (1, 0, 2)), gw_key.reshape(dim, 1, head_dim),
                gw_value.reshape(dim, 1, head_dim), gw_out.reshape(num_heads, head_dim, dim),
                gw_gate, gw_up, gw_down, g_attn[0], g_mlp[0])

    return jax.shard_map(device_fn, mesh=mesh, in_specs=in_specs, out_specs=out_specs, check_vma=False)
```
